256 devices in a mesh: rows: 8 (over y_hi, x), cols: 32 (over y_lo, z, core).
Axes of the slice: x: 4, y: 4 (y_hi: 2, y_lo: 2; y = y_hi * 2 + y_lo), z: 8, core: 2. Of those that a mesh axis runs over, the one named last changes fastest.
Arguments:
- embeddings: bfloat16 [65536, 768], P(('rows', 'cols')), may hold values from -6 to 6
- document_cluster_index: int32 [65536], P(('rows', 'cols')), may hold values from 0 to 127, as said below
Outputs:
- max_similarity: float32 [65536], P(('rows', 'cols'))
- histogram: float32 [128], replicated
The draws below stay inside these ranges and needn't reach their ends.
Inputs may be any that keep to these rules, and one draw needn't show every extreme that they name: `document_cluster_index`: cluster r * 16 to (r + 1) * 16 - 1 form row group r. Each device's block of 256 documents names at most 64 documents of any one row group, and exactly 64 of one. The documents that the devices with one index along cols name for one row group hold at most 64 documents of any one cluster, and in every draw some such set holds exactly 64 of one cluster.
All inputs are finite; a program needn't handle non-finite values.
Results may differ from the reference program's by a relative error of at most 0.0014.
Values may be sent and summed in bfloat16 or wider, within the bound.
No kernel may reach another device: no remote copies, remote signals or barrier semaphores. Data moves between devices by JAX's collectives and lax.ppermute only.
A program may use at most 64 MiB of HBM per device.

```python
import jax
import jax.numpy as jnp
from jax import lax

D = 768
CAP = 64
GROUP_CLUSTERS = 16
BINS = 128
CLUSTER_DOC_PEAK = 64
DOC_DEV = 256
DOCS = 65536
N_ROWS = 8
N_COLS = 32


def draw_document_cluster_index(key, part):
    row_offset = jax.random.randint(jax.random.fold_in(key, 7), (N_ROWS,), 0, GROUP_CLUSTERS)
    fixed_col = jax.random.randint(jax.random.fold_in(key, 8), (), 0, N_COLS)
    fixed_row = jax.random.randint(jax.random.fold_in(key, 9), (), 0, N_ROWS)
    device_base = jax.random.fold_in(key, 11)
    order_base = jax.random.fold_in(key, 12)
    pool_rows = jnp.arange((N_ROWS - 1) * CAP, dtype=jnp.int32) // CAP

    def one_device(device_index):
        device_key = jax.random.fold_in(device_base, device_index)
        first_row = jax.random.randint(jax.random.fold_in(device_key, 1), (), 0, N_ROWS)
        first_row = jnp.where(device_index % N_COLS == fixed_col, fixed_row, first_row).astype(jnp.int32)
        other_rows = (first_row + 1 + pool_rows) % N_ROWS
        other_rows = jax.random.permutation(jax.random.fold_in(device_key, 2), other_rows)[:DOC_DEV - CAP]
        targets = jnp.concatenate([jnp.full((CAP,), first_row, jnp.int32), other_rows.astype(jnp.int32)])
        return jax.random.permutation(jax.random.fold_in(device_key, 3), targets).astype(jnp.int32)
    targets = jax.vmap(one_device)(jnp.arange(N_ROWS * N_COLS, dtype=jnp.int32))
    column_wise = targets.reshape(N_ROWS, N_COLS, DOC_DEV).transpose(1, 0, 2).reshape(N_COLS, N_ROWS * DOC_DEV)
    onehot = (column_wise[:, :, None] == jnp.arange(N_ROWS, dtype=jnp.int32)[None, None, :]).astype(jnp.int32)
    ranks = jnp.sum((jnp.cumsum(onehot, axis=1) - 1) * onehot, axis=2).astype(jnp.int32)
    pooled_clusters = jnp.arange(GROUP_CLUSTERS * CLUSTER_DOC_PEAK, dtype=jnp.int32) // CLUSTER_DOC_PEAK
    stride_length = max(1, 2 ** 20 // GROUP_CLUSTERS)

    def single_order(order_index):
        row_group = order_index % N_ROWS
        sorting_key = jax.random.fold_in(order_base, order_index)
        current_best = (pooled_clusters - row_offset[row_group]) % GROUP_CLUSTERS
        similarity_scores = jax.random.randint(sorting_key, (GROUP_CLUSTERS * CLUSTER_DOC_PEAK,), 0, 2 ** 20) + current_best * stride_length
        similarity_scores = jnp.where(current_best == 0, -1, similarity_scores)
        return pooled_clusters[jnp.argsort(similarity_scores, stable=True)].astype(jnp.int32)
    order_list = jax.vmap(single_order)(jnp.arange(N_COLS * N_ROWS, dtype=jnp.int32)).reshape(N_COLS, N_ROWS, GROUP_CLUSTERS * CLUSTER_DOC_PEAK)
    cluster_member = order_list[jnp.arange(N_COLS, dtype=jnp.int32)[:, None], column_wise, ranks]
    cluster_labels = column_wise * GROUP_CLUSTERS + cluster_member
    return cluster_labels.reshape(N_COLS, N_ROWS, DOC_DEV).transpose(1, 0, 2).reshape(-1).astype(jnp.int32)


def shard_levels(stream_key, dims, split, least, high):
    def one(axis_at, blocks):
        steps = jax.random.uniform(jax.random.fold_in(jax.random.fold_in(stream_key, 6), axis_at), (blocks,), jnp.float32, least / len(split), high / len(split))
        return jnp.repeat(jnp.exp(steps), dims[axis_at] // blocks).reshape((-1,) + (1,) * (len(dims) - axis_at - 1))

    gain = one(*split[0])
    for cut in split[1:]:
        gain = gain * one(*cut)
    return gain


def noise(rng, shape, scale, limit, split=(), kind=jnp.bfloat16):
    loudness = shard_levels(rng, shape, split, -0.22, 0.18) if split else 1.0
    result = jax.random.normal(rng, shape, jnp.float32) * scale * loudness
    return jnp.minimum(jnp.maximum(result, -limit), limit).astype(kind)


def setup_inputs(seed: int = 0) -> dict:
    arg_keys = jax.random.split(jax.random.key(seed), 3)
    embeddings = noise(arg_keys[0], (DOCS, D), 1.0, 6.0, ((0, 256),))
    document_cluster_index = draw_document_cluster_index(jax.random.fold_in(arg_keys[2], 71), 0)
    return dict(embeddings=embeddings, document_cluster_index=document_cluster_index)


def reference(embeddings, document_cluster_index):
    values = embeddings.astype(jnp.float32)
    normed = (values * lax.rsqrt(lax.optimization_barrier(jnp.sum(values * values, axis=1, keepdims=True)) + 1e-06)).astype(jnp.bfloat16)
    doc_total = document_cluster_index.shape[0]
    owner_devices = (document_cluster_index // GROUP_CLUSTERS).astype(jnp.int32)
    doc_order = jnp.argsort(owner_devices, stable=True).astype(jnp.int32)
    counts = lax.optimization_barrier(jnp.sum((owner_devices[:, None] == jnp.arange(N_ROWS, dtype=jnp.int32)[None, :]).astype(jnp.int32), axis=0))
    starts = (jnp.cumsum(counts) - counts).astype(jnp.int32)
    row_span = CAP * N_ROWS * N_COLS
    tile_rows = min(512, row_span)
    sorted_rows = jnp.concatenate([normed[doc_order].astype(jnp.float32), jnp.zeros((row_span, normed.shape[1]), jnp.float32)], axis=0)
    cluster_labels = jnp.concatenate([document_cluster_index[doc_order].astype(jnp.int32), jnp.full((row_span,), -1, jnp.int32)], axis=0)
    span_index = jnp.arange(row_span, dtype=jnp.int32)

    def per_group(row_group):
        group_rows = lax.dynamic_slice_in_dim(sorted_rows, starts[row_group], row_span, 0)
        group_labels = lax.dynamic_slice_in_dim(cluster_labels, starts[row_group], row_span, 0)
        group_labels = jnp.where(span_index < counts[row_group], group_labels, -1)

        def per_tile(tile_index):
            tile_start = (tile_index * tile_rows).astype(jnp.int32)
            tile = lax.dynamic_slice_in_dim(group_rows, tile_start, tile_rows, 0)
            tile_labels = lax.dynamic_slice_in_dim(group_labels, tile_start, tile_rows, 0)
            similarity_scores = jnp.dot(tile, group_rows.T, precision=lax.Precision.HIGHEST)
            tile_index_rows = tile_start + jnp.arange(tile_rows, dtype=jnp.int32)
            same_cluster = (tile_labels[:, None] == group_labels[None, :]) & (tile_labels[:, None] >= 0)
            same_cluster = same_cluster & (tile_index_rows[:, None] != span_index[None, :])
            return lax.optimization_barrier(jnp.max(jnp.where(same_cluster, similarity_scores, -1.0), axis=1))
        return lax.map(per_tile, jnp.arange(row_span // tile_rows, dtype=jnp.int32)).reshape(row_span)
    results = lax.map(per_group, jnp.arange(N_ROWS, dtype=jnp.int32))
    sorted_owner = owner_devices[doc_order]
    offsets = (jnp.arange(doc_total, dtype=jnp.int32) - starts[sorted_owner]).astype(jnp.int32)
    sorted_values = results[sorted_owner, offsets]
    max_similarity = jnp.zeros((doc_total,), jnp.float32).at[doc_order].set(sorted_values)
    bin_width = 2.0 / (BINS - 1)
    centers = -1.0 + jnp.arange(BINS, dtype=jnp.float32) * bin_width
    bin_weights = jax.nn.relu(1.0 - jnp.abs(max_similarity[:, None] - centers[None, :]) / bin_width)
    histogram = lax.optimization_barrier(jnp.sum(bin_weights, axis=0)) / doc_total
    return (max_similarity, histogram)
```

```python
import jax
import jax.numpy as jnp
from jax import lax
from jax.experimental import pallas as pl
from jax.experimental.pallas import tpu as pltpu
from jax.sharding import Mesh
from jax.sharding import PartitionSpec as P

CAP = 64
GROUP_CLUSTERS = 16
BINS = 128
ROWS = ("rows_0", "rows_1")
COLS = ("cols_0", "cols_1", "cols_2")
ALL = ROWS + COLS
META = 8
EMPTY = 2.0
F32 = jnp.float32
BF16 = jnp.bfloat16


def iota(shape, dim):
    return lax.broadcasted_iota(jnp.int32, shape, dim)


def dot(a, b):
    return lax.dot_general(a, b, (((1,), (0,)), ((), ())), preferred_element_type=F32)


def dot_t(a, b):
    return lax.dot_general(a, b, (((1,), (1,)), ((), ())), preferred_element_type=F32)


def ones_where(mask):
    return jnp.where(mask, 1.0, 0.0).astype(BF16)


def before(n):
    return ones_where(iota((n, n), 0) < iota((n, n), 1))


def rank_of(onehot, n):
    earlier = dot(onehot, before(n))
    return jnp.sum(onehot.astype(F32) * earlier, axis=0, keepdims=True)


def normalise_and_slot(labels_ref, embeddings_ref, out_ref, rank_ref):
    docs, width = embeddings_ref.shape
    groups = out_ref.shape[0]
    clusters = groups * GROUP_CLUSTERS
    labels = labels_ref[...]
    group = lax.shift_right_logical(labels, 4)
    onehot = ones_where(iota((groups, docs), 0) == group)
    slot = group * CAP + rank_of(onehot, docs).astype(jnp.int32)
    places = ones_where(iota((groups * CAP, docs), 0) == slot)
    values = embeddings_ref[...].astype(F32)
    total = jnp.sum(values * values, axis=1, keepdims=True)
    normed = (values * lax.rsqrt(total + 1e-06)).astype(BF16)
    rows = dot(places, normed).astype(BF16)
    out_ref[:, 0:CAP, :] = rows.reshape(groups, CAP, width)
    shifted = jnp.broadcast_to((labels + 1).astype(F32), (META, docs)).astype(BF16)
    slot_labels = dot_t(shifted, places)
    of_cluster = ones_where(iota((clusters, docs), 0) == labels)
    counts = dot_t(jnp.ones((META, docs), BF16), of_cluster)
    blank = jnp.zeros((META, width - groups * CAP - clusters), F32)
    meta = jnp.concatenate([slot_labels, counts, blank], axis=1).astype(BF16)
    for g in range(groups):
        out_ref[g, CAP:, :] = meta
    rank_ref[...] = rank_of(of_cluster, docs)


def meta_rows(got_ref):
    groups = got_ref.shape[0]
    meta = got_ref[0, CAP:, :].astype(F32)
    row = iota(meta.shape, 0)
    for g in range(1, groups):
        meta = jnp.where(row == g, got_ref[g, CAP:, :].astype(F32), meta)
    return meta


def reslot(where_ref, got_ref, out_ref):
    groups, _, width = got_ref.shape
    slots = groups * CAP
    me = where_ref[0]
    labels = meta_rows(got_ref)[:, 0:slots].astype(BF16)
    lane, at = iota((slots, slots), 0), iota((slots, slots), 1)
    mine = ones_where(lane == me * CAP + lax.bitwise_and(at, CAP - 1))
    picked = dot(labels, mine)
    own = iota((groups, slots), 0) == lax.shift_right_logical(iota((groups, slots), 1), 6)
    label = jnp.sum(jnp.where(own, picked, 0.0), axis=0, keepdims=True).astype(jnp.int32)
    cluster = label - 1 - me * GROUP_CLUSTERS
    onehot = ones_where(iota((GROUP_CLUSTERS, slots), 0) == cluster)
    place = cluster * CAP + rank_of(onehot, slots).astype(jnp.int32)
    place = jnp.where(label > 0, place, -1)
    total = GROUP_CLUSTERS * CAP
    step = total // 4
    rows = got_ref[:, 0:CAP, :].reshape(slots, width)
    for s in range(0, total, step):
        places = jnp.where(iota((step, slots), 0) + s == place, 1.0, 0.0)
        filled = jnp.sum(places, axis=1, keepdims=True) > 0.5
        moved = dot(places.astype(BF16), rows)
        out_ref[s : s + step, :] = moved.astype(BF16)
        first = moved[:, 0:128]
        first = jnp.where((iota(first.shape, 1) == 0) & ~filled, EMPTY, first)
        out_ref[s : s + step, 0:128] = first.astype(BF16)


def return_index(where_ref, labels_ref, rank_ref, got_ref, out_ref):
    groups = got_ref.shape[0]
    docs = labels_ref.shape[1]
    clusters = groups * GROUP_CLUSTERS
    me = where_ref[0]
    counts = meta_rows(got_ref)[:, groups * CAP : groups * CAP + clusters]
    counts = jnp.where(iota(counts.shape, 0) < me, counts, 0.0).astype(BF16)
    labels = labels_ref[...]
    of_cluster = ones_where(iota((clusters, docs), 0) == labels)
    earlier = jnp.sum(dot(counts, of_cluster), axis=0, keepdims=True)
    out_ref[...] = labels * CAP + (rank_ref[...] + earlier).astype(jnp.int32)


def best_against(own_ref, other_ref, same):
    total = own_ref.shape[0]
    block = 256
    out = []
    for j in range(0, total, block):
        mine = own_ref[j : j + block, :]
        best = jnp.full((8, block), -1.0, F32)
        for i in range(0, total, block):
            theirs = other_ref[i : i + block, :]
            scores = dot_t(theirs, mine)
            keep = theirs[:, 0:1].astype(F32) < 1.5
            if same and i == j:
                keep = keep & (iota((block, block), 0) != iota((block, block), 1))
            scores = jnp.where(keep, scores, -1.0)
            best = jnp.maximum(best, jnp.max(scores.reshape(block // 8, 8, block), axis=0))
        out.append(jnp.max(best, axis=0, keepdims=True))
    return jnp.concatenate(out, axis=1)


def best_own(own_ref, out_ref):
    out_ref[...] = best_against(own_ref, own_ref, True)


def best_all(own_ref, other_ref, first_ref, out_ref):
    total = own_ref.shape[0]
    best = jnp.maximum(best_against(own_ref, other_ref, False), first_ref[...])
    pick = ones_where(iota((8, 256), 1) == 0)
    flag = dot_t(pick, own_ref[:, 0:256])[0:1, :]
    width = 2.0 / (BINS - 1)
    centers = -1.0 + iota((BINS, 1), 0).astype(F32) * width
    weights = jnp.maximum(1.0 - jnp.abs(best - centers) / width, 0.0)
    weights = jnp.where(flag < 1.5, weights, 0.0)
    folded = weights[:, 0:128]
    for s in range(128, total, 128):
        folded = folded + weights[:, s : s + 128]
    hist = jnp.sum(folded.T, axis=0, keepdims=True)
    rows = out_ref.shape[0]
    hists = jnp.broadcast_to(hist, (rows, BINS))
    out_ref[:, 128:256] = hists
    pieces = jnp.concatenate(
        [jnp.broadcast_to(best[:, s : s + 128], (4, 128)) for s in range(0, total, 128)], axis=0
    )
    for s in range(0, rows, 32):
        out_ref[s : s + 32, 0:128] = pieces


def pick_results(where_ref, index_ref, got_ref, best_ref, hist_ref):
    owners = got_ref.shape[0]
    docs = index_ref.shape[1]
    quarter = where_ref[1]
    index = index_ref[...]
    owner = lax.shift_right_logical(index, 5)
    lane = quarter * 32 + lax.bitwise_and(index, 31)
    onehot = ones_where(iota((owners, docs), 0) == owner)
    values = got_ref[:, 0:128].T
    high = values.astype(BF16)
    rest = values - high.astype(F32)
    middle = rest.astype(BF16)
    low = (rest - middle.astype(F32)).astype(BF16)
    picked = dot(high, onehot) + dot(middle, onehot) + dot(low, onehot)
    picked = jnp.where(iota((128, docs), 0) == lane, picked, 0.0)
    best_ref[...] = jnp.sum(picked, axis=0, keepdims=True)
    hist = jnp.sum(got_ref[:, 128:256], axis=0, keepdims=True)
    hist_ref[...] = hist * (1.0 / (owners * docs))


VMEM = pl.BlockSpec(memory_space=pltpu.VMEM)
SMEM = pl.BlockSpec(memory_space=pltpu.SMEM)


def call(kernel, outs, specs, flops):
    many = isinstance(outs, tuple)
    return pl.pallas_call(
        kernel,
        out_shape=outs,
        in_specs=specs,
        out_specs=tuple(VMEM for _ in outs) if many else VMEM,
        cost_estimate=pl.CostEstimate(flops=flops, bytes_accessed=4000000, transcendentals=0),
    )


def shape(dims, dtype):
    return jax.ShapeDtypeStruct(dims, dtype)


def exchange(x, axes):
    return lax.all_to_all(x, axes, split_axis=0, concat_axis=0, tiled=True)


def shards(embeddings, document_cluster_index):
    row_count = lax.axis_size(ROWS)
    col_count = lax.axis_size(COLS)
    docs, width = embeddings.shape
    labels = document_cluster_index.reshape(1, docs)
    col = lax.axis_index(COLS)
    where = jnp.stack([lax.axis_index(ROWS), col % 4]).astype(jnp.int32)
    block = CAP + META
    sends, rank = call(
        normalise_and_slot,
        (shape((row_count, block, width), BF16), shape((1, docs), F32)),
        [VMEM, VMEM],
        2 * row_count * CAP * docs * width,
    )(labels, embeddings)
    got = exchange(sends, ROWS)
    total = GROUP_CLUSTERS * CAP
    sends = call(
        reslot, shape((total, width), BF16), [SMEM, VMEM], 2 * total * row_count * CAP * width
    )(where, got)
    index = call(return_index, shape((1, docs), jnp.int32), [SMEM, VMEM, VMEM, VMEM], 2**26)(
        where, labels, rank, got
    )
    own = exchange(sends.reshape(col_count, total // col_count, width), COLS)
    own = own.reshape(total, width)
    other = lax.ppermute(own, COLS, [(i, i ^ 1) for i in range(col_count)])
    flops = 2 * total * total * width
    first = call(best_own, shape((1, total), F32), [VMEM], flops)(own)
    results = call(
        best_all, shape((row_count * col_count, 256), F32), [VMEM, VMEM, VMEM], flops
    )(own, other, first)
    results = exchange(results, ALL)
    best, hist = call(
        pick_results, (shape((1, docs), F32), shape((1, BINS), F32)), [SMEM, VMEM, VMEM], 2**26
    )(where, index, results)
    return (best.reshape(docs), hist.reshape(BINS))


def solution(mesh):
    torus = Mesh(
        mesh.devices.reshape(2, 4, 2, 8, 2), ("rows_0", "rows_1", "cols_0", "cols_1", "cols_2")
    )
    in_specs = (P(ALL, None), P(ALL))
    out_specs = (P(ALL), P())
    return jax.shard_map(
        shards, mesh=torus, in_specs=in_specs, out_specs=out_specs, check_vma=False
    )
```

```python
import jax
import jax.numpy as jnp
from jax import lax
from jax.experimental import pallas as pl
from jax.experimental.pallas import tpu as pltpu
from jax.sharding import Mesh
from jax.sharding import PartitionSpec as P

CAP = 64
GROUP_CLUSTERS = 16
BINS = 128
ROWS = ("rows_0", "rows_1")
COLS = ("cols_0", "cols_1", "cols_2")
ALL = ROWS + COLS
META = 8
EMPTY = 2.0
F32 = jnp.float32
BF16 = jnp.bfloat16


def iota(shape, dim):
    return lax.broadcasted_iota(jnp.int32, shape, dim)


def dot(a, b):
    return lax.dot_general(a, b, (((1,), (0,)), ((), ())), preferred_element_type=F32)


def dot_t(a, b):
    return lax.dot_general(a, b, (((1,), (1,)), ((), ())), preferred_element_type=F32)


def ones_where(mask):
    return jnp.where(mask, 1.0, 0.0).astype(BF16)


def before(n):
    return ones_where(iota((n, n), 0) < iota((n, n), 1))


def rank_of(onehot, n):
    earlier = dot(onehot, before(n))
    return jnp.sum(onehot.astype(F32) * earlier, axis=0, keepdims=True)


def normalise_and_slot(labels_ref, embeddings_ref, out_ref, rank_ref):
    docs, width = embeddings_ref.shape
    groups = out_ref.shape[0]
    clusters = groups * GROUP_CLUSTERS
    labels = labels_ref[...]
    group = lax.shift_right_logical(labels, 4)
    onehot = ones_where(iota((groups, docs), 0) == group)
    slot = group * CAP + rank_of(onehot, docs).astype(jnp.int32)
    places = ones_where(iota((groups * CAP, docs), 0) == slot)
    values = embeddings_ref[...].astype(F32)
    total = jnp.sum(values * values, axis=1, keepdims=True)
    normed = (values * lax.rsqrt(total + 1e-06)).astype(BF16)
    rows = dot(places, normed).astype(BF16)
    out_ref[:, 0:CAP, :] = rows.reshape(groups, CAP, width)
    shifted = jnp.broadcast_to((labels + 1).astype(F32), (META, docs)).astype(BF16)
    slot_labels = dot_t(shifted, places)
    of_cluster = ones_where(iota((clusters, docs), 0) == labels)
    counts = dot_t(jnp.ones((META, docs), BF16), of_cluster)
    blank = jnp.zeros((META, width - groups * CAP - clusters), F32)
    meta = jnp.concatenate([slot_labels, counts, blank], axis=1).astype(BF16)
    for g in range(groups):
        out_ref[g, CAP:, :] = meta
    rank_ref[...] = rank_of(of_cluster, docs)


def meta_rows(got_ref):
    groups = got_ref.shape[0]
    meta = got_ref[0, CAP:, :].astype(F32)
    row = iota(meta.shape, 0)
    for g in range(1, groups):
        meta = jnp.where(row == g, got_ref[g, CAP:, :].astype(F32), meta)
    return meta


def reslot(where_ref, got_ref, out_ref):
    groups, _, width = got_ref.shape
    slots = groups * CAP
    me = where_ref[0]
    labels = meta_rows(got_ref)[:, 0:slots].astype(BF16)
    lane, at = iota((slots, slots), 0), iota((slots, slots), 1)
    mine = ones_where(lane == me * CAP + lax.bitwise_and(at, CAP - 1))
    picked = dot(labels, mine)
    own = iota((groups, slots), 0) == lax.shift_right_logical(iota((groups, slots), 1), 6)
    label = jnp.sum(jnp.where(own, picked, 0.0), axis=0, keepdims=True).astype(jnp.int32)
    cluster = label - 1 - me * GROUP_CLUSTERS
    onehot = ones_where(iota((GROUP_CLUSTERS, slots), 0) == cluster)
    place = cluster * CAP + rank_of(onehot, slots).astype(jnp.int32)
    place = jnp.where(label > 0, place, -1)
    total = GROUP_CLUSTERS * CAP
    step = total // 4
    rows = got_ref[:, 0:CAP, :].reshape(slots, width)
    for s in range(0, total, step):
        places = jnp.where(iota((step, slots), 0) + s == place, 1.0, 0.0)
        filled = jnp.sum(places, axis=1, keepdims=True) > 0.5
        moved = dot(places.astype(BF16), rows)
        out_ref[s : s + step, :] = moved.astype(BF16)
        first = moved[:, 0:128]
        first = jnp.where((iota(first.shape, 1) == 0) & ~filled, EMPTY, first)
        out_ref[s : s + step, 0:128] = first.astype(BF16)


def return_index(where_ref, labels_ref, rank_ref, got_ref, out_ref):
    groups = got_ref.shape[0]
    docs = labels_ref.shape[1]
    clusters = groups * GROUP_CLUSTERS
    me = where_ref[0]
    counts = meta_rows(got_ref)[:, groups * CAP : groups * CAP + clusters]
    counts = jnp.where(iota(counts.shape, 0) < me, counts, 0.0).astype(BF16)
    labels = labels_ref[...]
    of_cluster = ones_where(iota((clusters, docs), 0) == labels)
    earlier = jnp.sum(dot(counts, of_cluster), axis=0, keepdims=True)
    out_ref[...] = labels * CAP + (rank_ref[...] + earlier).astype(jnp.int32)


def best_against(own_ref, other_ref, same):
    total = own_ref.shape[0]
    block = 256
    out = []
    for j in range(0, total, block):
        mine = own_ref[j : j + block, :]
        best = jnp.full((8, block), -1.0, F32)
        for i in range(0, total, block):
            theirs = other_ref[i : i + block, :]
            scores = dot_t(theirs, mine)
            keep = theirs[:, 0:1].astype(F32) < 1.5
            if same and i == j:
                keep = keep & (iota((block, block), 0) != iota((block, block), 1))
            scores = jnp.where(keep, scores, -1.0)
            best = jnp.maximum(best, jnp.max(scores.reshape(block // 8, 8, block), axis=0))
        out.append(jnp.max(best, axis=0, keepdims=True))
    return jnp.concatenate(out, axis=1)


def best_own(own_ref, out_ref):
    out_ref[...] = best_against(own_ref, own_ref, True)


def best_all(own_ref, other_ref, first_ref, out_ref):
    total = own_ref.shape[0]
    best = jnp.maximum(best_against(own_ref, other_ref, False), first_ref[...])
    pick = ones_where(iota((8, 256), 1) == 0)
    flag = dot_t(pick, own_ref[:, 0:256])[0:1, :]
    width = 2.0 / (BINS - 1)
    centers = -1.0 + iota((BINS, 1), 0).astype(F32) * width
    weights = jnp.maximum(1.0 - jnp.abs(best - centers) / width, 0.0)
    weights = jnp.where(flag < 1.5, weights, 0.0)
    folded = weights[:, 0:128]
    for s in range(128, total, 128):
        folded = folded + weights[:, s : s + 128]
    hist = jnp.sum(folded.T, axis=0, keepdims=True)
    even = lax.bitwise_and(iota((8, 128), 0), 1) == 0
    for s in range(0, total, 128):
        pair = jnp.where(even, best[:, s : s + 128], hist)
        for at in range(s // 16, out_ref.shape[0], total // 16):
            out_ref[at : at + 8, :] = pair


def pick_results(where_ref, index_ref, got_ref, best_ref, hist_ref):
    owners = got_ref.shape[0] // 2
    docs = index_ref.shape[1]
    quarter = where_ref[1]
    index = index_ref[...]
    owner = lax.shift_right_logical(index, 5)
    lane = quarter * 32 + lax.bitwise_and(index, 31)
    onehot = ones_where(iota((owners, docs), 0) == owner)
    values = got_ref[pl.ds(0, owners, stride=2), :].T
    high = values.astype(BF16)
    rest = values - high.astype(F32)
    middle = rest.astype(BF16)
    low = (rest - middle.astype(F32)).astype(BF16)
    picked = dot(high, onehot) + dot(middle, onehot) + dot(low, onehot)
    picked = jnp.where(iota((128, docs), 0) == lane, picked, 0.0)
    best_ref[...] = jnp.sum(picked, axis=0, keepdims=True)
    hist = jnp.sum(got_ref[pl.ds(1, owners, stride=2), :], axis=0, keepdims=True)
    hist_ref[...] = hist * (1.0 / (owners * docs))


VMEM = pl.BlockSpec(memory_space=pltpu.VMEM)
SMEM = pl.BlockSpec(memory_space=pltpu.SMEM)


def call(kernel, outs, specs, flops):
    many = isinstance(outs, tuple)
    return pl.pallas_call(
        kernel,
        out_shape=outs,
        in_specs=specs,
        out_specs=tuple(VMEM for _ in outs) if many else VMEM,
        compiler_params=pltpu.CompilerParams(vmem_limit_bytes=24 * 2**20),
        cost_estimate=pl.CostEstimate(flops=flops, bytes_accessed=4000000, transcendentals=0),
    )


def shape(dims, dtype):
    return jax.ShapeDtypeStruct(dims, dtype)


def exchange(x, axes):
    return lax.all_to_all(x, axes, split_axis=0, concat_axis=0, tiled=True)


def shards(embeddings, document_cluster_index):
    row_count = lax.axis_size(ROWS)
    col_count = lax.axis_size(COLS)
    docs, width = embeddings.shape
    labels = document_cluster_index.reshape(1, docs)
    col = lax.axis_index(COLS)
    where = jnp.stack([lax.axis_index(ROWS), col % 4]).astype(jnp.int32)
    block = CAP + META
    sends, rank = call(
        normalise_and_slot,
        (shape((row_count, block, width), BF16), shape((1, docs), F32)),
        [VMEM, VMEM],
        2 * row_count * CAP * docs * width,
    )(labels, embeddings)
    got = exchange(sends, ROWS)
    total = GROUP_CLUSTERS * CAP
    sends = call(
        reslot, shape((total, width), BF16), [SMEM, VMEM], 2 * total * row_count * CAP * width
    )(where, got)
    index = call(return_index, shape((1, docs), jnp.int32), [SMEM, VMEM, VMEM, VMEM], 2**26)(
        where, labels, rank, got
    )
    own = exchange(sends.reshape(col_count, total // col_count, width), COLS)
    own = own.reshape(total, width)
    other = lax.ppermute(own, COLS, [(i, i ^ 1) for i in range(col_count)])
    flops = 2 * total * total * width
    first = call(best_own, shape((1, total), F32), [VMEM], flops)(own)
    results = call(
        best_all, shape((row_count * col_count * 2, 128), F32), [VMEM, VMEM, VMEM], flops
    )(own, other, first)
    results = exchange(results.reshape(row_count * col_count, 2, 128), ALL)
    results = results.reshape(row_count * col_count * 2, 128)
    best, hist = call(
        pick_results, (shape((1, docs), F32), shape((1, BINS), F32)), [SMEM, VMEM, VMEM], 2**26
    )(where, index, results)
    return (best.reshape(docs), hist.reshape(BINS))


def solution(mesh):
    torus = Mesh(
        mesh.devices.reshape(2, 4, 2, 8, 2), ("rows_0", "rows_1", "cols_0", "cols_1", "cols_2")
    )
    in_specs = (P(ALL, None), P(ALL))
    out_specs = (P(ALL), P())
    return jax.shard_map(
        shards, mesh=torus, in_specs=in_specs, out_specs=out_specs, check_vma=False
    )
```

```python
import jax
import jax.numpy as jnp
from jax import lax
from jax.experimental import pallas as pl
from jax.experimental.pallas import tpu as pltpu
from jax.sharding import Mesh
from jax.sharding import PartitionSpec as P

CAP = 64
GROUP_CLUSTERS = 16
BINS = 128
ROWS = ("rows_0", "rows_1")
COLS = ("cols_0", "cols_1", "cols_2")
ALL = ROWS + COLS
LANES = 128
EMPTY = 2.0
F32 = jnp.float32
BF16 = jnp.bfloat16


def iota(shape, dim):
    return lax.broadcasted_iota(jnp.int32, shape, dim)


def dot(a, b):
    return lax.dot_general(a, b, (((1,), (0,)), ((), ())), preferred_element_type=F32)


def dot_t(a, b):
    return lax.dot_general(a, b, (((1,), (1,)), ((), ())), preferred_element_type=F32)


def ones_where(mask):
    return jnp.where(mask, 1.0, 0.0).astype(BF16)


def before(n):
    return ones_where(iota((n, n), 0) < iota((n, n), 1))


def rank_of(onehot, n):
    earlier = dot(onehot, before(n))
    return jnp.sum(onehot.astype(F32) * earlier, axis=0, keepdims=True)


def normalise_and_slot(labels_hbm, embeddings_hbm, out_ref, rank_ref, labels_ref, embeddings_ref, sems):
    labels_copy = pltpu.make_async_copy(labels_hbm, labels_ref, sems.at[0])
    embeddings_copy = pltpu.make_async_copy(embeddings_hbm, embeddings_ref, sems.at[1])
    labels_copy.start()
    embeddings_copy.start()
    docs, width = embeddings_ref.shape
    groups = out_ref.shape[0]
    clusters = groups * GROUP_CLUSTERS
    labels_copy.wait()
    labels = labels_ref[...]
    group = lax.shift_right_logical(labels, 4)
    onehot = ones_where(iota((groups, docs), 0) == group)
    slot = group * CAP + rank_of(onehot, docs).astype(jnp.int32)
    places = ones_where(iota((groups * CAP, docs), 0) == slot)
    shifted = jnp.broadcast_to((labels + 1).astype(F32), (8, docs)).astype(BF16)
    slot_labels = dot_t(shifted, places)
    of_cluster = ones_where(iota((clusters, docs), 0) == labels)
    counts = dot_t(jnp.ones((8, docs), BF16), of_cluster)
    row = iota((8, LANES), 0)
    meta = jnp.where(row == groups * CAP // LANES, counts, 0.0)
    for s in range(groups * CAP // LANES):
        meta = jnp.where(row == s, slot_labels[:, s * LANES : (s + 1) * LANES], meta)
    meta = meta.astype(BF16)
    rank_ref[...] = rank_of(of_cluster, docs)
    embeddings_copy.wait()
    values = embeddings_ref[...].astype(F32)
    total = jnp.sum(values * values, axis=1, keepdims=True)
    normed = (values * lax.rsqrt(total + 1e-06)).astype(BF16)
    rows = dot(places, normed).astype(BF16)
    pieces = width // LANES
    for g in range(groups):
        for f in range(pieces):
            block = rows[g * CAP : (g + 1) * CAP, f * LANES : (f + 1) * LANES]
            out_ref[g, f * CAP : (f + 1) * CAP, :] = block
        out_ref[g, pieces * CAP :, :] = meta


def slot_labels_of(got_ref, me):
    groups = got_ref.shape[0]
    slots = groups * CAP
    at = got_ref.shape[1] - 8
    source = lax.shift_right_logical(iota((8, slots), 1), 6)
    row = iota((8, LANES), 0)
    per_row = LANES // CAP
    picked = []
    for g in range(groups):
        meta = got_ref[g, at:, :].astype(F32)
        line = jnp.where(row == lax.shift_right_logical(me, 1), meta, 0.0)
        picked.append(jnp.sum(line, axis=0, keepdims=True))
    lines = jnp.concatenate(picked, axis=0).astype(BF16)
    lane, to = iota((LANES, slots), 0), iota((LANES, slots), 1)
    start = lax.bitwise_and(me, per_row - 1) * CAP
    move = ones_where(lane == start + lax.bitwise_and(to, CAP - 1))
    spread = jnp.where(iota((groups, slots), 0) == source, dot(lines, move), 0.0)
    return jnp.sum(spread, axis=0, keepdims=True)


def reslot(got_ref, out_ref):
    groups = got_ref.shape[0]
    slots = groups * CAP
    width = out_ref.shape[1]
    me = lax.axis_index(ROWS)
    label = slot_labels_of(got_ref, me).astype(jnp.int32)
    cluster = label - 1 - me * GROUP_CLUSTERS
    onehot = ones_where(iota((GROUP_CLUSTERS, slots), 0) == cluster)
    place = cluster * CAP + rank_of(onehot, slots).astype(jnp.int32)
    place = jnp.where(label > 0, place, -1)
    total = GROUP_CLUSTERS * CAP
    step = total // 4
    pieces = width // LANES
    rows = jnp.concatenate(
        [got_ref[:, f * CAP : (f + 1) * CAP, :].reshape(slots, LANES) for f in range(pieces)],
        axis=1,
    )
    for s in range(0, total, step):
        places = jnp.where(iota((step, slots), 0) + s == place, 1.0, 0.0)
        filled = jnp.sum(places, axis=1, keepdims=True) > 0.5
        moved = dot(places.astype(BF16), rows)
        out_ref[s : s + step, LANES:] = moved[:, LANES:].astype(BF16)
        first = moved[:, 0:LANES]
        first = jnp.where((iota(first.shape, 1) == 0) & ~filled, EMPTY, first)
        out_ref[s : s + step, 0:LANES] = first.astype(BF16)


def return_index(labels_ref, rank_ref, got_ref, out_ref):
    groups = got_ref.shape[0]
    docs = labels_ref.shape[1]
    clusters = groups * GROUP_CLUSTERS
    me = lax.axis_index(ROWS)
    at = got_ref.shape[1] - 8
    row = iota((8, LANES), 0)
    before_me = jnp.zeros((8, LANES), F32)
    for g in range(groups):
        before_me = before_me + jnp.where(g < me, got_ref[g, at:, :].astype(F32), 0.0)
    counts = jnp.where(row == groups * CAP // LANES, before_me, 0.0)
    labels = labels_ref[...]
    of_cluster = ones_where(iota((clusters, docs), 0) == labels)
    earlier = jnp.sum(dot(counts.astype(BF16), of_cluster), axis=0, keepdims=True)
    out_ref[...] = labels * CAP + (rank_ref[...] + earlier).astype(jnp.int32)


def best_against(own_ref, other_ref, same):
    block = 256
    out = []
    for j in range(0, own_ref.shape[0], block):
        mine = own_ref[j : j + block, :]
        best = jnp.full((8, block), -1.0, F32)
        for i in range(0, other_ref.shape[0], block):
            theirs = other_ref[i : i + block, :]
            scores = dot_t(theirs, mine)
            keep = theirs[:, 0:1].astype(F32) < 1.5
            if same and i == j:
                keep = keep & (iota((block, block), 0) != iota((block, block), 1))
            scores = jnp.where(keep, scores, -1.0)
            best = jnp.maximum(best, jnp.max(scores.reshape(block // 8, 8, block), axis=0))
        out.append(best)
    return jnp.concatenate(out, axis=1)


def best_own(own_ref, out_ref):
    out_ref[...] = best_against(own_ref, own_ref, True)


def best_more(own_ref, other_ref, so_far_ref, out_ref):
    out_ref[...] = jnp.maximum(best_against(own_ref, other_ref, False), so_far_ref[...])


def three_parts(x):
    high = x.astype(BF16).astype(F32)
    middle = (x - high).astype(BF16).astype(F32)
    return high, middle, x - high - middle


def best_last(own_ref, other_ref, so_far_ref, out_ref):
    total = own_ref.shape[0]
    best = jnp.maximum(best_against(own_ref, other_ref, False), so_far_ref[...])
    best = jnp.max(best, axis=0, keepdims=True)
    pick = ones_where(iota((8, 256), 1) == 0)
    flag = dot_t(pick, own_ref[:, 0:256])[0:1, :]
    width = 2.0 / (BINS - 1)
    centers = -1.0 + iota((BINS, 1), 0).astype(F32) * width
    weights = jnp.maximum(1.0 - jnp.abs(best - centers) / width, 0.0)
    weights = jnp.where(flag < 1.5, weights, 0.0)
    folded = weights[:, 0:LANES]
    for s in range(LANES, total, LANES):
        folded = folded + weights[:, s : s + LANES]
    hist = jnp.sum(folded.T, axis=0, keepdims=True)
    lines = jnp.concatenate([best[:, s : s + LANES] for s in range(0, total, LANES)], axis=0)
    parts = three_parts(lines)
    lane = iota((8, LANES), 1)
    sub = iota((8, LANES), 0)
    quarters = []
    for q in range(4):
        line = jnp.zeros((8, LANES), F32)
        for p in range(3):
            shift = (32 * (p - q)) % LANES
            moved = pltpu.roll(parts[p], shift, 1) if shift else parts[p]
            line = jnp.where(lax.shift_right_logical(lane, 5) == p, moved, line)
        quarters.append(line)
    blocks = []
    for s in range(total // LANES):
        block = jnp.broadcast_to(hist, (8, LANES))
        for q in range(4):
            block = jnp.where(sub == 2 * q + 1, quarters[q][s : s + 1, :], block)
        blocks.append(block)
    block = jnp.concatenate(blocks, axis=0).astype(BF16)
    for at in range(0, out_ref.shape[0], block.shape[0]):
        out_ref[at : at + block.shape[0], :] = block


def pick_results(index_ref, got_ref, best_ref, hist_ref):
    lines = got_ref.shape[0]
    docs = index_ref.shape[1]
    index = index_ref[...]
    line = lax.shift_right_logical(index, 5) * 2 + 1
    depth = lax.bitwise_and(index, 31)
    onehot = ones_where(iota((lines, docs), 0) == line)
    got = got_ref[...]
    picked = dot(got.astype(F32).T.astype(BF16), onehot)
    lane = iota((LANES, docs), 0)
    wanted = (lax.bitwise_and(lane, 31) == depth) & (lane < 96)
    best_ref[...] = jnp.sum(jnp.where(wanted, picked, 0.0), axis=0, keepdims=True)
    even = ones_where(lax.bitwise_and(iota((8, lines), 1), 1) == 0)
    hist = dot(even, got)[0:1, :]
    hist_ref[...] = hist * (1.0 / (lines // 2 * docs))


VMEM = pl.BlockSpec(memory_space=pltpu.VMEM)
ANY = pl.BlockSpec(memory_space=pl.ANY)


def call(kernel, outs, specs, flops, scratch=()):
    many = isinstance(outs, tuple)
    return pl.pallas_call(
        kernel,
        out_shape=outs,
        in_specs=specs,
        out_specs=tuple(VMEM for _ in outs) if many else VMEM,
        scratch_shapes=scratch,
        compiler_params=pltpu.CompilerParams(vmem_limit_bytes=24 * 2**20),
        cost_estimate=pl.CostEstimate(flops=flops, bytes_accessed=4000000, transcendentals=0),
    )


def shape(dims, dtype):
    return jax.ShapeDtypeStruct(dims, dtype)


def exchange(x, axes):
    return lax.all_to_all(x, axes, split_axis=0, concat_axis=0, tiled=True)


def shards(embeddings, document_cluster_index):
    row_count = lax.axis_size(ROWS)
    col_count = lax.axis_size(COLS)
    docs, width = embeddings.shape
    labels = document_cluster_index.reshape(1, docs)
    block = CAP * width // LANES + 8
    sends, rank = call(
        normalise_and_slot,
        (shape((row_count, block, LANES), BF16), shape((1, docs), F32)),
        [ANY, ANY],
        2 * row_count * CAP * docs * width,
        [
            pltpu.VMEM((1, docs), jnp.int32),
            pltpu.VMEM((docs, width), BF16),
            pltpu.SemaphoreType.DMA((2,)),
        ],
    )(labels, embeddings)
    got = exchange(sends, ROWS)
    total = GROUP_CLUSTERS * CAP
    sends = call(reslot, shape((total, width), BF16), [VMEM], 2 * total * row_count * CAP * width)(
        got
    )
    own = exchange(sends.reshape(col_count, total // col_count, width), COLS)
    own, got = lax.optimization_barrier((own.reshape(total, width), got))
    pairs = [(i, i ^ 1) for i in range(col_count)]
    half = total // 2
    other = [lax.ppermute(own[s : s + half], COLS, pairs) for s in (0, half)]
    flops = 2 * total * half * width
    best = call(best_own, shape((8, total), F32), [VMEM], 2 * flops)(own)
    best = call(best_more, shape((8, total), F32), [VMEM] * 3, flops)(own, other[0], best)
    index = call(return_index, shape((1, docs), jnp.int32), [VMEM] * 3, 2**26)(labels, rank, got)
    results = call(best_last, shape((row_count * col_count * 2, LANES), BF16), [VMEM] * 3, flops)(
        own, other[1], best
    )
    results, index = lax.optimization_barrier((results, index))
    results = exchange(results.reshape(row_count * col_count, 2, LANES), ALL)
    results = results.reshape(row_count * col_count * 2, LANES)
    best, hist = call(
        pick_results, (shape((1, docs), F32), shape((1, BINS), F32)), [VMEM, VMEM], 2**26
    )(index, results)
    return (best.reshape(docs), hist.reshape(BINS))


def solution(mesh):
    torus = Mesh(
        mesh.devices.reshape(2, 4, 2, 8, 2), ("rows_0", "rows_1", "cols_0", "cols_1", "cols_2")
    )
    in_specs = (P(ALL, None), P(ALL))
    out_specs = (P(ALL), P())
    return jax.shard_map(
        shards, mesh=torus, in_specs=in_specs, out_specs=out_specs, check_vma=False
    )
```

```python
import jax
import jax.numpy as jnp
from jax import lax
from jax.experimental import pallas as pl
from jax.experimental.pallas import tpu as pltpu
from jax.sharding import Mesh
from jax.sharding import PartitionSpec as P

CAP = 64
GROUP_CLUSTERS = 16
BINS = 128
ROWS = ("rows_0", "rows_1")
COLS = ("cols_0", "cols_1", "cols_2")
CHIPS = ("cols_0", "cols_1")
ALL = ROWS + COLS
SAME_CORE = ROWS + CHIPS
LANES = 128
EMPTY = 2.0
F32 = jnp.float32
BF16 = jnp.bfloat16


def iota(shape, dim):
    return lax.broadcasted_iota(jnp.int32, shape, dim)


def dot(a, b):
    return lax.dot_general(a, b, (((1,), (0,)), ((), ())), preferred_element_type=F32)


def dot_t(a, b):
    return lax.dot_general(a, b, (((1,), (1,)), ((), ())), preferred_element_type=F32)


def ones_where(mask):
    return jnp.where(mask, 1.0, 0.0).astype(BF16)


def before(n):
    return ones_where(iota((n, n), 0) < iota((n, n), 1))


def rank_of(onehot, n):
    earlier = dot(onehot, before(n))
    return jnp.sum(onehot.astype(F32) * earlier, axis=0, keepdims=True)


def normalise_and_slot(labels_hbm, embeddings_hbm, out_ref, rank_ref, labels_ref, embeddings_ref, sems):
    labels_copy = pltpu.make_async_copy(labels_hbm, labels_ref, sems.at[0])
    embeddings_copy = pltpu.make_async_copy(embeddings_hbm, embeddings_ref, sems.at[1])
    labels_copy.start()
    embeddings_copy.start()
    docs, width = embeddings_ref.shape
    groups = out_ref.shape[0]
    clusters = groups * GROUP_CLUSTERS
    labels_copy.wait()
    labels = labels_ref[...]
    group = lax.shift_right_logical(labels, 4)
    onehot = ones_where(iota((groups, docs), 0) == group)
    slot = group * CAP + rank_of(onehot, docs).astype(jnp.int32)
    places = ones_where(iota((groups * CAP, docs), 0) == slot)
    shifted = jnp.broadcast_to((labels + 1).astype(F32), (8, docs)).astype(BF16)
    slot_labels = dot_t(shifted, places)
    of_cluster = ones_where(iota((clusters, docs), 0) == labels)
    counts = dot_t(jnp.ones((8, docs), BF16), of_cluster)
    row = iota((8, LANES), 0)
    meta = jnp.where(row == groups * CAP // LANES, counts, 0.0)
    for s in range(groups * CAP // LANES):
        meta = jnp.where(row == s, slot_labels[:, s * LANES : (s + 1) * LANES], meta)
    meta = meta.astype(BF16)
    rank_ref[...] = rank_of(of_cluster, docs)
    embeddings_copy.wait()
    values = embeddings_ref[...].astype(F32)
    total = jnp.sum(values * values, axis=1, keepdims=True)
    normed = (values * lax.rsqrt(total + 1e-06)).astype(BF16)
    rows = dot(places, normed).astype(BF16)
    pieces = width // LANES
    for g in range(groups):
        for f in range(pieces):
            block = rows[g * CAP : (g + 1) * CAP, f * LANES : (f + 1) * LANES]
            out_ref[g, f * CAP : (f + 1) * CAP, :] = block
        out_ref[g, pieces * CAP :, :] = meta


def slot_labels_of(got_ref, me):
    groups = got_ref.shape[0]
    slots = groups * CAP
    at = got_ref.shape[1] - 8
    source = lax.shift_right_logical(iota((8, slots), 1), 6)
    row = iota((8, LANES), 0)
    per_row = LANES // CAP
    picked = []
    for g in range(groups):
        meta = got_ref[g, at:, :].astype(F32)
        line = jnp.where(row == lax.shift_right_logical(me, 1), meta, 0.0)
        picked.append(jnp.sum(line, axis=0, keepdims=True))
    lines = jnp.concatenate(picked, axis=0).astype(BF16)
    lane, to = iota((LANES, slots), 0), iota((LANES, slots), 1)
    start = lax.bitwise_and(me, per_row - 1) * CAP
    move = ones_where(lane == start + lax.bitwise_and(to, CAP - 1))
    spread = jnp.where(iota((groups, slots), 0) == source, dot(lines, move), 0.0)
    return jnp.sum(spread, axis=0, keepdims=True)


def reslot(got_ref, out_ref):
    groups = got_ref.shape[0]
    slots = groups * CAP
    width = out_ref.shape[1]
    me = lax.axis_index(ROWS)
    label = slot_labels_of(got_ref, me).astype(jnp.int32)
    cluster = label - 1 - me * GROUP_CLUSTERS
    onehot = ones_where(iota((GROUP_CLUSTERS, slots), 0) == cluster)
    place = cluster * CAP + rank_of(onehot, slots).astype(jnp.int32)
    place = jnp.where(label > 0, place, -1)
    total = GROUP_CLUSTERS * CAP
    step = total // 4
    pieces = width // LANES
    rows = jnp.concatenate(
        [got_ref[:, f * CAP : (f + 1) * CAP, :].reshape(slots, LANES) for f in range(pieces)],
        axis=1,
    )
    for s in range(0, total, step):
        places = jnp.where(iota((step, slots), 0) + s == place, 1.0, 0.0)
        filled = jnp.sum(places, axis=1, keepdims=True) > 0.5
        moved = dot(places.astype(BF16), rows)
        out_ref[s : s + step, LANES:] = moved[:, LANES:].astype(BF16)
        first = moved[:, 0:LANES]
        first = jnp.where((iota(first.shape, 1) == 0) & ~filled, EMPTY, first)
        out_ref[s : s + step, 0:LANES] = first.astype(BF16)


def return_index(labels_ref, rank_ref, got_ref, out_ref):
    groups = got_ref.shape[0]
    docs = labels_ref.shape[1]
    clusters = groups * GROUP_CLUSTERS
    me = lax.axis_index(ROWS)
    at = got_ref.shape[1] - 8
    row = iota((8, LANES), 0)
    before_me = jnp.zeros((8, LANES), F32)
    for g in range(groups):
        before_me = before_me + jnp.where(g < me, got_ref[g, at:, :].astype(F32), 0.0)
    counts = jnp.where(row == groups * CAP // LANES, before_me, 0.0)
    labels = labels_ref[...]
    of_cluster = ones_where(iota((clusters, docs), 0) == labels)
    earlier = jnp.sum(dot(counts.astype(BF16), of_cluster), axis=0, keepdims=True)
    out_ref[...] = labels * CAP + (rank_ref[...] + earlier).astype(jnp.int32)


def best_against(own_ref, other_ref, same):
    block = 256
    out = []
    for j in range(0, own_ref.shape[0], block):
        mine = own_ref[j : j + block, :]
        best = jnp.full((8, block), -1.0, F32)
        for i in range(0, other_ref.shape[0], block):
            theirs = other_ref[i : i + block, :]
            scores = dot_t(theirs, mine)
            keep = theirs[:, 0:1].astype(F32) < 1.5
            if same and i == j:
                keep = keep & (iota((block, block), 0) != iota((block, block), 1))
            scores = jnp.where(keep, scores, -1.0)
            best = jnp.maximum(best, jnp.max(scores.reshape(block // 8, 8, block), axis=0))
        out.append(best)
    return jnp.concatenate(out, axis=1)


def best_own(own_ref, out_ref):
    out_ref[...] = best_against(own_ref, own_ref, True)


def best_more(own_ref, other_ref, so_far_ref, out_ref):
    out_ref[...] = jnp.maximum(best_against(own_ref, other_ref, False), so_far_ref[...])


def best_last(own_ref, other_ref, so_far_ref, out_ref):
    total = own_ref.shape[0]
    best = jnp.maximum(best_against(own_ref, other_ref, False), so_far_ref[...])
    best = jnp.max(best, axis=0, keepdims=True)
    pick = ones_where(iota((8, 256), 1) == 0)
    flag = dot_t(pick, own_ref[:, 0:256])[0:1, :]
    width = 2.0 / (BINS - 1)
    centers = -1.0 + iota((BINS, 1), 0).astype(F32) * width
    weights = jnp.maximum(1.0 - jnp.abs(best - centers) / width, 0.0)
    weights = jnp.where(flag < 1.5, weights, 0.0)
    folded = weights[:, 0:LANES]
    for s in range(LANES, total, LANES):
        folded = folded + weights[:, s : s + LANES]
    hist = jnp.sum(folded.T, axis=0, keepdims=True)
    high = best.astype(BF16).astype(F32)
    low = best - high
    sub = iota((8, LANES), 0)
    left = iota((1, LANES), 1) < CAP
    blocks = []
    for s in range(0, total, 2 * LANES):
        block = jnp.broadcast_to(hist, (8, LANES))
        for h in range(2):
            at = s + h * LANES
            top, rest = high[:, at : at + LANES], low[:, at : at + LANES]
            first = jnp.where(left, top, pltpu.roll(rest, CAP, 1))
            second = jnp.where(left, pltpu.roll(top, CAP, 1), rest)
            block = jnp.where(sub == 4 * h + 1, first, block)
            block = jnp.where(sub == 4 * h + 3, second, block)
        blocks.append(block)
    block = jnp.concatenate(blocks, axis=0).astype(BF16)
    for at in range(0, out_ref.shape[0], block.shape[0]):
        out_ref[at : at + block.shape[0], :] = block


def sum_histograms(got_ref, hist_ref):
    lines = got_ref.shape[0]
    even = ones_where(lax.bitwise_and(iota((8, lines), 1), 1) == 0)
    hist_ref[...] = dot(even, got_ref[...])[0:1, :]


def pick_results(index_ref, got_ref, best_ref):
    lines = got_ref.shape[0]
    docs = index_ref.shape[1]
    index = index_ref[...]
    line = lax.shift_right_logical(index, 6) * 2 + 1
    rank = lax.bitwise_and(index, CAP - 1)
    onehot = ones_where(iota((lines, docs), 0) == line)
    picked = dot(got_ref[...].astype(F32).T.astype(BF16), onehot)
    wanted = lax.bitwise_and(iota((LANES, docs), 0), CAP - 1) == rank
    best_ref[...] = jnp.sum(jnp.where(wanted, picked, 0.0), axis=0, keepdims=True)


VMEM = pl.BlockSpec(memory_space=pltpu.VMEM)
ANY = pl.BlockSpec(memory_space=pl.ANY)


def call(kernel, outs, specs, flops, scratch=()):
    many = isinstance(outs, tuple)
    return pl.pallas_call(
        kernel,
        out_shape=outs,
        in_specs=specs,
        out_specs=tuple(VMEM for _ in outs) if many else VMEM,
        scratch_shapes=scratch,
        compiler_params=pltpu.CompilerParams(vmem_limit_bytes=24 * 2**20),
        cost_estimate=pl.CostEstimate(flops=flops, bytes_accessed=4000000, transcendentals=0),
    )


def shape(dims, dtype):
    return jax.ShapeDtypeStruct(dims, dtype)


def in_hbm(x):
    return pltpu.with_memory_space_constraint(x, pltpu.HBM)


def exchange(x, axes):
    return lax.all_to_all(x, axes, split_axis=0, concat_axis=0, tiled=True)


def shards(embeddings, document_cluster_index):
    row_count = lax.axis_size(ROWS)
    col_count = lax.axis_size(COLS)
    docs, width = embeddings.shape
    labels = document_cluster_index.reshape(1, docs)
    block = CAP * width // LANES + 8
    sends, rank = call(
        normalise_and_slot,
        (shape((row_count, block, LANES), BF16), shape((1, docs), F32)),
        [ANY, ANY],
        2 * row_count * CAP * docs * width,
        [
            pltpu.VMEM((1, docs), jnp.int32),
            pltpu.VMEM((docs, width), BF16),
            pltpu.SemaphoreType.DMA((2,)),
        ],
    )(in_hbm(labels), in_hbm(embeddings))
    got = exchange(sends, ROWS)
    total = GROUP_CLUSTERS * CAP
    sends = call(reslot, shape((total, width), BF16), [VMEM], 2 * total * row_count * CAP * width)(
        got
    )
    own = exchange(sends.reshape(GROUP_CLUSTERS, CAP, width), CHIPS)
    own, got = lax.optimization_barrier((own.reshape(total, width), got))
    pairs = [(i, i ^ 1) for i in range(col_count)]
    half = total // 2
    other = [lax.ppermute(own[s : s + half], COLS, pairs) for s in (0, half)]
    flops = 2 * total * half * width
    lines = row_count * GROUP_CLUSTERS * 2
    best = call(best_own, shape((8, total), F32), [VMEM], 2 * flops)(own)
    best = call(best_more, shape((8, total), F32), [VMEM] * 3, flops)(own, other[0], best)
    index = call(return_index, shape((1, docs), jnp.int32), [VMEM] * 3, 2**26)(labels, rank, got)
    results = call(best_last, shape((lines, LANES), BF16), [VMEM] * 3, flops)(
        own, other[1], best
    )
    results, index = lax.optimization_barrier((results, index))
    results = exchange(results.reshape(lines // 2, 2, LANES), SAME_CORE).reshape(lines, LANES)
    hist = call(sum_histograms, shape((1, BINS), F32), [VMEM], 2**24)(results)
    hist = (hist + lax.ppermute(hist, COLS, pairs)) / (docs * row_count * col_count)
    best = call(pick_results, shape((1, docs), F32), [VMEM, VMEM], 2**26)(index, results)
    return (best.reshape(docs), hist.reshape(BINS))


def solution(mesh):
    torus = Mesh(
        mesh.devices.reshape(2, 4, 2, 8, 2), ("rows_0", "rows_1", "cols_0", "cols_1", "cols_2")
    )
    in_specs = (P(ALL, None), P(ALL))
    out_specs = (P(ALL), P())
    return jax.shard_map(
        shards, mesh=torus, in_specs=in_specs, out_specs=out_specs, check_vma=False
    )
```

```python
import jax
import jax.numpy as jnp
from jax import lax
from jax.experimental import pallas as pl
from jax.experimental.pallas import tpu as pltpu
from jax.sharding import Mesh
from jax.sharding import PartitionSpec as P

CAP = 64
GROUP_CLUSTERS = 16
BINS = 128
ROWS = ("rows_0", "rows_1")
COLS = ("cols_0", "cols_1", "cols_2")
CHIPS = ("cols_0", "cols_1")
ALL = ROWS + COLS
SAME_CORE = ROWS + CHIPS
LANES = 128
BLOCK = 256
EMPTY = 2.0
F32 = jnp.float32
BF16 = jnp.bfloat16


def iota(shape, dim):
    return lax.broadcasted_iota(jnp.int32, shape, dim)


def dot(a, b):
    return lax.dot_general(a, b, (((1,), (0,)), ((), ())), preferred_element_type=F32)


def dot_t(a, b):
    return lax.dot_general(a, b, (((1,), (1,)), ((), ())), preferred_element_type=F32)


def ones_where(mask):
    return jnp.where(mask, 1.0, 0.0).astype(BF16)


def before(n):
    return ones_where(iota((n, n), 0) < iota((n, n), 1))


def rank_of(onehot, n):
    earlier = dot(onehot, before(n))
    return jnp.sum(onehot.astype(F32) * earlier, axis=0, keepdims=True)


def normalise_and_slot(labels_hbm, embeddings_hbm, out_ref, rank_ref, labels_ref, embeddings_ref, sems):
    labels_copy = pltpu.make_async_copy(labels_hbm, labels_ref, sems.at[0])
    embeddings_copy = pltpu.make_async_copy(embeddings_hbm, embeddings_ref, sems.at[1])
    labels_copy.start()
    embeddings_copy.start()
    docs, width = embeddings_ref.shape
    groups = out_ref.shape[0]
    clusters = groups * GROUP_CLUSTERS
    labels_copy.wait()
    labels = labels_ref[...]
    group = lax.shift_right_logical(labels, 4)
    onehot = ones_where(iota((groups, docs), 0) == group)
    slot = group * CAP + rank_of(onehot, docs).astype(jnp.int32)
    places = ones_where(iota((groups * CAP, docs), 0) == slot)
    shifted = jnp.broadcast_to((labels + 1).astype(F32), (8, docs)).astype(BF16)
    slot_labels = dot_t(shifted, places)
    of_cluster = ones_where(iota((clusters, docs), 0) == labels)
    counts = dot_t(jnp.ones((8, docs), BF16), of_cluster)
    row = iota((8, LANES), 0)
    meta = jnp.where(row == groups * CAP // LANES, counts, 0.0)
    for s in range(groups * CAP // LANES):
        meta = jnp.where(row == s, slot_labels[:, s * LANES : (s + 1) * LANES], meta)
    meta = meta.astype(BF16)
    rank_ref[...] = rank_of(of_cluster, docs)
    embeddings_copy.wait()
    values = embeddings_ref[...].astype(F32)
    total = jnp.sum(values * values, axis=1, keepdims=True)
    normed = (values * lax.rsqrt(total + 1e-06)).astype(BF16)
    rows = dot(places, normed).astype(BF16)
    pieces = width // LANES
    for g in range(groups):
        for f in range(pieces):
            block = rows[g * CAP : (g + 1) * CAP, f * LANES : (f + 1) * LANES]
            out_ref[g, f * CAP : (f + 1) * CAP, :] = block
        out_ref[g, pieces * CAP :, :] = meta


def slot_labels_of(got_ref, me):
    groups = got_ref.shape[0]
    slots = groups * CAP
    at = got_ref.shape[1] - 8
    source = lax.shift_right_logical(iota((8, slots), 1), 6)
    row = iota((8, LANES), 0)
    per_row = LANES // CAP
    picked = []
    for g in range(groups):
        meta = got_ref[g, at:, :].astype(F32)
        line = jnp.where(row == lax.shift_right_logical(me, 1), meta, 0.0)
        picked.append(jnp.sum(line, axis=0, keepdims=True))
    lines = jnp.concatenate(picked, axis=0).astype(BF16)
    lane, to = iota((LANES, slots), 0), iota((LANES, slots), 1)
    start = lax.bitwise_and(me, per_row - 1) * CAP
    move = ones_where(lane == start + lax.bitwise_and(to, CAP - 1))
    spread = jnp.where(iota((groups, slots), 0) == source, dot(lines, move), 0.0)
    return jnp.sum(spread, axis=0, keepdims=True)


def reslot(got_ref, out_ref):
    groups = got_ref.shape[0]
    slots = groups * CAP
    width = out_ref.shape[1]
    me = lax.axis_index(ROWS)
    label = slot_labels_of(got_ref, me).astype(jnp.int32)
    cluster = label - 1 - me * GROUP_CLUSTERS
    onehot = ones_where(iota((GROUP_CLUSTERS, slots), 0) == cluster)
    place = cluster * CAP + rank_of(onehot, slots).astype(jnp.int32)
    place = jnp.where(label > 0, place, -1)
    total = GROUP_CLUSTERS * CAP
    step = total // 4
    pieces = width // LANES
    rows = jnp.concatenate(
        [got_ref[:, f * CAP : (f + 1) * CAP, :].reshape(slots, LANES) for f in range(pieces)],
        axis=1,
    )
    for s in range(0, total, step):
        places = jnp.where(iota((step, slots), 0) + s == place, 1.0, 0.0)
        filled = jnp.sum(places, axis=1, keepdims=True) > 0.5
        moved = dot(places.astype(BF16), rows)
        out_ref[s : s + step, LANES:] = moved[:, LANES:].astype(BF16)
        first = moved[:, 0:LANES]
        first = jnp.where((iota(first.shape, 1) == 0) & ~filled, EMPTY, first)
        out_ref[s : s + step, 0:LANES] = first.astype(BF16)


def return_index(labels_ref, rank_ref, got_ref, out_ref):
    groups = got_ref.shape[0]
    docs = labels_ref.shape[1]
    clusters = groups * GROUP_CLUSTERS
    me = lax.axis_index(ROWS)
    at = got_ref.shape[1] - 8
    row = iota((8, LANES), 0)
    before_me = jnp.zeros((8, LANES), F32)
    for g in range(groups):
        before_me = before_me + jnp.where(g < me, got_ref[g, at:, :].astype(F32), 0.0)
    counts = jnp.where(row == groups * CAP // LANES, before_me, 0.0)
    labels = labels_ref[...]
    of_cluster = ones_where(iota((clusters, docs), 0) == labels)
    earlier = jnp.sum(dot(counts.astype(BF16), of_cluster), axis=0, keepdims=True)
    out_ref[...] = labels * CAP + (rank_ref[...] + earlier).astype(jnp.int32)


def penalties(ref):
    total, width = ref.shape
    column = jnp.where(ref[:, 0:1].astype(F32) < 1.5, 0.0, -4.0)
    pick = ones_where(iota((8, 256), 1) == 0)
    row = jnp.where(dot_t(pick, ref[:, 0:256])[0:1, :] < 1.5, 0.0, -4.0)
    return column, row


def over_columns(scores):
    return jnp.max(scores.reshape(BLOCK // 8, 8, BLOCK), axis=0)


def over_rows(scores):
    return jnp.maximum(scores[:, :LANES], scores[:, LANES:])


def as_line(columns, rows):
    out = []
    for column, row in zip(columns, rows):
        line = jnp.max(column, axis=0, keepdims=True)
        if row is not None:
            turned = [jnp.max(row[h : h + LANES].T, axis=0, keepdims=True) for h in (0, LANES)]
            line = jnp.maximum(line, jnp.concatenate(turned, axis=1))
        out.append(line)
    return jnp.concatenate(out, axis=1)


def larger(a, b):
    return b if a is None else jnp.maximum(a, b)


def within(ref, penalty, columns, rows):
    column, row = penalty
    count = ref.shape[0] // BLOCK
    for i in range(count):
        for j in range(i, count):
            at, to = i * BLOCK, j * BLOCK
            scores = dot_t(ref[at : at + BLOCK, :], ref[to : to + BLOCK, :])
            scores = scores + column[at : at + BLOCK] + row[:, to : to + BLOCK]
            if i == j:
                other = iota((BLOCK, BLOCK), 0) != iota((BLOCK, BLOCK), 1)
                scores = jnp.where(other, scores, -4.0)
            else:
                rows[i] = larger(rows[i], over_rows(scores))
            columns[j] = larger(columns[j], over_columns(scores))


def between(a_ref, a_penalty, b_ref, b_penalty, rows, columns):
    for i in range(a_ref.shape[0] // BLOCK):
        for j in range(b_ref.shape[0] // BLOCK):
            at, to = i * BLOCK, j * BLOCK
            scores = dot_t(a_ref[at : at + BLOCK, :], b_ref[to : to + BLOCK, :])
            scores = scores + a_penalty[0][at : at + BLOCK] + b_penalty[1][:, to : to + BLOCK]
            rows[i] = larger(rows[i], over_rows(scores))
            columns[j] = larger(columns[j], over_columns(scores))


def nothing(ref):
    return [None] * (ref.shape[0] // BLOCK)


def best_own(own_ref, best_ref):
    columns, rows = nothing(own_ref), nothing(own_ref)
    within(own_ref, penalties(own_ref), columns, rows)
    best_ref[...] = jnp.maximum(as_line(columns, rows), -1.0)


def best_more(own_ref, more_ref, so_far_ref, best_ref, best_more_ref):
    columns, rows, of_own = nothing(more_ref), nothing(more_ref), nothing(own_ref)
    penalty = penalties(more_ref)
    between(more_ref, penalty, own_ref, penalties(own_ref), rows, of_own)
    within(more_ref, penalty, columns, rows)
    best_more_ref[...] = as_line(columns, rows)
    best_ref[...] = jnp.maximum(as_line(of_own, nothing(own_ref)), so_far_ref[...])


def histogram_parts(best, penalty):
    width = 2.0 / (BINS - 1)
    centers = -1.0 + iota((BINS, 1), 0).astype(F32) * width
    weights = jnp.maximum(1.0 - jnp.abs(best - centers) / width, 0.0)
    weights = jnp.where(penalty < 0.0, 0.0, weights)
    folded = weights[:, 0:LANES]
    for s in range(LANES, best.shape[1], LANES):
        folded = folded + weights[:, s : s + LANES]
    return folded


def best_last(own_ref, more_ref, last_ref, so_far_ref, more_so_far_ref, out_ref):
    total = own_ref.shape[0]
    own_penalty, more_penalty = penalties(own_ref), penalties(more_ref)
    penalty = penalties(last_ref)
    columns, rows, of_own = nothing(last_ref), nothing(last_ref), nothing(own_ref)
    of_more = nothing(more_ref)
    between(more_ref, more_penalty, last_ref, penalty, of_more, columns)
    between(last_ref, penalty, own_ref, own_penalty, rows, of_own)
    within(last_ref, penalty, columns, rows)
    best = jnp.maximum(as_line(of_own, nothing(own_ref)), so_far_ref[...])
    more_line = [more_so_far_ref[:, s : s + BLOCK] for s in range(0, more_ref.shape[0], BLOCK)]
    more_best = jnp.maximum(as_line(more_line, of_more), -1.0)
    last_best = jnp.maximum(as_line(columns, rows), -1.0)
    mine = histogram_parts(best, own_penalty[1])
    theirs = histogram_parts(
        jnp.concatenate([more_best, last_best], axis=1),
        jnp.concatenate([more_penalty[1], penalty[1]], axis=1),
    )
    hist = jnp.sum((mine + theirs).T, axis=0, keepdims=True)
    high = best.astype(BF16).astype(F32)
    low = best - high
    sub = iota((8, LANES), 0)
    left = iota((1, LANES), 1) < CAP
    blocks = []
    for s in range(0, total, 2 * LANES):
        block = jnp.broadcast_to(hist, (8, LANES))
        for h in range(2):
            at = s + h * LANES
            top, rest = high[:, at : at + LANES], low[:, at : at + LANES]
            first = jnp.where(left, top, pltpu.roll(rest, CAP, 1))
            second = jnp.where(left, pltpu.roll(top, CAP, 1), rest)
            block = jnp.where(sub == 4 * h + 1, first, block)
            block = jnp.where(sub == 4 * h + 3, second, block)
        blocks.append(block)
    block = jnp.concatenate(blocks, axis=0).astype(BF16)
    for at in range(0, out_ref.shape[0], block.shape[0]):
        out_ref[at : at + block.shape[0], :] = block


def pick_results(index_ref, got_ref, best_ref, hist_ref):
    lines = got_ref.shape[0]
    docs = index_ref.shape[1]
    index = index_ref[...]
    line = lax.shift_right_logical(index, 6) * 2 + 1
    rank = lax.bitwise_and(index, CAP - 1)
    onehot = ones_where(iota((lines, docs), 0) == line)
    got = got_ref[...]
    picked = dot(got.astype(F32).T.astype(BF16), onehot)
    wanted = lax.bitwise_and(iota((LANES, docs), 0), CAP - 1) == rank
    best_ref[...] = jnp.sum(jnp.where(wanted, picked, 0.0), axis=0, keepdims=True)
    even = ones_where(lax.bitwise_and(iota((8, lines), 1), 1) == 0)
    hist_ref[...] = dot(even, got)[0:1, :] * (1.0 / (lines * docs))


VMEM = pl.BlockSpec(memory_space=pltpu.VMEM)
ANY = pl.BlockSpec(memory_space=pl.ANY)


def call(kernel, outs, specs, flops, scratch=()):
    many = isinstance(outs, tuple)
    return pl.pallas_call(
        kernel,
        out_shape=outs,
        in_specs=specs,
        out_specs=tuple(VMEM for _ in outs) if many else VMEM,
        scratch_shapes=scratch,
        compiler_params=pltpu.CompilerParams(vmem_limit_bytes=24 * 2**20),
        cost_estimate=pl.CostEstimate(flops=flops, bytes_accessed=4000000, transcendentals=0),
    )


def shape(dims, dtype):
    return jax.ShapeDtypeStruct(dims, dtype)


def in_hbm(x):
    return pltpu.with_memory_space_constraint(x, pltpu.HBM)


def exchange(x, axes):
    return lax.all_to_all(x, axes, split_axis=0, concat_axis=0, tiled=True)


def shards(embeddings, document_cluster_index):
    row_count = lax.axis_size(ROWS)
    col_count = lax.axis_size(COLS)
    docs, width = embeddings.shape
    labels = document_cluster_index.reshape(1, docs)
    block = CAP * width // LANES + 8
    sends, rank = call(
        normalise_and_slot,
        (shape((row_count, block, LANES), BF16), shape((1, docs), F32)),
        [ANY, ANY],
        2 * row_count * CAP * docs * width,
        [
            pltpu.VMEM((1, docs), jnp.int32),
            pltpu.VMEM((docs, width), BF16),
            pltpu.SemaphoreType.DMA((2,)),
        ],
    )(in_hbm(labels), in_hbm(embeddings))
    got = exchange(sends, ROWS)
    total = GROUP_CLUSTERS * CAP
    sends = call(reslot, shape((total, width), BF16), [VMEM], 2 * total * row_count * CAP * width)(
        got
    )
    own = exchange(sends.reshape(GROUP_CLUSTERS, CAP, width), CHIPS)
    own, got = lax.optimization_barrier((own.reshape(total, width), got))
    pairs = [(i, i ^ 1) for i in range(col_count)]
    half = total // 2
    other = [lax.ppermute(own[s : s + half], COLS, pairs) for s in (0, half)]
    flops = 2 * total * half * width
    lines = row_count * GROUP_CLUSTERS * 2
    whole, part = shape((1, total), F32), shape((1, half), F32)
    best = call(best_own, whole, [VMEM], flops)(own)
    best, more = call(best_more, (whole, part), [VMEM] * 3, flops)(own, other[0], best)
    index = call(return_index, shape((1, docs), jnp.int32), [VMEM] * 3, 2**26)(labels, rank, got)
    results = call(best_last, shape((lines, LANES), BF16), [VMEM] * 5, 2 * flops)(
        own, other[0], other[1], best, more
    )
    results, index = lax.optimization_barrier((results, index))
    results = exchange(results.reshape(lines // 2, 2, LANES), SAME_CORE).reshape(lines, LANES)
    best, hist = call(
        pick_results, (shape((1, docs), F32), shape((1, BINS), F32)), [VMEM, VMEM], 2**26
    )(index, results)
    return (best.reshape(docs), hist.reshape(BINS))


def solution(mesh):
    torus = Mesh(
        mesh.devices.reshape(2, 4, 2, 8, 2), ("rows_0", "rows_1", "cols_0", "cols_1", "cols_2")
    )
    in_specs = (P(ALL, None), P(ALL))
    out_specs = (P(ALL), P())
    return jax.shard_map(
        shards, mesh=torus, in_specs=in_specs, out_specs=out_specs, check_vma=False
    )
```

```python
import jax
import jax.numpy as jnp
from jax import lax
from jax.experimental import pallas as pl
from jax.experimental.pallas import tpu as pltpu
from jax.sharding import Mesh
from jax.sharding import PartitionSpec as P

CAP = 64
GROUP_CLUSTERS = 16
BINS = 128
ROWS = ("rows_0", "rows_1")
COLS = ("cols_0", "cols_1", "cols_2")
CHIPS = ("cols_0", "cols_1")
ALL = ROWS + COLS
SAME_CORE = ROWS + CHIPS
LANES = 128
BLOCK = 256
EMPTY = 2.0
F32 = jnp.float32
BF16 = jnp.bfloat16
WIRE = jnp.float16
HIGH_SCALE = 2.0**10
LOW_SCALE = 2.0**18
HIST_SCALE = 16.0


def iota(shape, dim):
    return lax.broadcasted_iota(jnp.int32, shape, dim)


def dot(a, b):
    return lax.dot_general(a, b, (((1,), (0,)), ((), ())), preferred_element_type=F32)


def dot_t(a, b):
    return lax.dot_general(a, b, (((1,), (1,)), ((), ())), preferred_element_type=F32)


def ones_where(mask):
    return jnp.where(mask, 1.0, 0.0).astype(BF16)


def before(n):
    return ones_where(iota((n, n), 0) < iota((n, n), 1))


def rank_of(onehot, n):
    earlier = dot(onehot, before(n))
    return jnp.sum(onehot.astype(F32) * earlier, axis=0, keepdims=True)


def normalise_and_slot(labels_hbm, embeddings_hbm, out_ref, rank_ref, labels_ref, embeddings_ref, sems):
    labels_copy = pltpu.make_async_copy(labels_hbm, labels_ref, sems.at[0])
    embeddings_copy = pltpu.make_async_copy(embeddings_hbm, embeddings_ref, sems.at[1])
    labels_copy.start()
    embeddings_copy.start()
    docs, width = embeddings_ref.shape
    groups = out_ref.shape[0]
    clusters = groups * GROUP_CLUSTERS
    labels_copy.wait()
    labels = labels_ref[...]
    group = lax.shift_right_logical(labels, 4)
    onehot = ones_where(iota((groups, docs), 0) == group)
    slot = group * CAP + rank_of(onehot, docs).astype(jnp.int32)
    places = ones_where(iota((groups * CAP, docs), 0) == slot)
    shifted = jnp.broadcast_to((labels + 1).astype(F32), (8, docs)).astype(BF16)
    slot_labels = dot_t(shifted, places)
    of_cluster = ones_where(iota((clusters, docs), 0) == labels)
    counts = dot_t(jnp.ones((8, docs), BF16), of_cluster)
    row = iota((8, LANES), 0)
    meta = jnp.where(row == groups * CAP // LANES, counts, 0.0)
    for s in range(groups * CAP // LANES):
        meta = jnp.where(row == s, slot_labels[:, s * LANES : (s + 1) * LANES], meta)
    meta = meta.astype(BF16)
    rank_ref[...] = rank_of(of_cluster, docs)
    embeddings_copy.wait()
    values = embeddings_ref[...].astype(F32)
    total = jnp.sum(values * values, axis=1, keepdims=True)
    normed = (values * lax.rsqrt(total + 1e-06)).astype(BF16)
    rows = dot(places, normed).astype(BF16)
    pieces = width // LANES
    for g in range(groups):
        for f in range(pieces):
            block = rows[g * CAP : (g + 1) * CAP, f * LANES : (f + 1) * LANES]
            out_ref[g, f * CAP : (f + 1) * CAP, :] = block
        out_ref[g, pieces * CAP :, :] = meta


def slot_labels_of(got_ref, me):
    groups = got_ref.shape[0]
    slots = groups * CAP
    at = got_ref.shape[1] - 8
    source = lax.shift_right_logical(iota((8, slots), 1), 6)
    row = iota((8, LANES), 0)
    per_row = LANES // CAP
    picked = []
    for g in range(groups):
        meta = got_ref[g, at:, :].astype(F32)
        line = jnp.where(row == lax.shift_right_logical(me, 1), meta, 0.0)
        picked.append(jnp.sum(line, axis=0, keepdims=True))
    lines = jnp.concatenate(picked, axis=0).astype(BF16)
    lane, to = iota((LANES, slots), 0), iota((LANES, slots), 1)
    start = lax.bitwise_and(me, per_row - 1) * CAP
    move = ones_where(lane == start + lax.bitwise_and(to, CAP - 1))
    spread = jnp.where(iota((groups, slots), 0) == source, dot(lines, move), 0.0)
    return jnp.sum(spread, axis=0, keepdims=True)


def reslot(got_ref, out_ref):
    groups = got_ref.shape[0]
    slots = groups * CAP
    width = out_ref.shape[1]
    me = lax.axis_index(ROWS)
    label = slot_labels_of(got_ref, me).astype(jnp.int32)
    cluster = label - 1 - me * GROUP_CLUSTERS
    onehot = ones_where(iota((GROUP_CLUSTERS, slots), 0) == cluster)
    place = cluster * CAP + rank_of(onehot, slots).astype(jnp.int32)
    place = jnp.where(label > 0, place, -1)
    total = GROUP_CLUSTERS * CAP
    step = total // 4
    pieces = width // LANES
    rows = jnp.concatenate(
        [got_ref[:, f * CAP : (f + 1) * CAP, :].reshape(slots, LANES) for f in range(pieces)],
        axis=1,
    )
    for s in range(0, total, step):
        places = jnp.where(iota((step, slots), 0) + s == place, 1.0, 0.0)
        filled = jnp.sum(places, axis=1, keepdims=True) > 0.5
        moved = dot(places.astype(BF16), rows)
        out_ref[s : s + step, LANES:] = moved[:, LANES:].astype(BF16)
        first = moved[:, 0:LANES]
        first = jnp.where((iota(first.shape, 1) == 0) & ~filled, EMPTY, first)
        out_ref[s : s + step, 0:LANES] = first.astype(BF16)


def return_index(labels_ref, rank_ref, got_ref, out_ref):
    groups = got_ref.shape[0]
    docs = labels_ref.shape[1]
    clusters = groups * GROUP_CLUSTERS
    me = lax.axis_index(ROWS)
    at = got_ref.shape[1] - 8
    row = iota((8, LANES), 0)
    before_me = jnp.zeros((8, LANES), F32)
    for g in range(groups):
        before_me = before_me + jnp.where(g < me, got_ref[g, at:, :].astype(F32), 0.0)
    counts = jnp.where(row == groups * CAP // LANES, before_me, 0.0)
    labels = labels_ref[...]
    of_cluster = ones_where(iota((clusters, docs), 0) == labels)
    earlier = jnp.sum(dot(counts.astype(BF16), of_cluster), axis=0, keepdims=True)
    out_ref[...] = labels * CAP + (rank_ref[...] + earlier).astype(jnp.int32)


def penalties(ref):
    total, width = ref.shape
    column = jnp.where(ref[:, 0:1].astype(F32) < 1.5, 0.0, -4.0)
    pick = ones_where(iota((8, 256), 1) == 0)
    row = jnp.where(dot_t(pick, ref[:, 0:256])[0:1, :] < 1.5, 0.0, -4.0)
    return column, row


def over_columns(scores):
    return jnp.max(scores.reshape(BLOCK // 8, 8, BLOCK), axis=0)


def over_rows(scores):
    return jnp.maximum(scores[:, :LANES], scores[:, LANES:])


def as_line(columns, rows):
    out = []
    for column, row in zip(columns, rows):
        line = jnp.max(column, axis=0, keepdims=True)
        if row is not None:
            turned = [jnp.max(row[h : h + LANES].T, axis=0, keepdims=True) for h in (0, LANES)]
            line = jnp.maximum(line, jnp.concatenate(turned, axis=1))
        out.append(line)
    return jnp.concatenate(out, axis=1)


def larger(a, b):
    return b if a is None else jnp.maximum(a, b)


def within(ref, penalty, columns, rows):
    column, row = penalty
    count = ref.shape[0] // BLOCK
    for i in range(count):
        for j in range(i, count):
            at, to = i * BLOCK, j * BLOCK
            scores = dot_t(ref[at : at + BLOCK, :], ref[to : to + BLOCK, :])
            scores = scores + column[at : at + BLOCK] + row[:, to : to + BLOCK]
            if i == j:
                other = iota((BLOCK, BLOCK), 0) != iota((BLOCK, BLOCK), 1)
                scores = jnp.where(other, scores, -4.0)
            else:
                rows[i] = larger(rows[i], over_rows(scores))
            columns[j] = larger(columns[j], over_columns(scores))


def between(a_ref, a_penalty, b_ref, b_penalty, rows, columns):
    for i in range(a_ref.shape[0] // BLOCK):
        for j in range(b_ref.shape[0] // BLOCK):
            at, to = i * BLOCK, j * BLOCK
            scores = dot_t(a_ref[at : at + BLOCK, :], b_ref[to : to + BLOCK, :])
            scores = scores + a_penalty[0][at : at + BLOCK] + b_penalty[1][:, to : to + BLOCK]
            rows[i] = larger(rows[i], over_rows(scores))
            columns[j] = larger(columns[j], over_columns(scores))


def nothing(ref):
    return [None] * (ref.shape[0] // BLOCK)


def best_own(own_ref, best_ref):
    columns, rows = nothing(own_ref), nothing(own_ref)
    within(own_ref, penalties(own_ref), columns, rows)
    best_ref[...] = jnp.maximum(as_line(columns, rows), -1.0)


def best_more(own_ref, more_ref, so_far_ref, best_ref, best_more_ref):
    columns, rows, of_own = nothing(more_ref), nothing(more_ref), nothing(own_ref)
    penalty = penalties(more_ref)
    between(more_ref, penalty, own_ref, penalties(own_ref), rows, of_own)
    within(more_ref, penalty, columns, rows)
    best_more_ref[...] = as_line(columns, rows)
    best_ref[...] = jnp.maximum(as_line(of_own, nothing(own_ref)), so_far_ref[...])


def histogram_parts(best, penalty):
    width = 2.0 / (BINS - 1)
    centers = -1.0 + iota((BINS, 1), 0).astype(F32) * width
    weights = jnp.maximum(1.0 - jnp.abs(best - centers) / width, 0.0)
    weights = jnp.where(penalty < 0.0, 0.0, weights)
    folded = weights[:, 0:LANES]
    for s in range(LANES, best.shape[1], LANES):
        folded = folded + weights[:, s : s + LANES]
    return folded


def best_last(own_ref, more_ref, last_ref, so_far_ref, more_so_far_ref, out_ref):
    total = own_ref.shape[0]
    own_penalty, more_penalty = penalties(own_ref), penalties(more_ref)
    penalty = penalties(last_ref)
    columns, rows, of_own = nothing(last_ref), nothing(last_ref), nothing(own_ref)
    of_more = nothing(more_ref)
    between(more_ref, more_penalty, last_ref, penalty, of_more, columns)
    between(last_ref, penalty, own_ref, own_penalty, rows, of_own)
    within(last_ref, penalty, columns, rows)
    best = jnp.maximum(as_line(of_own, nothing(own_ref)), so_far_ref[...])
    more_line = [more_so_far_ref[:, s : s + BLOCK] for s in range(0, more_ref.shape[0], BLOCK)]
    more_best = jnp.maximum(as_line(more_line, of_more), -1.0)
    last_best = jnp.maximum(as_line(columns, rows), -1.0)
    mine = histogram_parts(best, own_penalty[1])
    theirs = histogram_parts(
        jnp.concatenate([more_best, last_best], axis=1),
        jnp.concatenate([more_penalty[1], penalty[1]], axis=1),
    )
    hist = jnp.sum((mine + theirs).T, axis=0, keepdims=True)
    high = best.astype(BF16).astype(F32)
    low = (best - high) * LOW_SCALE
    high = high * HIGH_SCALE
    hist = hist * HIST_SCALE
    sub = iota((8, LANES), 0)
    left = iota((1, LANES), 1) < CAP
    blocks = []
    for s in range(0, total, 2 * LANES):
        block = jnp.broadcast_to(hist, (8, LANES))
        for h in range(2):
            at = s + h * LANES
            top, rest = high[:, at : at + LANES], low[:, at : at + LANES]
            first = jnp.where(left, top, pltpu.roll(rest, CAP, 1))
            second = jnp.where(left, pltpu.roll(top, CAP, 1), rest)
            block = jnp.where(sub == 4 * h + 1, first, block)
            block = jnp.where(sub == 4 * h + 3, second, block)
        blocks.append(block)
    block = jnp.concatenate(blocks, axis=0)
    for at in range(0, out_ref.shape[0], block.shape[0]):
        out_ref[at : at + block.shape[0], :] = block


def pick_results(index_ref, got_ref, best_ref, hist_ref):
    lines = got_ref.shape[0]
    docs = index_ref.shape[1]
    index = index_ref[...]
    line = lax.shift_right_logical(index, 6) * 2 + 1
    rank = lax.bitwise_and(index, CAP - 1)
    onehot = ones_where(iota((lines, docs), 0) == line)
    got = got_ref[...]
    turned = got.T
    high = turned.astype(BF16)
    low = (turned - high.astype(F32)).astype(BF16)
    picked = dot(high, onehot) + dot(low, onehot)
    lane = iota((LANES, docs), 0)
    picked = picked * jnp.where(lane < CAP, 1.0 / HIGH_SCALE, 1.0 / LOW_SCALE)
    wanted = lax.bitwise_and(lane, CAP - 1) == rank
    best_ref[...] = jnp.sum(jnp.where(wanted, picked, 0.0), axis=0, keepdims=True)
    even = lax.bitwise_and(iota((8, LANES), 0), 1) == 0
    total = jnp.zeros((8, LANES), F32)
    for s in range(0, lines, 8):
        total = total + jnp.where(even, got[s : s + 8, :], 0.0)
    hist_ref[...] = jnp.sum(total, axis=0, keepdims=True) * (1.0 / (HIST_SCALE * lines * docs))


VMEM = pl.BlockSpec(memory_space=pltpu.VMEM)
ANY = pl.BlockSpec(memory_space=pl.ANY)


def call(kernel, outs, specs, flops, scratch=()):
    many = isinstance(outs, tuple)
    return pl.pallas_call(
        kernel,
        out_shape=outs,
        in_specs=specs,
        out_specs=tuple(VMEM for _ in outs) if many else VMEM,
        scratch_shapes=scratch,
        compiler_params=pltpu.CompilerParams(vmem_limit_bytes=24 * 2**20),
        cost_estimate=pl.CostEstimate(flops=flops, bytes_accessed=4000000, transcendentals=0),
    )


def shape(dims, dtype):
    return jax.ShapeDtypeStruct(dims, dtype)


def in_hbm(x):
    return pltpu.with_memory_space_constraint(x, pltpu.HBM)


def exchange(x, axes):
    return lax.all_to_all(x, axes, split_axis=0, concat_axis=0, tiled=True)


def shards(embeddings, document_cluster_index):
    row_count = lax.axis_size(ROWS)
    col_count = lax.axis_size(COLS)
    docs, width = embeddings.shape
    labels = document_cluster_index.reshape(1, docs)
    block = CAP * width // LANES + 8
    sends, rank = call(
        normalise_and_slot,
        (shape((row_count, block, LANES), BF16), shape((1, docs), F32)),
        [ANY, ANY],
        2 * row_count * CAP * docs * width,
        [
            pltpu.VMEM((1, docs), jnp.int32),
            pltpu.VMEM((docs, width), BF16),
            pltpu.SemaphoreType.DMA((2,)),
        ],
    )(in_hbm(labels), in_hbm(embeddings))
    got = exchange(sends, ROWS)
    total = GROUP_CLUSTERS * CAP
    sends = call(reslot, shape((total, width), BF16), [VMEM], 2 * total * row_count * CAP * width)(
        got
    )
    own = exchange(sends.reshape(GROUP_CLUSTERS, CAP, width), CHIPS)
    own, got = lax.optimization_barrier((own.reshape(total, width), got))
    pairs = [(i, i ^ 1) for i in range(col_count)]
    half = total // 2
    other = [lax.ppermute(own[s : s + half], COLS, pairs) for s in (0, half)]
    flops = 2 * total * half * width
    lines = row_count * GROUP_CLUSTERS * 2
    whole, part = shape((1, total), F32), shape((1, half), F32)
    best = call(best_own, whole, [VMEM], flops)(own)
    best, more = call(best_more, (whole, part), [VMEM] * 3, flops)(own, other[0], best)
    index = call(return_index, shape((1, docs), jnp.int32), [VMEM] * 3, 2**26)(labels, rank, got)
    results = call(best_last, shape((lines, LANES), F32), [VMEM] * 5, 2 * flops)(
        own, other[0], other[1], best, more
    )
    results, index = lax.optimization_barrier((results, index))
    results = exchange(results.astype(WIRE).reshape(lines // 2, 2, LANES), SAME_CORE)
    results = results.reshape(lines, LANES).astype(F32)
    best, hist = call(
        pick_results, (shape((1, docs), F32), shape((1, BINS), F32)), [VMEM, VMEM], 2**26
    )(index, results)
    return (best.reshape(docs), hist.reshape(BINS))


def solution(mesh):
    torus = Mesh(
        mesh.devices.reshape(2, 4, 2, 8, 2), ("rows_0", "rows_1", "cols_0", "cols_1", "cols_2")
    )
    in_specs = (P(ALL, None), P(ALL))
    out_specs = (P(ALL), P())
    return jax.shard_map(
        shards, mesh=torus, in_specs=in_specs, out_specs=out_specs, check_vma=False
    )
```

```python
import jax
import jax.numpy as jnp
from jax import lax
from jax.experimental import pallas as pl
from jax.experimental.pallas import tpu as pltpu
from jax.sharding import Mesh
from jax.sharding import PartitionSpec as P

CAP = 64
GROUP_CLUSTERS = 16
BINS = 128
ROWS = ("rows_0", "rows_1")
COLS = ("cols_0", "cols_1", "cols_2")
CHIPS = ("cols_0", "cols_1")
ALL = ROWS + COLS
SAME_CORE = ROWS + CHIPS
LANES = 128
BLOCK = 256
EMPTY = 2.0
F32 = jnp.float32
BF16 = jnp.bfloat16
WIRE = jnp.float16
HIGH_SCALE = 2.0**10
LOW_SCALE = 2.0**18
HIST_SCALE = 16.0


def iota(shape, dim):
    return lax.broadcasted_iota(jnp.int32, shape, dim)


def dot(a, b):
    return lax.dot_general(a, b, (((1,), (0,)), ((), ())), preferred_element_type=F32)


def dot_t(a, b):
    return lax.dot_general(a, b, (((1,), (1,)), ((), ())), preferred_element_type=F32)


def ones_where(mask):
    return jnp.where(mask, 1.0, 0.0).astype(BF16)


def before(n):
    return ones_where(iota((n, n), 0) < iota((n, n), 1))


def rank_of(onehot, n):
    earlier = dot(onehot, before(n))
    return jnp.sum(onehot.astype(F32) * earlier, axis=0, keepdims=True)


def normalise_and_slot(labels_hbm, embeddings_hbm, out_ref, rank_ref, labels_ref, embeddings_ref, sems):
    labels_copy = pltpu.make_async_copy(labels_hbm, labels_ref, sems.at[0])
    embeddings_copy = pltpu.make_async_copy(embeddings_hbm, embeddings_ref, sems.at[1])
    labels_copy.start()
    embeddings_copy.start()
    docs, width = embeddings_ref.shape
    groups = out_ref.shape[0]
    clusters = groups * GROUP_CLUSTERS
    labels_copy.wait()
    labels = labels_ref[...]
    group = lax.shift_right_logical(labels, 4)
    onehot = ones_where(iota((groups, docs), 0) == group)
    slot = group * CAP + rank_of(onehot, docs).astype(jnp.int32)
    places = ones_where(iota((groups * CAP, docs), 0) == slot)
    shifted = jnp.broadcast_to((labels + 1).astype(F32), (8, docs)).astype(BF16)
    slot_labels = dot_t(shifted, places)
    of_cluster = ones_where(iota((clusters, docs), 0) == labels)
    counts = dot_t(jnp.ones((8, docs), BF16), of_cluster)
    row = iota((8, LANES), 0)
    meta = jnp.where(row == groups * CAP // LANES, counts, 0.0)
    for s in range(groups * CAP // LANES):
        meta = jnp.where(row == s, slot_labels[:, s * LANES : (s + 1) * LANES], meta)
    meta = meta.astype(BF16)
    rank_ref[...] = rank_of(of_cluster, docs)
    embeddings_copy.wait()
    values = embeddings_ref[...].astype(F32)
    total = jnp.sum(values * values, axis=1, keepdims=True)
    normed = (values * lax.rsqrt(total + 1e-06)).astype(BF16)
    rows = dot(places, normed).astype(BF16)
    pieces = width // LANES
    for g in range(groups):
        for f in range(pieces):
            block = rows[g * CAP : (g + 1) * CAP, f * LANES : (f + 1) * LANES]
            out_ref[g, f * CAP : (f + 1) * CAP, :] = block
        out_ref[g, pieces * CAP :, :] = meta


def slot_labels_of(got_ref, me):
    groups = got_ref.shape[0]
    slots = groups * CAP
    at = got_ref.shape[1] - 8
    source = lax.shift_right_logical(iota((8, slots), 1), 6)
    row = iota((8, LANES), 0)
    per_row = LANES // CAP
    picked = []
    for g in range(groups):
        meta = got_ref[g, at:, :].astype(F32)
        line = jnp.where(row == lax.shift_right_logical(me, 1), meta, 0.0)
        picked.append(jnp.sum(line, axis=0, keepdims=True))
    lines = jnp.concatenate(picked, axis=0).astype(BF16)
    lane, to = iota((LANES, slots), 0), iota((LANES, slots), 1)
    start = lax.bitwise_and(me, per_row - 1) * CAP
    move = ones_where(lane == start + lax.bitwise_and(to, CAP - 1))
    spread = jnp.where(iota((groups, slots), 0) == source, dot(lines, move), 0.0)
    return jnp.sum(spread, axis=0, keepdims=True)


def reslot(got_ref, out_ref):
    groups = got_ref.shape[0]
    slots = groups * CAP
    width = out_ref.shape[1]
    me = lax.axis_index(ROWS)
    label = slot_labels_of(got_ref, me).astype(jnp.int32)
    cluster = label - 1 - me * GROUP_CLUSTERS
    onehot = ones_where(iota((GROUP_CLUSTERS, slots), 0) == cluster)
    place = cluster * CAP + rank_of(onehot, slots).astype(jnp.int32)
    place = jnp.where(label > 0, place, -1)
    total = GROUP_CLUSTERS * CAP
    step = total // 4
    pieces = width // LANES
    rows = jnp.concatenate(
        [got_ref[:, f * CAP : (f + 1) * CAP, :].reshape(slots, LANES) for f in range(pieces)],
        axis=1,
    )
    for s in range(0, total, step):
        places = jnp.where(iota((step, slots), 0) + s == place, 1.0, 0.0)
        filled = jnp.sum(places, axis=1, keepdims=True) > 0.5
        moved = dot(places.astype(BF16), rows)
        out_ref[s : s + step, LANES:] = moved[:, LANES:].astype(BF16)
        first = moved[:, 0:LANES]
        first = jnp.where((iota(first.shape, 1) == 0) & ~filled, EMPTY, first)
        out_ref[s : s + step, 0:LANES] = first.astype(BF16)


def return_index(labels_ref, rank_ref, got_ref, out_ref):
    groups = got_ref.shape[0]
    docs = labels_ref.shape[1]
    clusters = groups * GROUP_CLUSTERS
    me = lax.axis_index(ROWS)
    at = got_ref.shape[1] - 8
    row = iota((8, LANES), 0)
    before_me = jnp.zeros((8, LANES), F32)
    for g in range(groups):
        before_me = before_me + jnp.where(g < me, got_ref[g, at:, :].astype(F32), 0.0)
    counts = jnp.where(row == groups * CAP // LANES, before_me, 0.0)
    labels = labels_ref[...]
    of_cluster = ones_where(iota((clusters, docs), 0) == labels)
    earlier = jnp.sum(dot(counts.astype(BF16), of_cluster), axis=0, keepdims=True)
    out_ref[...] = labels * CAP + (rank_ref[...] + earlier).astype(jnp.int32)


def penalties(ref):
    total, width = ref.shape
    column = jnp.where(ref[:, 0:1].astype(F32) < 1.5, 0.0, -4.0)
    pick = ones_where(iota((8, 256), 1) == 0)
    row = jnp.where(dot_t(pick, ref[:, 0:256])[0:1, :] < 1.5, 0.0, -4.0)
    return column, row


def over_columns(scores):
    return jnp.max(scores.reshape(BLOCK // 8, 8, BLOCK), axis=0)


def over_rows(scores):
    return jnp.maximum(scores[:, :LANES], scores[:, LANES:])


def as_line(columns, rows):
    out = []
    for column, row in zip(columns, rows):
        line = jnp.max(column, axis=0, keepdims=True)
        if row is not None:
            turned = [jnp.max(row[h : h + LANES].T, axis=0, keepdims=True) for h in (0, LANES)]
            line = jnp.maximum(line, jnp.concatenate(turned, axis=1))
        out.append(line)
    return jnp.concatenate(out, axis=1)


def larger(a, b):
    return b if a is None else jnp.maximum(a, b)


def within(ref, penalty, columns, rows):
    column, row = penalty
    count = ref.shape[0] // BLOCK
    for i in range(count):
        for j in range(i, count):
            at, to = i * BLOCK, j * BLOCK
            scores = dot_t(ref[at : at + BLOCK, :], ref[to : to + BLOCK, :])
            scores = scores + column[at : at + BLOCK] + row[:, to : to + BLOCK]
            if i == j:
                other = iota((BLOCK, BLOCK), 0) != iota((BLOCK, BLOCK), 1)
                scores = jnp.where(other, scores, -4.0)
            else:
                rows[i] = larger(rows[i], over_rows(scores))
            columns[j] = larger(columns[j], over_columns(scores))


def between(a_ref, a_penalty, b_ref, b_penalty, rows, columns):
    for i in range(a_ref.shape[0] // BLOCK):
        for j in range(b_ref.shape[0] // BLOCK):
            at, to = i * BLOCK, j * BLOCK
            scores = dot_t(a_ref[at : at + BLOCK, :], b_ref[to : to + BLOCK, :])
            scores = scores + a_penalty[0][at : at + BLOCK] + b_penalty[1][:, to : to + BLOCK]
            rows[i] = larger(rows[i], over_rows(scores))
            columns[j] = larger(columns[j], over_columns(scores))


def nothing(ref):
    return [None] * (ref.shape[0] // BLOCK)


def best_of(own_ref):
    columns, rows = nothing(own_ref), nothing(own_ref)
    within(own_ref, penalties(own_ref), columns, rows)
    return jnp.maximum(as_line(columns, rows), -1.0)


def best_own_early(own_ref, best_ref):
    early = lax.axis_index("cols_2") == 1

    @pl.when(early)
    def _():
        best_ref[...] = best_of(own_ref)

    @pl.when(jnp.logical_not(early))
    def _():
        best_ref[...] = jnp.full(best_ref.shape, -1.0, F32)


def best_own_late(own_ref, early_ref, best_ref):
    early = lax.axis_index("cols_2") == 1

    @pl.when(early)
    def _():
        best_ref[...] = early_ref[...]

    @pl.when(jnp.logical_not(early))
    def _():
        best_ref[...] = best_of(own_ref)


def best_more(own_ref, more_ref, so_far_ref, best_ref, best_more_ref):
    columns, rows, of_own = nothing(more_ref), nothing(more_ref), nothing(own_ref)
    penalty = penalties(more_ref)
    between(more_ref, penalty, own_ref, penalties(own_ref), rows, of_own)
    within(more_ref, penalty, columns, rows)
    best_more_ref[...] = as_line(columns, rows)
    best_ref[...] = jnp.maximum(as_line(of_own, nothing(own_ref)), so_far_ref[...])


def histogram_parts(best, penalty):
    width = 2.0 / (BINS - 1)
    at = jnp.where(penalty < 0.0, 2.0 * BINS, (best + 1.0) * (1.0 / width))
    weights = jnp.maximum(1.0 - jnp.abs(at - iota((BINS, 1), 0).astype(F32)), 0.0)
    folded = weights[:, 0:LANES]
    for s in range(LANES, best.shape[1], LANES):
        folded = folded + weights[:, s : s + LANES]
    return folded


def best_last(own_ref, more_ref, last_ref, so_far_ref, more_so_far_ref, out_ref):
    total = own_ref.shape[0]
    own_penalty, more_penalty = penalties(own_ref), penalties(more_ref)
    penalty = penalties(last_ref)
    columns, rows, of_own = nothing(last_ref), nothing(last_ref), nothing(own_ref)
    of_more = nothing(more_ref)
    between(more_ref, more_penalty, last_ref, penalty, of_more, columns)
    between(last_ref, penalty, own_ref, own_penalty, rows, of_own)
    within(last_ref, penalty, columns, rows)
    best = jnp.maximum(as_line(of_own, nothing(own_ref)), so_far_ref[...])
    more_line = [more_so_far_ref[:, s : s + BLOCK] for s in range(0, more_ref.shape[0], BLOCK)]
    more_best = jnp.maximum(as_line(more_line, of_more), -1.0)
    last_best = jnp.maximum(as_line(columns, rows), -1.0)
    mine = histogram_parts(best, own_penalty[1])
    theirs = histogram_parts(
        jnp.concatenate([more_best, last_best], axis=1),
        jnp.concatenate([more_penalty[1], penalty[1]], axis=1),
    )
    hist = jnp.sum((mine + theirs).T, axis=0, keepdims=True)
    high = best.astype(BF16).astype(F32)
    low = (best - high) * LOW_SCALE
    high = high * HIGH_SCALE
    hist = hist * HIST_SCALE
    sub = iota((8, LANES), 0)
    left = iota((1, LANES), 1) < CAP
    blocks = []
    for s in range(0, total, 2 * LANES):
        block = jnp.broadcast_to(hist, (8, LANES))
        for h in range(2):
            at = s + h * LANES
            top, rest = high[:, at : at + LANES], low[:, at : at + LANES]
            first = jnp.where(left, top, pltpu.roll(rest, CAP, 1))
            second = jnp.where(left, pltpu.roll(top, CAP, 1), rest)
            block = jnp.where(sub == 4 * h + 1, first, block)
            block = jnp.where(sub == 4 * h + 3, second, block)
        blocks.append(block)
    block = jnp.concatenate(blocks, axis=0)
    for at in range(0, out_ref.shape[0], block.shape[0]):
        out_ref[at : at + block.shape[0], :] = block


def pick_results(index_ref, got_ref, best_ref, hist_ref):
    lines = got_ref.shape[0]
    docs = index_ref.shape[1]
    index = index_ref[...]
    line = lax.shift_right_logical(index, 6) * 2 + 1
    rank = lax.bitwise_and(index, CAP - 1)
    onehot = ones_where(iota((lines, docs), 0) == line)
    got = got_ref[...]
    turned = got.T
    high = turned.astype(BF16)
    low = (turned - high.astype(F32)).astype(BF16)
    picked = dot(high, onehot) + dot(low, onehot)
    lane = iota((LANES, docs), 0)
    picked = picked * jnp.where(lane < CAP, 1.0 / HIGH_SCALE, 1.0 / LOW_SCALE)
    wanted = lax.bitwise_and(lane, CAP - 1) == rank
    best_ref[...] = jnp.sum(jnp.where(wanted, picked, 0.0), axis=0, keepdims=True)
    even = lax.bitwise_and(iota((8, LANES), 0), 1) == 0
    total = jnp.zeros((8, LANES), F32)
    for s in range(0, lines, 8):
        total = total + jnp.where(even, got[s : s + 8, :], 0.0)
    hist_ref[...] = jnp.sum(total, axis=0, keepdims=True) * (1.0 / (HIST_SCALE * lines * docs))


VMEM = pl.BlockSpec(memory_space=pltpu.VMEM)
ANY = pl.BlockSpec(memory_space=pl.ANY)


def call(kernel, outs, specs, flops, scratch=()):
    many = isinstance(outs, tuple)
    return pl.pallas_call(
        kernel,
        out_shape=outs,
        in_specs=specs,
        out_specs=tuple(VMEM for _ in outs) if many else VMEM,
        scratch_shapes=scratch,
        compiler_params=pltpu.CompilerParams(vmem_limit_bytes=24 * 2**20),
        cost_estimate=pl.CostEstimate(flops=flops, bytes_accessed=4000000, transcendentals=0),
    )


def shape(dims, dtype):
    return jax.ShapeDtypeStruct(dims, dtype)


def in_hbm(x):
    return pltpu.with_memory_space_constraint(x, pltpu.HBM)


def exchange(x, axes):
    return lax.all_to_all(x, axes, split_axis=0, concat_axis=0, tiled=True)


def shards(embeddings, document_cluster_index):
    row_count = lax.axis_size(ROWS)
    col_count = lax.axis_size(COLS)
    docs, width = embeddings.shape
    labels = document_cluster_index.reshape(1, docs)
    block = CAP * width // LANES + 8
    sends, rank = call(
        normalise_and_slot,
        (shape((row_count, block, LANES), BF16), shape((1, docs), F32)),
        [ANY, ANY],
        2 * row_count * CAP * docs * width,
        [
            pltpu.VMEM((1, docs), jnp.int32),
            pltpu.VMEM((docs, width), BF16),
            pltpu.SemaphoreType.DMA((2,)),
        ],
    )(in_hbm(labels), in_hbm(embeddings))
    got = exchange(sends, ROWS)
    total = GROUP_CLUSTERS * CAP
    sends = call(reslot, shape((total, width), BF16), [VMEM], 2 * total * row_count * CAP * width)(
        got
    )
    own = exchange(sends.reshape(GROUP_CLUSTERS, CAP, width), CHIPS)
    own, got = lax.optimization_barrier((own.reshape(total, width), got))
    whole, part = shape((1, total), F32), shape((1, total // 2), F32)
    flops = 2 * total * total // 2 * width
    early = call(best_own_early, whole, [VMEM], flops)(own)
    own, early = lax.optimization_barrier((own, early))
    pairs = [(i, i ^ 1) for i in range(col_count)]
    half = total // 2
    other = [lax.ppermute(own[s : s + half], COLS, pairs) for s in (0, half)]
    lines = row_count * GROUP_CLUSTERS * 2
    best = call(best_own_late, whole, [VMEM] * 2, flops)(own, early)
    best, more = call(best_more, (whole, part), [VMEM] * 3, flops)(own, other[0], best)
    index = call(return_index, shape((1, docs), jnp.int32), [VMEM] * 3, 2**26)(labels, rank, got)
    results = call(best_last, shape((lines, LANES), F32), [VMEM] * 5, 2 * flops)(
        own, other[0], other[1], best, more
    )
    results, index = lax.optimization_barrier((results, index))
    results = exchange(results.astype(WIRE).reshape(lines // 2, 2, LANES), SAME_CORE)
    results = results.reshape(lines, LANES).astype(F32)
    best, hist = call(
        pick_results, (shape((1, docs), F32), shape((1, BINS), F32)), [VMEM, VMEM], 2**26
    )(index, results)
    return (best.reshape(docs), hist.reshape(BINS))


def solution(mesh):
    torus = Mesh(
        mesh.devices.reshape(2, 4, 2, 8, 2), ("rows_0", "rows_1", "cols_0", "cols_1", "cols_2")
    )
    in_specs = (P(ALL, None), P(ALL))
    out_specs = (P(ALL), P())
    return jax.shard_map(
        shards, mesh=torus, in_specs=in_specs, out_specs=out_specs, check_vma=False
    )
```

```python
import jax
import jax.numpy as jnp
from jax import lax
from jax.experimental import pallas as pl
from jax.experimental.pallas import tpu as pltpu
from jax.sharding import Mesh
from jax.sharding import PartitionSpec as P


CAP = 64
GROUP_CLUSTERS = 16
BINS = 128
ROWS = ("rows_0", "rows_1")
COLS = ("cols_0", "cols_1", "cols_2")
CHIPS = ("cols_0", "cols_1")
ALL = ROWS + COLS
SAME_CORE = ROWS + CHIPS
LANES = 128
BLOCK = 256
EMPTY = 2.0
F32 = jnp.float32
BF16 = jnp.bfloat16
WIRE = jnp.float16
HIGH_SCALE = 2.0**10
LOW_SCALE = 2.0**18
HIST_SCALE = 16.0


def iota(shape, dim):
    return lax.broadcasted_iota(jnp.int32, shape, dim)


def dot(a, b):
    return lax.dot_general(a, b, (((1,), (0,)), ((), ())), preferred_element_type=F32)


def dot_t(a, b):
    return lax.dot_general(a, b, (((1,), (1,)), ((), ())), preferred_element_type=F32)


def ones_where(mask):
    return jnp.where(mask, 1.0, 0.0).astype(BF16)


def before(n):
    return ones_where(iota((n, n), 0) < iota((n, n), 1))


def rank_of(onehot, n):
    earlier = dot(onehot, before(n))
    return jnp.sum(onehot.astype(F32) * earlier, axis=0, keepdims=True)


def normalise_and_slot(labels_hbm, embeddings_hbm, out_ref, rank_ref, labels_ref, embeddings_ref, sems):
    labels_copy = pltpu.make_async_copy(labels_hbm, labels_ref, sems.at[0])
    embeddings_copy = pltpu.make_async_copy(embeddings_hbm, embeddings_ref, sems.at[1])
    labels_copy.start()
    embeddings_copy.start()
    docs, width = embeddings_ref.shape
    groups = out_ref.shape[0]
    clusters = groups * GROUP_CLUSTERS
    labels_copy.wait()
    labels = labels_ref[...]
    group = lax.shift_right_logical(labels, 4)
    onehot = ones_where(iota((groups, docs), 0) == group)
    slot = group * CAP + rank_of(onehot, docs).astype(jnp.int32)
    places = ones_where(iota((groups * CAP, docs), 0) == slot)
    shifted = jnp.broadcast_to((labels + 1).astype(F32), (8, docs)).astype(BF16)
    slot_labels = dot_t(shifted, places)
    of_cluster = ones_where(iota((clusters, docs), 0) == labels)
    counts = dot_t(jnp.ones((8, docs), BF16), of_cluster)
    row = iota((8, LANES), 0)
    meta = jnp.where(row == groups * CAP // LANES, counts, 0.0)
    for s in range(groups * CAP // LANES):
        meta = jnp.where(row == s, slot_labels[:, s * LANES : (s + 1) * LANES], meta)
    meta = meta.astype(BF16)
    rank_ref[...] = rank_of(of_cluster, docs)
    embeddings_copy.wait()
    values = embeddings_ref[...].astype(F32)
    total = jnp.sum(values * values, axis=1, keepdims=True)
    normed = (values * lax.rsqrt(total + 1e-06)).astype(BF16)
    rows = dot(places, normed).astype(BF16)
    pieces = width // LANES
    for g in range(groups):
        for f in range(pieces):
            block = rows[g * CAP : (g + 1) * CAP, f * LANES : (f + 1) * LANES]
            out_ref[g, f * CAP : (f + 1) * CAP, :] = block
        out_ref[g, pieces * CAP :, :] = meta


def slot_labels_of(got_ref, me):
    groups = got_ref.shape[0]
    slots = groups * CAP
    at = got_ref.shape[1] - 8
    source = lax.shift_right_logical(iota((8, slots), 1), 6)
    row = iota((8, LANES), 0)
    per_row = LANES // CAP
    picked = []
    for g in range(groups):
        meta = got_ref[g, at:, :].astype(F32)
        line = jnp.where(row == lax.shift_right_logical(me, 1), meta, 0.0)
        picked.append(jnp.sum(line, axis=0, keepdims=True))
    lines = jnp.concatenate(picked, axis=0).astype(BF16)
    lane, to = iota((LANES, slots), 0), iota((LANES, slots), 1)
    start = lax.bitwise_and(me, per_row - 1) * CAP
    move = ones_where(lane == start + lax.bitwise_and(to, CAP - 1))
    spread = jnp.where(iota((groups, slots), 0) == source, dot(lines, move), 0.0)
    return jnp.sum(spread, axis=0, keepdims=True)


def reslot(got_ref, out_ref):
    groups = got_ref.shape[0]
    slots = groups * CAP
    width = out_ref.shape[1]
    me = lax.axis_index(ROWS)
    label = slot_labels_of(got_ref, me).astype(jnp.int32)
    cluster = label - 1 - me * GROUP_CLUSTERS
    onehot = ones_where(iota((GROUP_CLUSTERS, slots), 0) == cluster)
    place = cluster * CAP + rank_of(onehot, slots).astype(jnp.int32)
    place = jnp.where(label > 0, place, -1)
    total = GROUP_CLUSTERS * CAP
    step = total // 4
    pieces = width // LANES
    rows = jnp.concatenate(
        [got_ref[:, f * CAP : (f + 1) * CAP, :].reshape(slots, LANES) for f in range(pieces)],
        axis=1,
    )
    for s in range(0, total, step):
        places = jnp.where(iota((step, slots), 0) + s == place, 1.0, 0.0)
        filled = jnp.sum(places, axis=1, keepdims=True) > 0.5
        moved = dot(places.astype(BF16), rows)
        out_ref[s : s + step, LANES:] = moved[:, LANES:].astype(BF16)
        first = moved[:, 0:LANES]
        first = jnp.where((iota(first.shape, 1) == 0) & ~filled, EMPTY, first)
        out_ref[s : s + step, 0:LANES] = first.astype(BF16)


def return_index(labels_ref, rank_ref, got_ref, out_ref):
    groups = got_ref.shape[0]
    docs = labels_ref.shape[1]
    clusters = groups * GROUP_CLUSTERS
    me = lax.axis_index(ROWS)
    at = got_ref.shape[1] - 8
    row = iota((8, LANES), 0)
    before_me = jnp.zeros((8, LANES), F32)
    for g in range(groups):
        before_me = before_me + jnp.where(g < me, got_ref[g, at:, :].astype(F32), 0.0)
    counts = jnp.where(row == groups * CAP // LANES, before_me, 0.0)
    labels = labels_ref[...]
    of_cluster = ones_where(iota((clusters, docs), 0) == labels)
    earlier = jnp.sum(dot(counts.astype(BF16), of_cluster), axis=0, keepdims=True)
    out_ref[...] = labels * CAP + (rank_ref[...] + earlier).astype(jnp.int32)


def penalties(ref):
    column = jnp.where(ref[:, 0:1].astype(F32) < 1.5, 0.0, -4.0)
    pick = ones_where(iota((8, 256), 1) == 0)
    row = jnp.where(dot_t(pick, ref[:, 0:256])[0:1, :] < 1.5, 0.0, -4.0)
    return column, row


def over_columns(scores):
    return jnp.max(scores.reshape(BLOCK // 8, 8, BLOCK), axis=0)


def over_rows(scores):
    return jnp.maximum(scores[:, :LANES], scores[:, LANES:])


def as_line(columns, rows):
    out = []
    for column, row in zip(columns, rows):
        line = jnp.max(column, axis=0, keepdims=True)
        if row is not None:
            turned = [jnp.max(row[h : h + LANES].T, axis=0, keepdims=True) for h in (0, LANES)]
            line = jnp.maximum(line, jnp.concatenate(turned, axis=1))
        out.append(line)
    return jnp.concatenate(out, axis=1)


def larger(a, b):
    return b if a is None else jnp.maximum(a, b)


def within(ref, penalty, columns, rows):
    column, row = penalty
    count = ref.shape[0] // BLOCK
    for i in range(count):
        for j in range(i, count):
            at, to = i * BLOCK, j * BLOCK
            scores = dot_t(ref[at : at + BLOCK, :], ref[to : to + BLOCK, :])
            scores = scores + column[at : at + BLOCK] + row[:, to : to + BLOCK]
            if i == j:
                other = iota((BLOCK, BLOCK), 0) != iota((BLOCK, BLOCK), 1)
                scores = jnp.where(other, scores, -4.0)
            else:
                rows[i] = larger(rows[i], over_rows(scores))
            columns[j] = larger(columns[j], over_columns(scores))


def between(a_ref, a_penalty, b_ref, b_penalty, rows, columns):
    for i in range(a_ref.shape[0] // BLOCK):
        for j in range(b_ref.shape[0] // BLOCK):
            at, to = i * BLOCK, j * BLOCK
            scores = dot_t(a_ref[at : at + BLOCK, :], b_ref[to : to + BLOCK, :])
            scores = scores + a_penalty[0][at : at + BLOCK] + b_penalty[1][:, to : to + BLOCK]
            rows[i] = larger(rows[i], over_rows(scores))
            columns[j] = larger(columns[j], over_columns(scores))


def nothing(ref):
    return [None] * (ref.shape[0] // BLOCK)


def best_of(own_ref):
    columns, rows = nothing(own_ref), nothing(own_ref)
    within(own_ref, penalties(own_ref), columns, rows)
    return jnp.maximum(as_line(columns, rows), -1.0)


def best_own_early(own_ref, best_ref):
    early = lax.axis_index("cols_2") == 1

    @pl.when(early)
    def _():
        best_ref[...] = best_of(own_ref)

    @pl.when(jnp.logical_not(early))
    def _():
        best_ref[...] = jnp.full(best_ref.shape, -1.0, F32)


def best_own_late(own_ref, early_ref, best_ref):
    early = lax.axis_index("cols_2") == 1

    @pl.when(early)
    def _():
        best_ref[...] = early_ref[...]

    @pl.when(jnp.logical_not(early))
    def _():
        best_ref[...] = best_of(own_ref)


def best_more(own_ref, more_ref, so_far_ref, best_ref, best_more_ref):
    columns, rows, of_own = nothing(more_ref), nothing(more_ref), nothing(own_ref)
    penalty = penalties(more_ref)
    between(more_ref, penalty, own_ref, penalties(own_ref), rows, of_own)
    within(more_ref, penalty, columns, rows)
    best_more_ref[...] = as_line(columns, rows)
    best_ref[...] = jnp.maximum(as_line(of_own, nothing(own_ref)), so_far_ref[...])


def histogram_parts(best, penalty):
    width = 2.0 / (BINS - 1)
    at = jnp.where(penalty < 0.0, 2.0 * BINS, (best + 1.0) * (1.0 / width))
    weights = jnp.maximum(1.0 - jnp.abs(at - iota((BINS, 1), 0).astype(F32)), 0.0)
    folded = weights[:, 0:LANES]
    for s in range(LANES, best.shape[1], LANES):
        folded = folded + weights[:, s : s + LANES]
    return folded


def best_last(own_ref, more_ref, last_ref, so_far_ref, more_so_far_ref, out_ref):
    total = own_ref.shape[0]
    own_penalty, more_penalty = penalties(own_ref), penalties(more_ref)
    penalty = penalties(last_ref)
    columns, rows, of_own = nothing(last_ref), nothing(last_ref), nothing(own_ref)
    of_more = nothing(more_ref)
    between(more_ref, more_penalty, last_ref, penalty, of_more, columns)
    between(last_ref, penalty, own_ref, own_penalty, rows, of_own)
    within(last_ref, penalty, columns, rows)
    best = jnp.maximum(as_line(of_own, nothing(own_ref)), so_far_ref[...])
    more_line = [more_so_far_ref[:, s : s + BLOCK] for s in range(0, more_ref.shape[0], BLOCK)]
    more_best = jnp.maximum(as_line(more_line, of_more), -1.0)
    last_best = jnp.maximum(as_line(columns, rows), -1.0)
    mine = histogram_parts(best, own_penalty[1])
    theirs = histogram_parts(
        jnp.concatenate([more_best, last_best], axis=1),
        jnp.concatenate([more_penalty[1], penalty[1]], axis=1),
    )
    hist = jnp.sum((mine + theirs).T, axis=0, keepdims=True)
    high = best.astype(BF16).astype(F32)
    low = (best - high) * LOW_SCALE
    high = high * HIGH_SCALE
    hist = hist * HIST_SCALE
    sub = iota((8, LANES), 0)
    left = iota((1, LANES), 1) < CAP
    blocks = []
    for s in range(0, total, 2 * LANES):
        block = jnp.broadcast_to(hist, (8, LANES))
        for h in range(2):
            at = s + h * LANES
            top, rest = high[:, at : at + LANES], low[:, at : at + LANES]
            first = jnp.where(left, top, pltpu.roll(rest, CAP, 1))
            second = jnp.where(left, pltpu.roll(top, CAP, 1), rest)
            block = jnp.where(sub == 4 * h + 1, first, block)
            block = jnp.where(sub == 4 * h + 3, second, block)
        blocks.append(block)
    block = jnp.concatenate(blocks, axis=0)
    for at in range(0, out_ref.shape[0], block.shape[0]):
        out_ref[at : at + block.shape[0], :] = block


def pick_results(index_ref, got_ref, best_hbm, hist_hbm, best_ref, hist_ref, sems):
    lines = got_ref.shape[0]
    docs = index_ref.shape[1]
    got = got_ref[...]
    even = lax.bitwise_and(iota((8, LANES), 0), 1) == 0
    total = jnp.zeros((8, LANES), F32)
    for s in range(0, lines, 8):
        total = total + jnp.where(even, got[s : s + 8, :], 0.0)
    total = jnp.sum(total, axis=0, keepdims=True)
    hist_ref[...] = total * (1.0 / (HIST_SCALE * lines * docs))
    hist_copy = pltpu.make_async_copy(hist_ref, hist_hbm, sems.at[0])
    hist_copy.start()
    index = index_ref[...]
    line = lax.shift_right_logical(index, 6) * 2 + 1
    rank = lax.bitwise_and(index, CAP - 1)
    onehot = ones_where(iota((lines, docs), 0) == line)
    turned = got.T
    high = turned.astype(BF16)
    low = (turned - high.astype(F32)).astype(BF16)
    picked = dot(high, onehot) + dot(low, onehot)
    lane = iota((LANES, docs), 0)
    picked = picked * jnp.where(lane < CAP, 1.0 / HIGH_SCALE, 1.0 / LOW_SCALE)
    wanted = lax.bitwise_and(lane, CAP - 1) == rank
    best_ref[...] = jnp.sum(jnp.where(wanted, picked, 0.0), axis=0, keepdims=True)
    best_copy = pltpu.make_async_copy(best_ref, best_hbm, sems.at[1])
    best_copy.start()
    hist_copy.wait()
    best_copy.wait()


VMEM = pl.BlockSpec(memory_space=pltpu.VMEM)
ANY = pl.BlockSpec(memory_space=pl.ANY)


def call(kernel, outs, specs, flops, scratch=(), place=VMEM):
    many = isinstance(outs, tuple)
    return pl.pallas_call(
        kernel,
        out_shape=outs,
        in_specs=specs,
        out_specs=tuple(place for _ in outs) if many else place,
        scratch_shapes=scratch,
        compiler_params=pltpu.CompilerParams(vmem_limit_bytes=24 * 2**20),
        cost_estimate=pl.CostEstimate(flops=flops, bytes_accessed=4000000, transcendentals=0),
    )


def shape(dims, dtype):
    return jax.ShapeDtypeStruct(dims, dtype)


def in_hbm(x):
    return pltpu.with_memory_space_constraint(x, pltpu.HBM)


def exchange(x, axes):
    return lax.all_to_all(x, axes, split_axis=0, concat_axis=0, tiled=True)


def shards(embeddings, document_cluster_index):
    row_count = lax.axis_size(ROWS)
    col_count = lax.axis_size(COLS)
    docs, width = embeddings.shape
    labels = document_cluster_index.reshape(1, docs)
    block = CAP * width // LANES + 8
    sends, rank = call(
        normalise_and_slot,
        (shape((row_count, block, LANES), BF16), shape((1, docs), F32)),
        [ANY, ANY],
        2 * row_count * CAP * docs * width,
        [
            pltpu.VMEM((1, docs), jnp.int32),
            pltpu.VMEM((docs, width), BF16),
            pltpu.SemaphoreType.DMA((2,)),
        ],
    )(in_hbm(labels), in_hbm(embeddings))
    got = exchange(sends, ROWS)
    total = GROUP_CLUSTERS * CAP
    sends = call(reslot, shape((total, width), BF16), [VMEM], 2 * total * row_count * CAP * width)(
        got
    )
    own = exchange(sends.reshape(GROUP_CLUSTERS, CAP, width), CHIPS)
    own, got = lax.optimization_barrier((own.reshape(total, width), got))
    whole, part = shape((1, total), F32), shape((1, BLOCK), F32)
    flops = 2 * total * total // 2 * width
    early = call(best_own_early, whole, [VMEM], flops)(own)
    own, early = lax.optimization_barrier((own, early))
    pairs = [(i, i ^ 1) for i in range(col_count)]
    first = lax.ppermute(own[:BLOCK], COLS, pairs)
    rest = lax.ppermute(own[BLOCK:], COLS, pairs)
    lines = row_count * GROUP_CLUSTERS * 2
    best = call(best_own_late, whole, [VMEM] * 2, flops)(own, early)
    best, more = call(best_more, (whole, part), [VMEM] * 3, flops)(own, first, best)
    index = call(return_index, shape((1, docs), jnp.int32), [VMEM] * 3, 2**26)(labels, rank, got)
    results = call(best_last, shape((lines, LANES), F32), [VMEM] * 5, 2 * flops)(
        own, first, rest, best, more
    )
    results, index = lax.optimization_barrier((results, index))
    results = exchange(results.astype(WIRE).reshape(lines // 2, 2, LANES), SAME_CORE)
    results = results.reshape(lines, LANES).astype(F32)
    outs = (shape((1, docs), F32), shape((1, BINS), F32))
    scratch = [pltpu.VMEM((1, docs), F32), pltpu.VMEM((1, BINS), F32), pltpu.SemaphoreType.DMA((2,))]
    best, hist = call(pick_results, outs, [VMEM, VMEM], 2**26, scratch, ANY)(index, results)
    return (best.reshape(docs), hist.reshape(BINS))


def solution(mesh):
    torus = Mesh(
        mesh.devices.reshape(2, 4, 2, 8, 2), ("rows_0", "rows_1", "cols_0", "cols_1", "cols_2")
    )
    in_specs = (P(ALL, None), P(ALL))
    out_specs = (P(ALL), P())
    return jax.shard_map(
        shards, mesh=torus, in_specs=in_specs, out_specs=out_specs, check_vma=False
    )
```

```python
import jax
import jax.numpy as jnp
from jax import lax
from jax.experimental import pallas as pl
from jax.experimental.pallas import tpu as pltpu
from jax.sharding import Mesh
from jax.sharding import PartitionSpec as P

CAP = 64
GROUP_CLUSTERS = 16
BINS = 128
ROWS = ("rows_1", "rows_0")
COLS = ("cols_0", "cols_1", "cols_2")
CHIPS = ("cols_0", "cols_1")
ALL = ("rows_0", "rows_1") + COLS
SAME_CORE = ROWS + CHIPS
LANES = 128
BLOCK = 256
EMPTY = 2.0
F32 = jnp.float32
BF16 = jnp.bfloat16
WIRE = jnp.float16
HIGH_SCALE = 2.0**10
LOW_SCALE = 2.0**18
HIST_SCALE = 16.0


def iota(shape, dim):
    return lax.broadcasted_iota(jnp.int32, shape, dim)


def dot(a, b):
    return lax.dot_general(a, b, (((1,), (0,)), ((), ())), preferred_element_type=F32)


def dot_t(a, b):
    return lax.dot_general(a, b, (((1,), (1,)), ((), ())), preferred_element_type=F32)


def ones_where(mask):
    return jnp.where(mask, 1.0, 0.0).astype(BF16)


def before(n):
    return ones_where(iota((n, n), 0) < iota((n, n), 1))


def rank_of(onehot, n):
    earlier = dot(onehot, before(n))
    return jnp.sum(onehot.astype(F32) * earlier, axis=0, keepdims=True)


def normalise_and_slot(labels_hbm, embeddings_hbm, out_ref, rank_ref, labels_ref, embeddings_ref, sems):
    labels_copy = pltpu.make_async_copy(labels_hbm, labels_ref, sems.at[0])
    embeddings_copy = pltpu.make_async_copy(embeddings_hbm, embeddings_ref, sems.at[1])
    labels_copy.start()
    embeddings_copy.start()
    docs, width = embeddings_ref.shape
    groups = out_ref.shape[0]
    clusters = groups * GROUP_CLUSTERS
    labels_copy.wait()
    labels = labels_ref[...]
    group = lax.shift_right_logical(labels, 4)
    onehot = ones_where(iota((groups, docs), 0) == group)
    slot = group * CAP + rank_of(onehot, docs).astype(jnp.int32)
    places = ones_where(iota((groups * CAP, docs), 0) == slot)
    shifted = jnp.broadcast_to((labels + 1).astype(F32), (8, docs)).astype(BF16)
    slot_labels = dot_t(shifted, places)
    of_cluster = ones_where(iota((clusters, docs), 0) == labels)
    counts = dot_t(jnp.ones((8, docs), BF16), of_cluster)
    row = iota((8, LANES), 0)
    meta = jnp.where(row == groups * CAP // LANES, counts, 0.0)
    for s in range(groups * CAP // LANES):
        meta = jnp.where(row == s, slot_labels[:, s * LANES : (s + 1) * LANES], meta)
    meta = meta.astype(BF16)
    rank_ref[...] = rank_of(of_cluster, docs)
    embeddings_copy.wait()
    values = embeddings_ref[...].astype(F32)
    total = jnp.sum(values * values, axis=1, keepdims=True)
    normed = (values * lax.rsqrt(total + 1e-06)).astype(BF16)
    rows = dot(places, normed).astype(BF16)
    pieces = width // LANES
    for g in range(groups):
        for f in range(pieces):
            block = rows[g * CAP : (g + 1) * CAP, f * LANES : (f + 1) * LANES]
            out_ref[g, f * CAP : (f + 1) * CAP, :] = block
        out_ref[g, pieces * CAP :, :] = meta


def slot_labels_of(got_ref, me):
    groups = got_ref.shape[0]
    slots = groups * CAP
    at = got_ref.shape[1] - 8
    source = lax.shift_right_logical(iota((8, slots), 1), 6)
    row = iota((8, LANES), 0)
    per_row = LANES // CAP
    picked = []
    for g in range(groups):
        meta = got_ref[g, at:, :].astype(F32)
        line = jnp.where(row == lax.shift_right_logical(me, 1), meta, 0.0)
        picked.append(jnp.sum(line, axis=0, keepdims=True))
    lines = jnp.concatenate(picked, axis=0).astype(BF16)
    lane, to = iota((LANES, slots), 0), iota((LANES, slots), 1)
    start = lax.bitwise_and(me, per_row - 1) * CAP
    move = ones_where(lane == start + lax.bitwise_and(to, CAP - 1))
    spread = jnp.where(iota((groups, slots), 0) == source, dot(lines, move), 0.0)
    return jnp.sum(spread, axis=0, keepdims=True)


def reslot(got_ref, out_ref):
    groups = got_ref.shape[0]
    slots = groups * CAP
    width = out_ref.shape[1]
    me = lax.axis_index(ROWS)
    label = slot_labels_of(got_ref, me).astype(jnp.int32)
    cluster = label - 1 - me * GROUP_CLUSTERS
    onehot = ones_where(iota((GROUP_CLUSTERS, slots), 0) == cluster)
    place = cluster * CAP + rank_of(onehot, slots).astype(jnp.int32)
    place = jnp.where(label > 0, place, -1)
    counts = jnp.sum(onehot.astype(F32), axis=1, keepdims=True).astype(jnp.int32)
    total = GROUP_CLUSTERS * CAP
    step = total // 4
    pieces = width // LANES
    rows = jnp.concatenate(
        [got_ref[:, f * CAP : (f + 1) * CAP, :].reshape(slots, LANES) for f in range(pieces)],
        axis=1,
    )
    lane, rank = iota((CAP, LANES), 1), iota((CAP, LANES), 0)
    marks = []
    for c in range(GROUP_CLUSTERS):
        empty = (rank >= counts[c : c + 1, :]) & (lane == 0)
        marks.append(jnp.where(empty, EMPTY, 0.0))
    for s in range(0, total, step):
        places = ones_where(iota((step, slots), 0) + s == place)
        moved = dot(places, rows)
        out_ref[s : s + step, LANES:] = moved[:, LANES:].astype(BF16)
        mark = jnp.concatenate(marks[s // CAP : (s + step) // CAP], axis=0)
        out_ref[s : s + step, 0:LANES] = (moved[:, 0:LANES] + mark).astype(BF16)


def return_index(labels_ref, rank_ref, got_ref, out_ref):
    groups = got_ref.shape[0]
    docs = labels_ref.shape[1]
    clusters = groups * GROUP_CLUSTERS
    me = lax.axis_index(ROWS)
    at = got_ref.shape[1] - 8
    row = iota((8, LANES), 0)
    before_me = jnp.zeros((8, LANES), F32)
    for g in range(groups):
        before_me = before_me + jnp.where(g < me, got_ref[g, at:, :].astype(F32), 0.0)
    counts = jnp.where(row == groups * CAP // LANES, before_me, 0.0)
    labels = labels_ref[...]
    of_cluster = ones_where(iota((clusters, docs), 0) == labels)
    earlier = jnp.sum(dot(counts.astype(BF16), of_cluster), axis=0, keepdims=True)
    out_ref[...] = labels * CAP + (rank_ref[...] + earlier).astype(jnp.int32)


def column_of(ref):
    return jnp.where(ref[:, 0:1].astype(F32) < 1.5, 0.0, -4.0)


def penalties(ref):
    column = column_of(ref)
    pick = ones_where(iota((8, 256), 1) == 0)
    row = jnp.where(dot_t(pick, ref[:, 0:256])[0:1, :] < 1.5, 0.0, -4.0)
    return column, row


def over_columns(scores):
    return jnp.max(scores.reshape(BLOCK // 8, 8, BLOCK), axis=0)


def over_rows(scores):
    return jnp.maximum(scores[:, :LANES], scores[:, LANES:])


def as_line(columns, rows):
    out = []
    for column, row in zip(columns, rows):
        line = jnp.max(column, axis=0, keepdims=True)
        if row is not None:
            turned = [jnp.max(row[h : h + LANES].T, axis=0, keepdims=True) for h in (0, LANES)]
            line = jnp.maximum(line, jnp.concatenate(turned, axis=1))
        out.append(line)
    return jnp.concatenate(out, axis=1)


def larger(a, b):
    return b if a is None else jnp.maximum(a, b)


def within(ref, penalty, columns, rows):
    column, row = penalty
    count = ref.shape[0] // BLOCK
    for i in range(count):
        for j in range(i, count):
            at, to = i * BLOCK, j * BLOCK
            scores = dot_t(ref[at : at + BLOCK, :], ref[to : to + BLOCK, :])
            scores = scores + column[at : at + BLOCK] + row[:, to : to + BLOCK]
            if i == j:
                other = iota((BLOCK, BLOCK), 0) != iota((BLOCK, BLOCK), 1)
                scores = jnp.where(other, scores, -4.0)
            else:
                rows[i] = larger(rows[i], over_rows(scores))
            columns[j] = larger(columns[j], over_columns(scores))


def between(a_ref, a_penalty, b_ref, b_penalty, rows, columns):
    for i in range(a_ref.shape[0] // BLOCK):
        for j in range(b_ref.shape[0] // BLOCK):
            at, to = i * BLOCK, j * BLOCK
            scores = dot_t(a_ref[at : at + BLOCK, :], b_ref[to : to + BLOCK, :])
            scores = scores + a_penalty[0][at : at + BLOCK] + b_penalty[1][:, to : to + BLOCK]
            rows[i] = larger(rows[i], over_rows(scores))
            columns[j] = larger(columns[j], over_columns(scores))


def nothing(ref):
    return [None] * (ref.shape[0] // BLOCK)


def best_own(own_ref, best_ref, penalty_ref):
    columns, rows = nothing(own_ref), nothing(own_ref)
    penalty = penalties(own_ref)
    within(own_ref, penalty, columns, rows)
    best_ref[...] = jnp.maximum(as_line(columns, rows), -1.0)
    penalty_ref[...] = penalty[1]


def best_more(own_ref, more_ref, so_far_ref, own_row_ref, best_ref, columns_ref, rows_ref):
    columns, rows, of_own = nothing(more_ref), nothing(more_ref), nothing(own_ref)
    penalty = penalties(more_ref)
    between(more_ref, penalty, own_ref, (None, own_row_ref[...]), rows, of_own)
    within(more_ref, penalty, columns, rows)
    columns_ref[...] = jnp.concatenate(columns, axis=1)
    rows_ref[...] = jnp.concatenate(rows, axis=0)
    best_ref[...] = jnp.maximum(as_line(of_own, nothing(own_ref)), so_far_ref[...])


def histogram_parts(best, penalty):
    width = 2.0 / (BINS - 1)
    centers = -1.0 + iota((BINS, 1), 0).astype(F32) * width
    weights = jnp.maximum(1.0 - jnp.abs(best - centers) / width, 0.0)
    weights = jnp.where(penalty < 0.0, 0.0, weights)
    folded = weights[:, 0:LANES]
    for s in range(LANES, best.shape[1], LANES):
        folded = folded + weights[:, s : s + LANES]
    return folded


def best_last(
    own_ref, more_ref, last_ref, so_far_ref, own_row_ref, more_columns_ref, more_rows_ref, out_ref
):
    total = own_ref.shape[0]
    own_penalty, more_penalty = (None, own_row_ref[...]), penalties(more_ref)
    penalty = penalties(last_ref)
    columns, rows, of_own = nothing(last_ref), nothing(last_ref), nothing(own_ref)
    starts = range(0, more_ref.shape[0], BLOCK)
    of_more = [more_rows_ref[s : s + BLOCK, :] for s in starts]
    between(more_ref, more_penalty, last_ref, penalty, of_more, columns)
    between(last_ref, penalty, own_ref, own_penalty, rows, of_own)
    within(last_ref, penalty, columns, rows)
    best = jnp.maximum(as_line(of_own, nothing(own_ref)), so_far_ref[...])
    more_line = [more_columns_ref[:, s : s + BLOCK] for s in starts]
    more_best = jnp.maximum(as_line(more_line, of_more), -1.0)
    last_best = jnp.maximum(as_line(columns, rows), -1.0)
    mine = histogram_parts(best, own_penalty[1])
    theirs = histogram_parts(
        jnp.concatenate([more_best, last_best], axis=1),
        jnp.concatenate([more_penalty[1], penalty[1]], axis=1),
    )
    hist = jnp.sum((mine + theirs).T, axis=0, keepdims=True)
    high = best.astype(BF16).astype(F32)
    low = (best - high) * LOW_SCALE
    high = high * HIGH_SCALE
    hist = hist * HIST_SCALE
    sub = iota((8, LANES), 0)
    left = iota((1, LANES), 1) < CAP
    blocks = []
    for s in range(0, total, 2 * LANES):
        block = jnp.broadcast_to(hist, (8, LANES))
        for h in range(2):
            at = s + h * LANES
            top, rest = high[:, at : at + LANES], low[:, at : at + LANES]
            first = jnp.where(left, top, pltpu.roll(rest, CAP, 1))
            second = jnp.where(left, pltpu.roll(top, CAP, 1), rest)
            block = jnp.where(sub == 4 * h + 1, first, block)
            block = jnp.where(sub == 4 * h + 3, second, block)
        blocks.append(block)
    block = jnp.concatenate(blocks, axis=0)
    for at in range(0, out_ref.shape[0], block.shape[0]):
        out_ref[at : at + block.shape[0], :] = block


def pick_results(index_ref, got_ref, best_ref, hist_ref):
    lines = got_ref.shape[0]
    docs = index_ref.shape[1]
    index = index_ref[...]
    line = lax.shift_right_logical(index, 6) * 2 + 1
    rank = lax.bitwise_and(index, CAP - 1)
    onehot = ones_where(iota((lines, docs), 0) == line)
    got = got_ref[...]
    turned = got.T
    high = turned.astype(BF16)
    low = (turned - high.astype(F32)).astype(BF16)
    picked = dot(high, onehot) + dot(low, onehot)
    lane = iota((LANES, docs), 0)
    picked = picked * jnp.where(lane < CAP, 1.0 / HIGH_SCALE, 1.0 / LOW_SCALE)
    wanted = lax.bitwise_and(lane, CAP - 1) == rank
    best_ref[...] = jnp.sum(jnp.where(wanted, picked, 0.0), axis=0, keepdims=True)
    even = lax.bitwise_and(iota((8, LANES), 0), 1) == 0
    total = jnp.zeros((8, LANES), F32)
    for s in range(0, lines, 8):
        total = total + jnp.where(even, got[s : s + 8, :], 0.0)
    hist_ref[...] = jnp.sum(total, axis=0, keepdims=True) * (1.0 / (HIST_SCALE * lines * docs))


VMEM = pl.BlockSpec(memory_space=pltpu.VMEM)
ANY = pl.BlockSpec(memory_space=pl.ANY)


def call(kernel, outs, specs, flops, scratch=()):
    many = isinstance(outs, tuple)
    return pl.pallas_call(
        kernel,
        out_shape=outs,
        in_specs=specs,
        out_specs=tuple(VMEM for _ in outs) if many else VMEM,
        scratch_shapes=scratch,
        compiler_params=pltpu.CompilerParams(vmem_limit_bytes=24 * 2**20),
        cost_estimate=pl.CostEstimate(flops=flops, bytes_accessed=4000000, transcendentals=0),
    )


def shape(dims, dtype):
    return jax.ShapeDtypeStruct(dims, dtype)


def in_hbm(x):
    return pltpu.with_memory_space_constraint(x, pltpu.HBM)


def exchange(x, axes):
    return lax.all_to_all(x, axes, split_axis=0, concat_axis=0, tiled=True)


def shards(embeddings, document_cluster_index):
    row_count = lax.axis_size(ROWS)
    col_count = lax.axis_size(COLS)
    docs, width = embeddings.shape
    labels = document_cluster_index.reshape(1, docs)
    block = CAP * width // LANES + 8
    sends, rank = call(
        normalise_and_slot,
        (shape((row_count, block, LANES), BF16), shape((1, docs), F32)),
        [ANY, ANY],
        2 * row_count * CAP * docs * width,
        [
            pltpu.VMEM((1, docs), jnp.int32),
            pltpu.VMEM((docs, width), BF16),
            pltpu.SemaphoreType.DMA((2,)),
        ],
    )(in_hbm(labels), in_hbm(embeddings))
    got = exchange(sends, ROWS)
    total = GROUP_CLUSTERS * CAP
    sends = call(reslot, shape((total, width), BF16), [VMEM], 2 * total * row_count * CAP * width)(
        got
    )
    own = exchange(sends.reshape(GROUP_CLUSTERS, CAP, width), CHIPS)
    own, got = lax.optimization_barrier((own.reshape(total, width), got))
    pairs = [(i, i ^ 1) for i in range(col_count)]
    half = total // 2
    other = [lax.ppermute(own[s : s + half], COLS, pairs) for s in (0, half)]
    flops = 2 * total * half * width
    lines = row_count * GROUP_CLUSTERS * 2
    whole = shape((1, total), F32)
    best, own_row = call(best_own, (whole, whole), [VMEM], flops)(own)
    parts = (whole, shape((8, half), F32), shape((half, LANES), F32))
    best, more_columns, more_rows = call(best_more, parts, [VMEM] * 4, flops)(
        own, other[0], best, own_row
    )
    index = call(return_index, shape((1, docs), jnp.int32), [VMEM] * 3, 2**26)(labels, rank, got)
    results = call(best_last, shape((lines, LANES), F32), [VMEM] * 7, 2 * flops)(
        own, other[0], other[1], best, own_row, more_columns, more_rows
    )
    results, index = lax.optimization_barrier((results, index))
    results = exchange(results.astype(WIRE).reshape(lines // 2, 2, LANES), SAME_CORE)
    results = results.reshape(lines, LANES).astype(F32)
    best, hist = call(
        pick_results, (shape((1, docs), F32), shape((1, BINS), F32)), [VMEM, VMEM], 2**26
    )(index, results)
    return (best.reshape(docs), hist.reshape(BINS))


def solution(mesh):
    torus = Mesh(
        mesh.devices.reshape(2, 4, 2, 8, 2), ("rows_0", "rows_1", "cols_0", "cols_1", "cols_2")
    )
    in_specs = (P(ALL, None), P(ALL))
    out_specs = (P(ALL), P())
    return jax.shard_map(
        shards, mesh=torus, in_specs=in_specs, out_specs=out_specs, check_vma=False
    )
```

```python
import jax
import jax.numpy as jnp
from jax import lax
from jax.experimental import pallas as pl
from jax.experimental.pallas import tpu as pltpu
from jax.sharding import Mesh
from jax.sharding import PartitionSpec as P

CAP = 64
GROUP_CLUSTERS = 16
BINS = 128
ROWS = ("rows_1", "rows_0")
COLS = ("cols_0", "cols_1", "cols_2")
CHIPS = ("cols_0", "cols_1")
ALL = ("rows_0", "rows_1") + COLS
SAME_CORE = ROWS + CHIPS
LANES = 128
BLOCK = 256
EMPTY = 2.0
F32 = jnp.float32
BF16 = jnp.bfloat16
WIRE = jnp.float16
HIGH_SCALE = 2.0**10
LOW_SCALE = 2.0**18
HIST_SCALE = 16.0


def iota(shape, dim):
    return lax.broadcasted_iota(jnp.int32, shape, dim)


def dot(a, b):
    return lax.dot_general(a, b, (((1,), (0,)), ((), ())), preferred_element_type=F32)


def dot_t(a, b):
    return lax.dot_general(a, b, (((1,), (1,)), ((), ())), preferred_element_type=F32)


def ones_where(mask):
    return jnp.where(mask, 1.0, 0.0).astype(BF16)


def before(n):
    return ones_where(iota((n, n), 0) < iota((n, n), 1))


def rank_of(onehot, n):
    earlier = dot(onehot, before(n))
    return jnp.sum(onehot.astype(F32) * earlier, axis=0, keepdims=True)


def normalise_and_slot(labels_hbm, embeddings_hbm, out_ref, rank_ref, labels_ref, embeddings_ref, sems):
    labels_copy = pltpu.make_async_copy(labels_hbm, labels_ref, sems.at[0])
    embeddings_copy = pltpu.make_async_copy(embeddings_hbm, embeddings_ref, sems.at[1])
    labels_copy.start()
    embeddings_copy.start()
    docs, width = embeddings_ref.shape
    groups = out_ref.shape[0]
    clusters = groups * GROUP_CLUSTERS
    labels_copy.wait()
    labels = labels_ref[...]
    group = lax.shift_right_logical(labels, 4)
    onehot = ones_where(iota((groups, docs), 0) == group)
    slot = group * CAP + rank_of(onehot, docs).astype(jnp.int32)
    places = ones_where(iota((groups * CAP, docs), 0) == slot)
    shifted = jnp.broadcast_to((labels + 1).astype(F32), (8, docs)).astype(BF16)
    slot_labels = dot_t(shifted, places)
    of_cluster = ones_where(iota((clusters, docs), 0) == labels)
    counts = dot_t(jnp.ones((8, docs), BF16), of_cluster)
    row = iota((8, LANES), 0)
    meta = jnp.where(row == groups * CAP // LANES, counts, 0.0)
    for s in range(groups * CAP // LANES):
        meta = jnp.where(row == s, slot_labels[:, s * LANES : (s + 1) * LANES], meta)
    meta = meta.astype(BF16)
    rank_ref[...] = rank_of(of_cluster, docs)
    embeddings_copy.wait()
    values = embeddings_ref[...].astype(F32)
    total = jnp.sum(values * values, axis=1, keepdims=True)
    normed = (values * lax.rsqrt(total + 1e-06)).astype(BF16)
    rows = dot(places, normed).astype(BF16)
    pieces = width // LANES
    for g in range(groups):
        for f in range(pieces):
            block = rows[g * CAP : (g + 1) * CAP, f * LANES : (f + 1) * LANES]
            out_ref[g, f * CAP : (f + 1) * CAP, :] = block
        out_ref[g, pieces * CAP :, :] = meta


def slot_labels_of(got_ref, me):
    groups = got_ref.shape[0]
    slots = groups * CAP
    at = got_ref.shape[1] - 8
    source = lax.shift_right_logical(iota((8, slots), 1), 6)
    row = iota((8, LANES), 0)
    per_row = LANES // CAP
    picked = []
    for g in range(groups):
        meta = got_ref[g, at:, :].astype(F32)
        line = jnp.where(row == lax.shift_right_logical(me, 1), meta, 0.0)
        picked.append(jnp.sum(line, axis=0, keepdims=True))
    lines = jnp.concatenate(picked, axis=0).astype(BF16)
    lane, to = iota((LANES, slots), 0), iota((LANES, slots), 1)
    start = lax.bitwise_and(me, per_row - 1) * CAP
    move = ones_where(lane == start + lax.bitwise_and(to, CAP - 1))
    spread = jnp.where(iota((groups, slots), 0) == source, dot(lines, move), 0.0)
    return jnp.sum(spread, axis=0, keepdims=True)


def reslot(got_ref, out_ref):
    groups = got_ref.shape[0]
    slots = groups * CAP
    width = out_ref.shape[1]
    me = lax.axis_index(ROWS)
    label = slot_labels_of(got_ref, me).astype(jnp.int32)
    cluster = label - 1 - me * GROUP_CLUSTERS
    onehot = ones_where(iota((GROUP_CLUSTERS, slots), 0) == cluster)
    place = cluster * CAP + rank_of(onehot, slots).astype(jnp.int32)
    place = jnp.where(label > 0, place, -1)
    counts = jnp.sum(onehot.astype(F32), axis=1, keepdims=True).astype(jnp.int32)
    total = GROUP_CLUSTERS * CAP
    step = total // 4
    pieces = width // LANES
    rows = jnp.concatenate(
        [got_ref[:, f * CAP : (f + 1) * CAP, :].reshape(slots, LANES) for f in range(pieces)],
        axis=1,
    )
    lane, rank = iota((CAP, LANES), 1), iota((CAP, LANES), 0)
    marks = []
    for c in range(GROUP_CLUSTERS):
        empty = (rank >= counts[c : c + 1, :]) & (lane == 0)
        marks.append(jnp.where(empty, EMPTY, 0.0))
    for s in range(0, total, step):
        places = ones_where(iota((step, slots), 0) + s == place)
        moved = dot(places, rows)
        out_ref[s : s + step, LANES:] = moved[:, LANES:].astype(BF16)
        mark = jnp.concatenate(marks[s // CAP : (s + step) // CAP], axis=0)
        out_ref[s : s + step, 0:LANES] = (moved[:, 0:LANES] + mark).astype(BF16)


def return_index(labels_ref, rank_ref, got_ref, out_ref):
    groups = got_ref.shape[0]
    docs = labels_ref.shape[1]
    clusters = groups * GROUP_CLUSTERS
    me = lax.axis_index(ROWS)
    at = got_ref.shape[1] - 8
    row = iota((8, LANES), 0)
    before_me = jnp.zeros((8, LANES), F32)
    for g in range(groups):
        before_me = before_me + jnp.where(g < me, got_ref[g, at:, :].astype(F32), 0.0)
    counts = jnp.where(row == groups * CAP // LANES, before_me, 0.0)
    labels = labels_ref[...]
    of_cluster = ones_where(iota((clusters, docs), 0) == labels)
    earlier = jnp.sum(dot(counts.astype(BF16), of_cluster), axis=0, keepdims=True)
    out_ref[...] = labels * CAP + (rank_ref[...] + earlier).astype(jnp.int32)


def column_of(ref):
    return jnp.where(ref[:, 0:1].astype(F32) < 1.5, 0.0, -4.0)


def penalties(ref):
    column = column_of(ref)
    pick = ones_where(iota((8, 256), 1) == 0)
    row = jnp.where(dot_t(pick, ref[:, 0:256])[0:1, :] < 1.5, 0.0, -4.0)
    return column, row


def over_columns(scores):
    return jnp.max(scores.reshape(BLOCK // 8, 8, BLOCK), axis=0)


def over_rows(scores):
    return jnp.maximum(scores[:, :LANES], scores[:, LANES:])


def as_line(columns, rows):
    out = []
    for column, row in zip(columns, rows):
        line = jnp.max(column, axis=0, keepdims=True)
        if row is not None:
            turned = [jnp.max(row[h : h + LANES].T, axis=0, keepdims=True) for h in (0, LANES)]
            line = jnp.maximum(line, jnp.concatenate(turned, axis=1))
        out.append(line)
    return jnp.concatenate(out, axis=1)


def larger(a, b):
    return b if a is None else jnp.maximum(a, b)


def within(ref, penalty, columns, rows):
    column, row = penalty
    count = ref.shape[0] // BLOCK
    for i in range(count):
        for j in range(i, count):
            at, to = i * BLOCK, j * BLOCK
            scores = dot_t(ref[at : at + BLOCK, :], ref[to : to + BLOCK, :])
            scores = scores + column[at : at + BLOCK] + row[:, to : to + BLOCK]
            if i == j:
                other = iota((BLOCK, BLOCK), 0) != iota((BLOCK, BLOCK), 1)
                scores = jnp.where(other, scores, -4.0)
            else:
                rows[i] = larger(rows[i], over_rows(scores))
            columns[j] = larger(columns[j], over_columns(scores))


def between(a_ref, a_penalty, b_ref, b_penalty, rows, columns):
    for i in range(a_ref.shape[0] // BLOCK):
        for j in range(b_ref.shape[0] // BLOCK):
            at, to = i * BLOCK, j * BLOCK
            scores = dot_t(a_ref[at : at + BLOCK, :], b_ref[to : to + BLOCK, :])
            scores = scores + a_penalty[0][at : at + BLOCK] + b_penalty[1][:, to : to + BLOCK]
            rows[i] = larger(rows[i], over_rows(scores))
            columns[j] = larger(columns[j], over_columns(scores))


def nothing(ref):
    return [None] * (ref.shape[0] // BLOCK)


def best_own(own_ref, found_ref):
    columns, rows = nothing(own_ref), nothing(own_ref)
    penalty = penalties(own_ref)
    within(own_ref, penalty, columns, rows)
    found_ref[0:1, :] = jnp.maximum(as_line(columns, rows), -1.0)
    found_ref[1:2, :] = penalty[1]


def best_more(own_ref, more_ref, found_ref, best_ref, rows_ref):
    rows, of_own = nothing(more_ref), nothing(own_ref)
    penalty = (column_of(more_ref), None)
    between(more_ref, penalty, own_ref, (None, found_ref[1:2, :]), rows, of_own)
    rows_ref[...] = jnp.concatenate(rows, axis=0)
    best_ref[...] = jnp.maximum(as_line(of_own, nothing(own_ref)), found_ref[0:1, :])


def histogram_parts(best, penalty):
    width = 2.0 / (BINS - 1)
    centers = -1.0 + iota((BINS, 1), 0).astype(F32) * width
    weights = jnp.maximum(1.0 - jnp.abs(best - centers) / width, 0.0)
    weights = jnp.where(penalty < 0.0, 0.0, weights)
    folded = weights[:, 0:LANES]
    for s in range(LANES, best.shape[1], LANES):
        folded = folded + weights[:, s : s + LANES]
    return folded


def best_last(
    own_ref, last_ref, so_far_ref, found_ref, more_rows_ref, theirs_ref, out_ref
):
    total = own_ref.shape[0]
    own_penalty = (None, found_ref[1:2, :])
    rows, of_own = nothing(last_ref), nothing(own_ref)
    starts = range(0, more_rows_ref.shape[0], BLOCK)
    more_rows = [more_rows_ref[s : s + BLOCK, :] for s in starts]
    between(last_ref, (column_of(last_ref), None), own_ref, own_penalty, rows, of_own)
    best = jnp.maximum(as_line(of_own, nothing(own_ref)), so_far_ref[...])
    rows = more_rows + rows
    their_line = [theirs_ref[0:1, s : s + BLOCK] for s in range(0, total, BLOCK)]
    their_best = as_line(their_line, rows)
    mine = histogram_parts(best, own_penalty[1])
    theirs = histogram_parts(their_best, theirs_ref[1:2, :])
    hist = jnp.sum((mine + theirs).T, axis=0, keepdims=True)
    high = best.astype(BF16).astype(F32)
    low = (best - high) * LOW_SCALE
    high = high * HIGH_SCALE
    hist = hist * HIST_SCALE
    sub = iota((8, LANES), 0)
    left = iota((1, LANES), 1) < CAP
    blocks = []
    for s in range(0, total, 2 * LANES):
        block = jnp.broadcast_to(hist, (8, LANES))
        for h in range(2):
            at = s + h * LANES
            top, rest = high[:, at : at + LANES], low[:, at : at + LANES]
            first = jnp.where(left, top, pltpu.roll(rest, CAP, 1))
            second = jnp.where(left, pltpu.roll(top, CAP, 1), rest)
            block = jnp.where(sub == 4 * h + 1, first, block)
            block = jnp.where(sub == 4 * h + 3, second, block)
        blocks.append(block)
    block = jnp.concatenate(blocks, axis=0)
    for at in range(0, out_ref.shape[0], block.shape[0]):
        out_ref[at : at + block.shape[0], :] = block


def pick_results(index_ref, got_ref, best_ref, hist_ref):
    lines = got_ref.shape[0]
    docs = index_ref.shape[1]
    index = index_ref[...]
    line = lax.shift_right_logical(index, 6) * 2 + 1
    rank = lax.bitwise_and(index, CAP - 1)
    onehot = ones_where(iota((lines, docs), 0) == line)
    got = got_ref[...]
    turned = got.T
    high = turned.astype(BF16)
    low = (turned - high.astype(F32)).astype(BF16)
    picked = dot(high, onehot) + dot(low, onehot)
    lane = iota((LANES, docs), 0)
    picked = picked * jnp.where(lane < CAP, 1.0 / HIGH_SCALE, 1.0 / LOW_SCALE)
    wanted = lax.bitwise_and(lane, CAP - 1) == rank
    best_ref[...] = jnp.sum(jnp.where(wanted, picked, 0.0), axis=0, keepdims=True)
    even = lax.bitwise_and(iota((8, LANES), 0), 1) == 0
    total = jnp.zeros((8, LANES), F32)
    for s in range(0, lines, 8):
        total = total + jnp.where(even, got[s : s + 8, :], 0.0)
    hist_ref[...] = jnp.sum(total, axis=0, keepdims=True) * (1.0 / (HIST_SCALE * lines * docs))


VMEM = pl.BlockSpec(memory_space=pltpu.VMEM)
ANY = pl.BlockSpec(memory_space=pl.ANY)


def call(kernel, outs, specs, flops, scratch=()):
    many = isinstance(outs, tuple)
    return pl.pallas_call(
        kernel,
        out_shape=outs,
        in_specs=specs,
        out_specs=tuple(VMEM for _ in outs) if many else VMEM,
        scratch_shapes=scratch,
        compiler_params=pltpu.CompilerParams(vmem_limit_bytes=24 * 2**20),
        cost_estimate=pl.CostEstimate(flops=flops, bytes_accessed=4000000, transcendentals=0),
    )


def shape(dims, dtype):
    return jax.ShapeDtypeStruct(dims, dtype)


def in_hbm(x):
    return pltpu.with_memory_space_constraint(x, pltpu.HBM)


def exchange(x, axes):
    return lax.all_to_all(x, axes, split_axis=0, concat_axis=0, tiled=True)


def shards(embeddings, document_cluster_index):
    row_count = lax.axis_size(ROWS)
    col_count = lax.axis_size(COLS)
    docs, width = embeddings.shape
    labels = document_cluster_index.reshape(1, docs)
    block = CAP * width // LANES + 8
    sends, rank = call(
        normalise_and_slot,
        (shape((row_count, block, LANES), BF16), shape((1, docs), F32)),
        [ANY, ANY],
        2 * row_count * CAP * docs * width,
        [
            pltpu.VMEM((1, docs), jnp.int32),
            pltpu.VMEM((docs, width), BF16),
            pltpu.SemaphoreType.DMA((2,)),
        ],
    )(in_hbm(labels), in_hbm(embeddings))
    got = exchange(sends, ROWS)
    total = GROUP_CLUSTERS * CAP
    sends = call(reslot, shape((total, width), BF16), [VMEM], 2 * total * row_count * CAP * width)(
        got
    )
    own = exchange(sends.reshape(GROUP_CLUSTERS, CAP, width), CHIPS)
    own, got = lax.optimization_barrier((own.reshape(total, width), got))
    pairs = [(i, i ^ 1) for i in range(col_count)]
    half = total // 2
    other = [lax.ppermute(own[s : s + half], COLS, pairs) for s in (0, half)]
    flops = 2 * total * half * width
    lines = row_count * GROUP_CLUSTERS * 2
    found = call(best_own, shape((2, total), F32), [VMEM], flops)(own)
    theirs = lax.ppermute(found, COLS, pairs)
    parts = (shape((1, total), F32), shape((half, LANES), F32))
    best, more_rows = call(best_more, parts, [VMEM] * 3, flops)(own, other[0], found)
    index = call(return_index, shape((1, docs), jnp.int32), [VMEM] * 3, 2**26)(labels, rank, got)
    results = call(best_last, shape((lines, LANES), F32), [VMEM] * 6, flops)(
        own, other[1], best, found, more_rows, theirs
    )
    results, index = lax.optimization_barrier((results, index))
    results = exchange(results.astype(WIRE).reshape(lines // 2, 2, LANES), SAME_CORE)
    results = results.reshape(lines, LANES).astype(F32)
    best, hist = call(
        pick_results, (shape((1, docs), F32), shape((1, BINS), F32)), [VMEM, VMEM], 2**26
    )(index, results)
    return (best.reshape(docs), hist.reshape(BINS))


def solution(mesh):
    torus = Mesh(
        mesh.devices.reshape(2, 4, 2, 8, 2), ("rows_0", "rows_1", "cols_0", "cols_1", "cols_2")
    )
    in_specs = (P(ALL, None), P(ALL))
    out_specs = (P(ALL), P())
    return jax.shard_map(
        shards, mesh=torus, in_specs=in_specs, out_specs=out_specs, check_vma=False
    )
```

```python
import jax
import jax.numpy as jnp
from jax import lax
from jax.experimental import pallas as pl
from jax.experimental.pallas import tpu as pltpu
from jax.sharding import Mesh
from jax.sharding import PartitionSpec as P

CAP = 64
GROUP_CLUSTERS = 16
BINS = 128
ROWS = ("rows_1", "rows_0")
COLS = ("cols_0", "cols_1", "cols_2")
CHIPS = ("cols_0", "cols_1")
ALL = ("rows_0", "rows_1") + COLS
SAME_CORE = ROWS + CHIPS
LANES = 128
BLOCK = 256
EMPTY = 2.0
F32 = jnp.float32
BF16 = jnp.bfloat16
WIRE = jnp.float16
HIGH_SCALE = 2.0**10
LOW_SCALE = 2.0**18
HIST_SCALE = 16.0


def iota(shape, dim):
    return lax.broadcasted_iota(jnp.int32, shape, dim)


def dot(a, b):
    return lax.dot_general(a, b, (((1,), (0,)), ((), ())), preferred_element_type=F32)


def dot_t(a, b):
    return lax.dot_general(a, b, (((1,), (1,)), ((), ())), preferred_element_type=F32)


def ones_where(mask):
    return jnp.where(mask, 1.0, 0.0).astype(BF16)


def before(n):
    return ones_where(iota((n, n), 0) < iota((n, n), 1))


def rank_of(onehot, n):
    earlier = dot(onehot, before(n))
    return jnp.sum(onehot.astype(F32) * earlier, axis=0, keepdims=True)


def normalise_and_slot(labels_hbm, embeddings_hbm, out_ref, rank_ref, labels_ref, embeddings_ref, sems):
    labels_copy = pltpu.make_async_copy(labels_hbm, labels_ref, sems.at[0])
    embeddings_copy = pltpu.make_async_copy(embeddings_hbm, embeddings_ref, sems.at[1])
    labels_copy.start()
    embeddings_copy.start()
    docs, width = embeddings_ref.shape
    groups = out_ref.shape[0]
    clusters = groups * GROUP_CLUSTERS
    labels_copy.wait()
    labels = labels_ref[...]
    group = lax.shift_right_logical(labels, 4)
    onehot = ones_where(iota((groups, docs), 0) == group)
    slot = group * CAP + rank_of(onehot, docs).astype(jnp.int32)
    places = ones_where(iota((groups * CAP, docs), 0) == slot)
    shifted = jnp.broadcast_to((labels + 1).astype(F32), (8, docs)).astype(BF16)
    slot_labels = dot_t(shifted, places)
    of_cluster = ones_where(iota((clusters, docs), 0) == labels)
    counts = dot_t(jnp.ones((8, docs), BF16), of_cluster)
    row = iota((8, LANES), 0)
    meta = jnp.where(row == groups * CAP // LANES, counts, 0.0)
    for s in range(groups * CAP // LANES):
        meta = jnp.where(row == s, slot_labels[:, s * LANES : (s + 1) * LANES], meta)
    meta = meta.astype(BF16)
    rank_ref[...] = rank_of(of_cluster, docs)
    embeddings_copy.wait()
    values = embeddings_ref[...].astype(F32)
    total = jnp.sum(values * values, axis=1, keepdims=True)
    normed = (values * lax.rsqrt(total + 1e-06)).astype(BF16)
    rows = dot(places, normed).astype(BF16)
    pieces = width // LANES
    for g in range(groups):
        for f in range(pieces):
            block = rows[g * CAP : (g + 1) * CAP, f * LANES : (f + 1) * LANES]
            out_ref[g, f * CAP : (f + 1) * CAP, :] = block
        out_ref[g, pieces * CAP :, :] = meta


def slot_labels_of(got_ref, me):
    groups = got_ref.shape[0]
    slots = groups * CAP
    at = got_ref.shape[1] - 8
    source = lax.shift_right_logical(iota((8, slots), 1), 6)
    row = iota((8, LANES), 0)
    per_row = LANES // CAP
    picked = []
    for g in range(groups):
        meta = got_ref[g, at:, :].astype(F32)
        line = jnp.where(row == lax.shift_right_logical(me, 1), meta, 0.0)
        picked.append(jnp.sum(line, axis=0, keepdims=True))
    lines = jnp.concatenate(picked, axis=0).astype(BF16)
    lane, to = iota((LANES, slots), 0), iota((LANES, slots), 1)
    start = lax.bitwise_and(me, per_row - 1) * CAP
    move = ones_where(lane == start + lax.bitwise_and(to, CAP - 1))
    spread = jnp.where(iota((groups, slots), 0) == source, dot(lines, move), 0.0)
    return jnp.sum(spread, axis=0, keepdims=True)


def reslot(got_ref, out_ref):
    groups = got_ref.shape[0]
    slots = groups * CAP
    width = out_ref.shape[1]
    me = lax.axis_index(ROWS)
    label = slot_labels_of(got_ref, me).astype(jnp.int32)
    cluster = label - 1 - me * GROUP_CLUSTERS
    onehot = ones_where(iota((GROUP_CLUSTERS, slots), 0) == cluster)
    place = cluster * CAP + rank_of(onehot, slots).astype(jnp.int32)
    place = jnp.where(label > 0, place, -1)
    counts = jnp.sum(onehot.astype(F32), axis=1, keepdims=True).astype(jnp.int32)
    total = GROUP_CLUSTERS * CAP
    step = total // 4
    pieces = width // LANES
    rows = jnp.concatenate(
        [got_ref[:, f * CAP : (f + 1) * CAP, :].reshape(slots, LANES) for f in range(pieces)],
        axis=1,
    )
    lane, rank = iota((CAP, LANES), 1), iota((CAP, LANES), 0)
    marks = []
    for c in range(GROUP_CLUSTERS):
        empty = (rank >= counts[c : c + 1, :]) & (lane == 0)
        marks.append(jnp.where(empty, EMPTY, 0.0))
    for s in range(0, total, step):
        places = ones_where(iota((step, slots), 0) + s == place)
        moved = dot(places, rows)
        out_ref[s : s + step, LANES:] = moved[:, LANES:].astype(BF16)
        mark = jnp.concatenate(marks[s // CAP : (s + step) // CAP], axis=0)
        out_ref[s : s + step, 0:LANES] = (moved[:, 0:LANES] + mark).astype(BF16)


def return_index(labels_ref, rank_ref, got_ref, out_ref):
    groups = got_ref.shape[0]
    docs = labels_ref.shape[1]
    clusters = groups * GROUP_CLUSTERS
    me = lax.axis_index(ROWS)
    at = got_ref.shape[1] - 8
    row = iota((8, LANES), 0)
    before_me = jnp.zeros((8, LANES), F32)
    for g in range(groups):
        before_me = before_me + jnp.where(g < me, got_ref[g, at:, :].astype(F32), 0.0)
    counts = jnp.where(row == groups * CAP // LANES, before_me, 0.0)
    labels = labels_ref[...]
    of_cluster = ones_where(iota((clusters, docs), 0) == labels)
    earlier = jnp.sum(dot(counts.astype(BF16), of_cluster), axis=0, keepdims=True)
    out_ref[...] = labels * CAP + (rank_ref[...] + earlier).astype(jnp.int32)


def column_of(ref):
    return jnp.where(ref[:, 0:1].astype(F32) < 1.5, 0.0, -4.0)


def penalties(ref):
    column = column_of(ref)
    pick = ones_where(iota((8, 256), 1) == 0)
    row = jnp.where(dot_t(pick, ref[:, 0:256])[0:1, :] < 1.5, 0.0, -4.0)
    return column, row


def over_columns(scores):
    return jnp.max(scores.reshape(BLOCK // 8, 8, BLOCK), axis=0)


def over_rows(scores):
    return jnp.maximum(scores[:, :LANES], scores[:, LANES:])


def as_line(columns, rows):
    out = []
    for column, row in zip(columns, rows):
        line = jnp.max(column, axis=0, keepdims=True)
        if row is not None:
            turned = [jnp.max(row[h : h + LANES].T, axis=0, keepdims=True) for h in (0, LANES)]
            line = jnp.maximum(line, jnp.concatenate(turned, axis=1))
        out.append(line)
    return jnp.concatenate(out, axis=1)


def larger(a, b):
    return b if a is None else jnp.maximum(a, b)


def within(ref, penalty, columns, rows):
    column, row = penalty
    count = ref.shape[0] // BLOCK
    for i in range(count):
        for j in range(i, count):
            at, to = i * BLOCK, j * BLOCK
            scores = dot_t(ref[at : at + BLOCK, :], ref[to : to + BLOCK, :])
            scores = scores + column[at : at + BLOCK] + row[:, to : to + BLOCK]
            if i == j:
                other = iota((BLOCK, BLOCK), 0) != iota((BLOCK, BLOCK), 1)
                scores = jnp.where(other, scores, -4.0)
            else:
                rows[i] = larger(rows[i], over_rows(scores))
            columns[j] = larger(columns[j], over_columns(scores))


def between(a_ref, a_penalty, b_ref, b_penalty, rows, columns):
    for i in range(a_ref.shape[0] // BLOCK):
        for j in range(b_ref.shape[0] // BLOCK):
            at, to = i * BLOCK, j * BLOCK
            scores = dot_t(a_ref[at : at + BLOCK, :], b_ref[to : to + BLOCK, :])
            scores = scores + a_penalty[0][at : at + BLOCK] + b_penalty[1][:, to : to + BLOCK]
            rows[i] = larger(rows[i], over_rows(scores))
            columns[j] = larger(columns[j], over_columns(scores))


def nothing(ref):
    return [None] * (ref.shape[0] // BLOCK)


def best_own(own_ref, found_ref):
    columns, rows = nothing(own_ref), nothing(own_ref)
    penalty = penalties(own_ref)
    within(own_ref, penalty, columns, rows)
    found_ref[0:1, :] = jnp.maximum(as_line(columns, rows), -1.0)
    found_ref[1:2, :] = penalty[1]


def best_own_early(own_ref, found_ref):
    early = lax.axis_index("cols_2") == 1

    @pl.when(early)
    def _():
        best_own(own_ref, found_ref)

    @pl.when(jnp.logical_not(early))
    def _():
        found_ref[...] = jnp.full(found_ref.shape, -1.0, F32)


def best_own_late(own_ref, early_ref, labels_ref, rank_ref, got_ref, found_ref, index_ref):
    early = lax.axis_index("cols_2") == 1
    return_index(labels_ref, rank_ref, got_ref, index_ref)

    @pl.when(early)
    def _():
        found_ref[...] = early_ref[...]

    @pl.when(jnp.logical_not(early))
    def _():
        best_own(own_ref, found_ref)


def best_more(own_ref, more_ref, found_ref, best_ref, rows_ref):
    rows, of_own = nothing(more_ref), nothing(own_ref)
    penalty = (column_of(more_ref), None)
    between(more_ref, penalty, own_ref, (None, found_ref[1:2, :]), rows, of_own)
    rows_ref[...] = jnp.concatenate(rows, axis=0)
    best_ref[...] = jnp.maximum(as_line(of_own, nothing(own_ref)), found_ref[0:1, :])


def histogram_parts(best, penalty):
    width = 2.0 / (BINS - 1)
    centers = -1.0 + iota((BINS, 1), 0).astype(F32) * width
    weights = jnp.maximum(1.0 - jnp.abs(best - centers) / width, 0.0)
    weights = jnp.where(penalty < 0.0, 0.0, weights)
    folded = weights[:, 0:LANES]
    for s in range(LANES, best.shape[1], LANES):
        folded = folded + weights[:, s : s + LANES]
    return folded


def best_last(
    own_ref, last_ref, so_far_ref, found_ref, more_rows_ref, theirs_ref, out_ref
):
    total = own_ref.shape[0]
    own_penalty = (None, found_ref[1:2, :])
    rows, of_own = nothing(last_ref), nothing(own_ref)
    starts = range(0, more_rows_ref.shape[0], BLOCK)
    more_rows = [more_rows_ref[s : s + BLOCK, :] for s in starts]
    between(last_ref, (column_of(last_ref), None), own_ref, own_penalty, rows, of_own)
    best = jnp.maximum(as_line(of_own, nothing(own_ref)), so_far_ref[...])
    rows = more_rows + rows
    their_line = [theirs_ref[0:1, s : s + BLOCK] for s in range(0, total, BLOCK)]
    their_best = as_line(their_line, rows)
    mine = histogram_parts(best, own_penalty[1])
    theirs = histogram_parts(their_best, theirs_ref[1:2, :])
    hist = jnp.sum((mine + theirs).T, axis=0, keepdims=True)
    high = best.astype(BF16).astype(F32)
    low = (best - high) * LOW_SCALE
    high = high * HIGH_SCALE
    hist = hist * HIST_SCALE
    sub = iota((8, LANES), 0)
    left = iota((1, LANES), 1) < CAP
    blocks = []
    for s in range(0, total, 2 * LANES):
        block = jnp.broadcast_to(hist, (8, LANES))
        for h in range(2):
            at = s + h * LANES
            top, rest = high[:, at : at + LANES], low[:, at : at + LANES]
            first = jnp.where(left, top, pltpu.roll(rest, CAP, 1))
            second = jnp.where(left, pltpu.roll(top, CAP, 1), rest)
            block = jnp.where(sub == 4 * h + 1, first, block)
            block = jnp.where(sub == 4 * h + 3, second, block)
        blocks.append(block)
    block = jnp.concatenate(blocks, axis=0)
    for at in range(0, out_ref.shape[0], block.shape[0]):
        out_ref[at : at + block.shape[0], :] = block


def pick_results(index_ref, got_ref, best_ref, hist_ref):
    lines = got_ref.shape[0]
    docs = index_ref.shape[1]
    index = index_ref[...]
    line = lax.shift_right_logical(index, 6) * 2 + 1
    rank = lax.bitwise_and(index, CAP - 1)
    onehot = ones_where(iota((lines, docs), 0) == line)
    got = got_ref[...]
    turned = got.T
    high = turned.astype(BF16)
    low = (turned - high.astype(F32)).astype(BF16)
    picked = dot(high, onehot) + dot(low, onehot)
    lane = iota((LANES, docs), 0)
    picked = picked * jnp.where(lane < CAP, 1.0 / HIGH_SCALE, 1.0 / LOW_SCALE)
    wanted = lax.bitwise_and(lane, CAP - 1) == rank
    best_ref[...] = jnp.sum(jnp.where(wanted, picked, 0.0), axis=0, keepdims=True)
    even = lax.bitwise_and(iota((8, LANES), 0), 1) == 0
    total = jnp.zeros((8, LANES), F32)
    for s in range(0, lines, 8):
        total = total + jnp.where(even, got[s : s + 8, :], 0.0)
    hist_ref[...] = jnp.sum(total, axis=0, keepdims=True) * (1.0 / (HIST_SCALE * lines * docs))


VMEM = pl.BlockSpec(memory_space=pltpu.VMEM)
ANY = pl.BlockSpec(memory_space=pl.ANY)


def call(kernel, outs, specs, flops, scratch=()):
    many = isinstance(outs, tuple)
    return pl.pallas_call(
        kernel,
        out_shape=outs,
        in_specs=specs,
        out_specs=tuple(VMEM for _ in outs) if many else VMEM,
        scratch_shapes=scratch,
        compiler_params=pltpu.CompilerParams(vmem_limit_bytes=24 * 2**20),
        cost_estimate=pl.CostEstimate(flops=flops, bytes_accessed=4000000, transcendentals=0),
    )


def shape(dims, dtype):
    return jax.ShapeDtypeStruct(dims, dtype)


def in_hbm(x):
    return pltpu.with_memory_space_constraint(x, pltpu.HBM)


def exchange(x, axes):
    return lax.all_to_all(x, axes, split_axis=0, concat_axis=0, tiled=True)


def shards(embeddings, document_cluster_index):
    row_count = lax.axis_size(ROWS)
    col_count = lax.axis_size(COLS)
    docs, width = embeddings.shape
    labels = document_cluster_index.reshape(1, docs)
    block = CAP * width // LANES + 8
    sends, rank = call(
        normalise_and_slot,
        (shape((row_count, block, LANES), BF16), shape((1, docs), F32)),
        [ANY, ANY],
        2 * row_count * CAP * docs * width,
        [
            pltpu.VMEM((1, docs), jnp.int32),
            pltpu.VMEM((docs, width), BF16),
            pltpu.SemaphoreType.DMA((2,)),
        ],
    )(in_hbm(labels), in_hbm(embeddings))
    got = exchange(sends, ROWS)
    total = GROUP_CLUSTERS * CAP
    sends = call(reslot, shape((total, width), BF16), [VMEM], 2 * total * row_count * CAP * width)(
        got
    )
    own = exchange(sends.reshape(GROUP_CLUSTERS, CAP, width), CHIPS)
    own, got = lax.optimization_barrier((own.reshape(total, width), got))
    flops = 2 * total * total // 2 * width
    early = call(best_own_early, shape((2, total), F32), [VMEM], flops)(own)
    own, early = lax.optimization_barrier((own, early))
    pairs = [(i, i ^ 1) for i in range(col_count)]
    half = total // 2
    other = [lax.ppermute(own[s : s + half], COLS, pairs) for s in (0, half)]
    lines = row_count * GROUP_CLUSTERS * 2
    outs = (shape((2, total), F32), shape((1, docs), jnp.int32))
    found, index = call(best_own_late, outs, [VMEM] * 5, flops)(own, early, labels, rank, got)
    theirs = lax.ppermute(found, COLS, pairs)
    parts = (shape((1, total), F32), shape((half, LANES), F32))
    best, more_rows = call(best_more, parts, [VMEM] * 3, flops)(own, other[0], found)
    results = call(best_last, shape((lines, LANES), F32), [VMEM] * 6, flops)(
        own, other[1], best, found, more_rows, theirs
    )
    results = exchange(results.astype(WIRE).reshape(lines // 2, 2, LANES), SAME_CORE)
    results = results.reshape(lines, LANES).astype(F32)
    best, hist = call(
        pick_results, (shape((1, docs), F32), shape((1, BINS), F32)), [VMEM, VMEM], 2**26
    )(index, results)
    return (best.reshape(docs), hist.reshape(BINS))


def solution(mesh):
    torus = Mesh(
        mesh.devices.reshape(2, 4, 2, 8, 2), ("rows_0", "rows_1", "cols_0", "cols_1", "cols_2")
    )
    in_specs = (P(ALL, None), P(ALL))
    out_specs = (P(ALL), P())
    return jax.shard_map(
        shards, mesh=torus, in_specs=in_specs, out_specs=out_specs, check_vma=False
    )
```

```python
import jax
import jax.numpy as jnp
from jax import lax
from jax.experimental import pallas as pl
from jax.experimental.pallas import tpu as pltpu
from jax.sharding import Mesh
from jax.sharding import PartitionSpec as P

CAP = 64
GROUP_CLUSTERS = 16
BINS = 128
ROWS = ("rows_1", "rows_0")
COLS = ("cols_0", "cols_1", "cols_2")
CHIPS = ("cols_0", "cols_1")
ALL = ("rows_0", "rows_1") + COLS
SAME_CORE = ROWS + CHIPS
LANES = 128
BLOCK = 256
EMPTY = 2.0
F32 = jnp.float32
BF16 = jnp.bfloat16
WIRE = jnp.float16
HIGH_SCALE = 2.0**10
LOW_SCALE = 2.0**18
HIST_SCALE = 16.0


def iota(shape, dim):
    return lax.broadcasted_iota(jnp.int32, shape, dim)


def dot(a, b):
    return lax.dot_general(a, b, (((1,), (0,)), ((), ())), preferred_element_type=F32)


def dot_t(a, b):
    return lax.dot_general(a, b, (((1,), (1,)), ((), ())), preferred_element_type=F32)


def ones_where(mask):
    return jnp.where(mask, 1.0, 0.0).astype(BF16)


def before(n):
    return ones_where(iota((n, n), 0) < iota((n, n), 1))


def rank_of(onehot, n):
    earlier = dot(onehot, before(n))
    return jnp.sum(onehot.astype(F32) * earlier, axis=0, keepdims=True)


def normalise_and_slot(labels_hbm, embeddings_hbm, out_ref, rank_ref, labels_ref, embeddings_ref, sems):
    labels_copy = pltpu.make_async_copy(labels_hbm, labels_ref, sems.at[0])
    embeddings_copy = pltpu.make_async_copy(embeddings_hbm, embeddings_ref, sems.at[1])
    labels_copy.start()
    embeddings_copy.start()
    docs, width = embeddings_ref.shape
    groups = out_ref.shape[0]
    clusters = groups * GROUP_CLUSTERS
    labels_copy.wait()
    labels = labels_ref[...]
    group = lax.shift_right_logical(labels, 4)
    onehot = ones_where(iota((groups, docs), 0) == group)
    slot = group * CAP + rank_of(onehot, docs).astype(jnp.int32)
    places = ones_where(iota((groups * CAP, docs), 0) == slot)
    shifted = jnp.broadcast_to((labels + 1).astype(F32), (8, docs)).astype(BF16)
    slot_labels = dot_t(shifted, places)
    of_cluster = ones_where(iota((clusters, docs), 0) == labels)
    counts = dot_t(jnp.ones((8, docs), BF16), of_cluster)
    row = iota((8, LANES), 0)
    meta = jnp.where(row == groups * CAP // LANES, counts, 0.0)
    for s in range(groups * CAP // LANES):
        meta = jnp.where(row == s, slot_labels[:, s * LANES : (s + 1) * LANES], meta)
    meta = meta.astype(BF16)
    rank_ref[...] = rank_of(of_cluster, docs)
    embeddings_copy.wait()
    values = embeddings_ref[...].astype(F32)
    total = jnp.sum(values * values, axis=1, keepdims=True)
    normed = (values * lax.rsqrt(total + 1e-06)).astype(BF16)
    rows = dot(places, normed).astype(BF16)
    pieces = width // LANES
    for g in range(groups):
        for f in range(pieces):
            block = rows[g * CAP : (g + 1) * CAP, f * LANES : (f + 1) * LANES]
            out_ref[g, f * CAP : (f + 1) * CAP, :] = block
        out_ref[g, pieces * CAP :, :] = meta


def slot_labels_of(got_ref, me):
    groups = got_ref.shape[0]
    slots = groups * CAP
    at = got_ref.shape[1] - 8
    source = lax.shift_right_logical(iota((8, slots), 1), 6)
    row = iota((8, LANES), 0)
    per_row = LANES // CAP
    picked = []
    for g in range(groups):
        meta = got_ref[g, at:, :].astype(F32)
        line = jnp.where(row == lax.shift_right_logical(me, 1), meta, 0.0)
        picked.append(jnp.sum(line, axis=0, keepdims=True))
    lines = jnp.concatenate(picked, axis=0).astype(BF16)
    lane, to = iota((LANES, slots), 0), iota((LANES, slots), 1)
    start = lax.bitwise_and(me, per_row - 1) * CAP
    move = ones_where(lane == start + lax.bitwise_and(to, CAP - 1))
    spread = jnp.where(iota((groups, slots), 0) == source, dot(lines, move), 0.0)
    return jnp.sum(spread, axis=0, keepdims=True)


def reslot(got_ref, out_ref):
    groups = got_ref.shape[0]
    slots = groups * CAP
    width = out_ref.shape[1]
    me = lax.axis_index(ROWS)
    label = slot_labels_of(got_ref, me).astype(jnp.int32)
    cluster = label - 1 - me * GROUP_CLUSTERS
    onehot = ones_where(iota((GROUP_CLUSTERS, slots), 0) == cluster)
    place = cluster * CAP + rank_of(onehot, slots).astype(jnp.int32)
    place = jnp.where(label > 0, place, -1)
    counts = jnp.sum(onehot.astype(F32), axis=1, keepdims=True).astype(jnp.int32)
    total = GROUP_CLUSTERS * CAP
    step = total // 4
    pieces = width // LANES
    rows = jnp.concatenate(
        [got_ref[:, f * CAP : (f + 1) * CAP, :].reshape(slots, LANES) for f in range(pieces)],
        axis=1,
    )
    lane, rank = iota((CAP, LANES), 1), iota((CAP, LANES), 0)
    marks = []
    for c in range(GROUP_CLUSTERS):
        empty = (rank >= counts[c : c + 1, :]) & (lane == 0)
        marks.append(jnp.where(empty, EMPTY, 0.0))
    for s in range(0, total, step):
        places = ones_where(iota((step, slots), 0) + s == place)
        moved = dot(places, rows)
        out_ref[s : s + step, LANES:] = moved[:, LANES:].astype(BF16)
        mark = jnp.concatenate(marks[s // CAP : (s + step) // CAP], axis=0)
        out_ref[s : s + step, 0:LANES] = (moved[:, 0:LANES] + mark).astype(BF16)


def return_index(labels_ref, rank_ref, got_ref, out_ref):
    groups = got_ref.shape[0]
    docs = labels_ref.shape[1]
    clusters = groups * GROUP_CLUSTERS
    me = lax.axis_index(ROWS)
    at = got_ref.shape[1] - 8
    row = iota((8, LANES), 0)
    before_me = jnp.zeros((8, LANES), F32)
    for g in range(groups):
        before_me = before_me + jnp.where(g < me, got_ref[g, at:, :].astype(F32), 0.0)
    counts = jnp.where(row == groups * CAP // LANES, before_me, 0.0)
    labels = labels_ref[...]
    of_cluster = ones_where(iota((clusters, docs), 0) == labels)
    earlier = jnp.sum(dot(counts.astype(BF16), of_cluster), axis=0, keepdims=True)
    out_ref[...] = labels * CAP + (rank_ref[...] + earlier).astype(jnp.int32)


def column_of(ref):
    return jnp.where(ref[:, 0:1].astype(F32) < 1.5, 0.0, -4.0)


def penalties(ref):
    column = column_of(ref)
    pick = ones_where(iota((8, 256), 1) == 0)
    row = jnp.where(dot_t(pick, ref[:, 0:256])[0:1, :] < 1.5, 0.0, -4.0)
    return column, row


def over_columns(scores):
    return jnp.max(scores.reshape(BLOCK // 8, 8, BLOCK), axis=0)


def over_rows(scores):
    return jnp.maximum(scores[:, :LANES], scores[:, LANES:])


def as_line(columns, rows):
    out = []
    for column, row in zip(columns, rows):
        line = jnp.max(column, axis=0, keepdims=True)
        if row is not None:
            turned = [jnp.max(row[h : h + LANES].T, axis=0, keepdims=True) for h in (0, LANES)]
            line = jnp.maximum(line, jnp.concatenate(turned, axis=1))
        out.append(line)
    return jnp.concatenate(out, axis=1)


def larger(a, b):
    return b if a is None else jnp.maximum(a, b)


def within(ref, penalty, columns, rows):
    column, row = penalty
    count = ref.shape[0] // BLOCK
    for i in range(count):
        for j in range(i, count):
            at, to = i * BLOCK, j * BLOCK
            scores = dot_t(ref[at : at + BLOCK, :], ref[to : to + BLOCK, :])
            scores = scores + column[at : at + BLOCK] + row[:, to : to + BLOCK]
            if i == j:
                other = iota((BLOCK, BLOCK), 0) != iota((BLOCK, BLOCK), 1)
                scores = jnp.where(other, scores, -4.0)
            else:
                rows[i] = larger(rows[i], over_rows(scores))
            columns[j] = larger(columns[j], over_columns(scores))


def between(a_ref, a_penalty, b_ref, b_penalty, rows, columns):
    for i in range(a_ref.shape[0] // BLOCK):
        for j in range(b_ref.shape[0] // BLOCK):
            at, to = i * BLOCK, j * BLOCK
            scores = dot_t(a_ref[at : at + BLOCK, :], b_ref[to : to + BLOCK, :])
            scores = scores + a_penalty[0][at : at + BLOCK] + b_penalty[1][:, to : to + BLOCK]
            rows[i] = larger(rows[i], over_rows(scores))
            columns[j] = larger(columns[j], over_columns(scores))


def nothing(ref):
    return [None] * (ref.shape[0] // BLOCK)


def best_own(own_ref, labels_ref, rank_ref, got_ref, found_ref, index_ref):
    return_index(labels_ref, rank_ref, got_ref, index_ref)
    columns, rows = nothing(own_ref), nothing(own_ref)
    penalty = penalties(own_ref)
    within(own_ref, penalty, columns, rows)
    best = jnp.maximum(as_line(columns, rows), -1.0)
    found_ref[...] = jnp.where(penalty[1] < 0.0, -8.0, best)


def penalty_of(found):
    return jnp.where(found < -4.0, -4.0, 0.0)


def best_more(own_ref, more_ref, found_ref, best_ref, rows_ref):
    rows, of_own = nothing(more_ref), nothing(own_ref)
    penalty = (column_of(more_ref), None)
    between(more_ref, penalty, own_ref, (None, penalty_of(found_ref[...])), rows, of_own)
    rows_ref[...] = jnp.concatenate(rows, axis=0)
    best_ref[...] = jnp.maximum(as_line(of_own, nothing(own_ref)), found_ref[...])


def histogram_parts(best, penalty):
    width = 2.0 / (BINS - 1)
    centers = -1.0 + iota((BINS, 1), 0).astype(F32) * width
    weights = jnp.maximum(1.0 - jnp.abs(best - centers) / width, 0.0)
    weights = jnp.where(penalty < 0.0, 0.0, weights)
    folded = weights[:, 0:LANES]
    for s in range(LANES, best.shape[1], LANES):
        folded = folded + weights[:, s : s + LANES]
    return folded


def best_last(
    own_ref, last_ref, so_far_ref, found_ref, more_rows_ref, theirs_ref, out_ref
):
    total = own_ref.shape[0]
    own_penalty = (None, penalty_of(found_ref[...]))
    rows, of_own = nothing(last_ref), nothing(own_ref)
    starts = range(0, more_rows_ref.shape[0], BLOCK)
    more_rows = [more_rows_ref[s : s + BLOCK, :] for s in starts]
    between(last_ref, (column_of(last_ref), None), own_ref, own_penalty, rows, of_own)
    best = jnp.maximum(as_line(of_own, nothing(own_ref)), so_far_ref[...])
    rows = more_rows + rows
    their_line = [theirs_ref[:, s : s + BLOCK] for s in range(0, total, BLOCK)]
    their_best = as_line(their_line, rows)
    mine = histogram_parts(best, own_penalty[1])
    theirs = histogram_parts(their_best, penalty_of(theirs_ref[...]))
    hist = jnp.sum((mine + theirs).T, axis=0, keepdims=True)
    high = best.astype(BF16).astype(F32)
    low = (best - high) * LOW_SCALE
    high = high * HIGH_SCALE
    hist = hist * HIST_SCALE
    sub = iota((8, LANES), 0)
    left = iota((1, LANES), 1) < CAP
    blocks = []
    for s in range(0, total, 2 * LANES):
        block = jnp.broadcast_to(hist, (8, LANES))
        for h in range(2):
            at = s + h * LANES
            top, rest = high[:, at : at + LANES], low[:, at : at + LANES]
            first = jnp.where(left, top, pltpu.roll(rest, CAP, 1))
            second = jnp.where(left, pltpu.roll(top, CAP, 1), rest)
            block = jnp.where(sub == 4 * h + 1, first, block)
            block = jnp.where(sub == 4 * h + 3, second, block)
        blocks.append(block)
    block = jnp.concatenate(blocks, axis=0)
    for at in range(0, out_ref.shape[0], block.shape[0]):
        out_ref[at : at + block.shape[0], :] = block


def pick_results(index_ref, got_ref, best_ref, hist_ref):
    lines = got_ref.shape[0]
    docs = index_ref.shape[1]
    index = index_ref[...]
    line = lax.shift_right_logical(index, 6) * 2 + 1
    rank = lax.bitwise_and(index, CAP - 1)
    onehot = ones_where(iota((lines, docs), 0) == line)
    got = got_ref[...]
    turned = got.T
    high = turned.astype(BF16)
    low = (turned - high.astype(F32)).astype(BF16)
    picked = dot(high, onehot) + dot(low, onehot)
    lane = iota((LANES, docs), 0)
    picked = picked * jnp.where(lane < CAP, 1.0 / HIGH_SCALE, 1.0 / LOW_SCALE)
    wanted = lax.bitwise_and(lane, CAP - 1) == rank
    best_ref[...] = jnp.sum(jnp.where(wanted, picked, 0.0), axis=0, keepdims=True)
    even = lax.bitwise_and(iota((8, LANES), 0), 1) == 0
    total = jnp.zeros((8, LANES), F32)
    for s in range(0, lines, 8):
        total = total + jnp.where(even, got[s : s + 8, :], 0.0)
    hist_ref[...] = jnp.sum(total, axis=0, keepdims=True) * (1.0 / (HIST_SCALE * lines * docs))


VMEM = pl.BlockSpec(memory_space=pltpu.VMEM)
ANY = pl.BlockSpec(memory_space=pl.ANY)


def call(kernel, outs, specs, flops, scratch=()):
    many = isinstance(outs, tuple)
    return pl.pallas_call(
        kernel,
        out_shape=outs,
        in_specs=specs,
        out_specs=tuple(VMEM for _ in outs) if many else VMEM,
        scratch_shapes=scratch,
        compiler_params=pltpu.CompilerParams(vmem_limit_bytes=24 * 2**20),
        cost_estimate=pl.CostEstimate(flops=flops, bytes_accessed=4000000, transcendentals=0),
    )


def shape(dims, dtype):
    return jax.ShapeDtypeStruct(dims, dtype)


def in_hbm(x):
    return pltpu.with_memory_space_constraint(x, pltpu.HBM)


def exchange(x, axes):
    return lax.all_to_all(x, axes, split_axis=0, concat_axis=0, tiled=True)


def shards(embeddings, document_cluster_index):
    row_count = lax.axis_size(ROWS)
    col_count = lax.axis_size(COLS)
    docs, width = embeddings.shape
    labels = document_cluster_index.reshape(1, docs)
    block = CAP * width // LANES + 8
    sends, rank = call(
        normalise_and_slot,
        (shape((row_count, block, LANES), BF16), shape((1, docs), F32)),
        [ANY, ANY],
        2 * row_count * CAP * docs * width,
        [
            pltpu.VMEM((1, docs), jnp.int32),
            pltpu.VMEM((docs, width), BF16),
            pltpu.SemaphoreType.DMA((2,)),
        ],
    )(in_hbm(labels), in_hbm(embeddings))
    got = exchange(sends, ROWS)
    total = GROUP_CLUSTERS * CAP
    sends = call(reslot, shape((total, width), BF16), [VMEM], 2 * total * row_count * CAP * width)(
        got
    )
    own = exchange(sends.reshape(GROUP_CLUSTERS, CAP, width), CHIPS)
    own, got = lax.optimization_barrier((own.reshape(total, width), got))
    pairs = [(i, i ^ 1) for i in range(col_count)]
    half = total // 2
    other = [lax.ppermute(own[s : s + half], COLS, pairs) for s in (0, half)]
    flops = 2 * total * half * width
    lines = row_count * GROUP_CLUSTERS * 2
    outs = (shape((1, total), F32), shape((1, docs), jnp.int32))
    found, index = call(best_own, outs, [VMEM] * 4, flops)(own, labels, rank, got)
    theirs = lax.ppermute(found, COLS, pairs)
    parts = (shape((1, total), F32), shape((half, LANES), F32))
    best, more_rows = call(best_more, parts, [VMEM] * 3, flops)(own, other[0], found)
    results = call(best_last, shape((lines, LANES), F32), [VMEM] * 6, flops)(
        own, other[1], best, found, more_rows, theirs
    )
    results = exchange(results.astype(WIRE).reshape(lines // 2, 2, LANES), SAME_CORE)
    results = results.reshape(lines, LANES).astype(F32)
    best, hist = call(
        pick_results, (shape((1, docs), F32), shape((1, BINS), F32)), [VMEM, VMEM], 2**26
    )(index, results)
    return (best.reshape(docs), hist.reshape(BINS))


def solution(mesh):
    torus = Mesh(
        mesh.devices.reshape(2, 4, 2, 8, 2), ("rows_0", "rows_1", "cols_0", "cols_1", "cols_2")
    )
    in_specs = (P(ALL, None), P(ALL))
    out_specs = (P(ALL), P())
    return jax.shard_map(
        shards, mesh=torus, in_specs=in_specs, out_specs=out_specs, check_vma=False
    )
```

```python
import jax
import jax.numpy as jnp
from jax import lax
from jax.experimental import pallas as pl
from jax.experimental.pallas import tpu as pltpu
from jax.sharding import Mesh
from jax.sharding import PartitionSpec as P

CAP = 64
GROUP_CLUSTERS = 16
BINS = 128
ROWS = ("rows_1", "rows_0")
COLS = ("cols_0", "cols_1", "cols_2")
CHIPS = ("cols_0", "cols_1")
ALL = ("rows_0", "rows_1") + COLS
SAME_CORE = ROWS + CHIPS
LANES = 128
BLOCK = 256
PIECES = 4
EMPTY = 2.0
F32 = jnp.float32
BF16 = jnp.bfloat16
WIRE = jnp.float16
HIGH_SCALE = 2.0**10
LOW_SCALE = 2.0**18
HIST_SCALE = 16.0


def iota(shape, dim):
    return lax.broadcasted_iota(jnp.int32, shape, dim)


def dot(a, b):
    return lax.dot_general(a, b, (((1,), (0,)), ((), ())), preferred_element_type=F32)


def dot_t(a, b):
    return lax.dot_general(a, b, (((1,), (1,)), ((), ())), preferred_element_type=F32)


def ones_where(mask):
    return jnp.where(mask, 1.0, 0.0).astype(BF16)


def before(n):
    return ones_where(iota((n, n), 0) < iota((n, n), 1))


def rank_of(onehot, n):
    earlier = dot(onehot, before(n))
    return jnp.sum(onehot.astype(F32) * earlier, axis=0, keepdims=True)


def normalise_and_slot(labels_hbm, embeddings_hbm, out_ref, rank_ref, labels_ref, embeddings_ref, sems):
    labels_copy = pltpu.make_async_copy(labels_hbm, labels_ref, sems.at[0])
    step = embeddings_ref.shape[0] // PIECES
    pieces_of = [pl.ds(p * step, step) for p in range(PIECES)]
    embeddings_copies = [
        pltpu.make_async_copy(embeddings_hbm.at[at], embeddings_ref.at[at], sems.at[1 + p])
        for p, at in enumerate(pieces_of)
    ]
    labels_copy.start()
    for copy in embeddings_copies:
        copy.start()
    docs, width = embeddings_ref.shape
    groups = out_ref.shape[0]
    clusters = groups * GROUP_CLUSTERS
    labels_copy.wait()
    labels = labels_ref[...]
    group = lax.shift_right_logical(labels, 4)
    onehot = ones_where(iota((groups, docs), 0) == group)
    slot = group * CAP + rank_of(onehot, docs).astype(jnp.int32)
    places = ones_where(iota((groups * CAP, docs), 0) == slot)
    shifted = jnp.broadcast_to((labels + 1).astype(F32), (8, docs)).astype(BF16)
    slot_labels = dot_t(shifted, places)
    of_cluster = ones_where(iota((clusters, docs), 0) == labels)
    counts = dot_t(jnp.ones((8, docs), BF16), of_cluster)
    row = iota((8, LANES), 0)
    meta = jnp.where(row == groups * CAP // LANES, counts, 0.0)
    for s in range(groups * CAP // LANES):
        meta = jnp.where(row == s, slot_labels[:, s * LANES : (s + 1) * LANES], meta)
    meta = meta.astype(BF16)
    rank_ref[...] = rank_of(of_cluster, docs)
    normed = []
    for copy, at in zip(embeddings_copies, pieces_of):
        copy.wait()
        values = embeddings_ref[at, :].astype(F32)
        total = jnp.sum(values * values, axis=1, keepdims=True)
        normed.append((values * lax.rsqrt(total + 1e-06)).astype(BF16))
    normed = jnp.concatenate(normed, axis=0)
    rows = dot(places, normed).astype(BF16)
    pieces = width // LANES
    for g in range(groups):
        for f in range(pieces):
            block = rows[g * CAP : (g + 1) * CAP, f * LANES : (f + 1) * LANES]
            out_ref[g, f * CAP : (f + 1) * CAP, :] = block
        out_ref[g, pieces * CAP :, :] = meta


def slot_labels_of(got_ref, me):
    groups = got_ref.shape[0]
    slots = groups * CAP
    at = got_ref.shape[1] - 8
    source = lax.shift_right_logical(iota((8, slots), 1), 6)
    row = iota((8, LANES), 0)
    per_row = LANES // CAP
    picked = []
    for g in range(groups):
        meta = got_ref[g, at:, :].astype(F32)
        line = jnp.where(row == lax.shift_right_logical(me, 1), meta, 0.0)
        picked.append(jnp.sum(line, axis=0, keepdims=True))
    lines = jnp.concatenate(picked, axis=0).astype(BF16)
    lane, to = iota((LANES, slots), 0), iota((LANES, slots), 1)
    start = lax.bitwise_and(me, per_row - 1) * CAP
    move = ones_where(lane == start + lax.bitwise_and(to, CAP - 1))
    spread = jnp.where(iota((groups, slots), 0) == source, dot(lines, move), 0.0)
    return jnp.sum(spread, axis=0, keepdims=True)


def reslot(got_ref, out_ref):
    groups = got_ref.shape[0]
    slots = groups * CAP
    width = out_ref.shape[1]
    me = lax.axis_index(ROWS)
    label = slot_labels_of(got_ref, me).astype(jnp.int32)
    cluster = label - 1 - me * GROUP_CLUSTERS
    onehot = ones_where(iota((GROUP_CLUSTERS, slots), 0) == cluster)
    place = cluster * CAP + rank_of(onehot, slots).astype(jnp.int32)
    place = jnp.where(label > 0, place, -1)
    counts = jnp.sum(onehot.astype(F32), axis=1, keepdims=True).astype(jnp.int32)
    total = GROUP_CLUSTERS * CAP
    step = total // 4
    pieces = width // LANES
    rows = jnp.concatenate(
        [got_ref[:, f * CAP : (f + 1) * CAP, :].reshape(slots, LANES) for f in range(pieces)],
        axis=1,
    )
    lane, rank = iota((CAP, LANES), 1), iota((CAP, LANES), 0)
    marks = []
    for c in range(GROUP_CLUSTERS):
        empty = (rank >= counts[c : c + 1, :]) & (lane == 0)
        marks.append(jnp.where(empty, EMPTY, 0.0))
    for s in range(0, total, step):
        places = ones_where(iota((step, slots), 0) + s == place)
        moved = dot(places, rows)
        out_ref[s : s + step, LANES:] = moved[:, LANES:].astype(BF16)
        mark = jnp.concatenate(marks[s // CAP : (s + step) // CAP], axis=0)
        out_ref[s : s + step, 0:LANES] = (moved[:, 0:LANES] + mark).astype(BF16)


def return_index(labels_ref, rank_ref, got_ref, out_ref):
    groups = got_ref.shape[0]
    docs = labels_ref.shape[1]
    clusters = groups * GROUP_CLUSTERS
    me = lax.axis_index(ROWS)
    at = got_ref.shape[1] - 8
    row = iota((8, LANES), 0)
    before_me = jnp.zeros((8, LANES), F32)
    for g in range(groups):
        before_me = before_me + jnp.where(g < me, got_ref[g, at:, :].astype(F32), 0.0)
    counts = jnp.where(row == groups * CAP // LANES, before_me, 0.0)
    labels = labels_ref[...]
    of_cluster = ones_where(iota((clusters, docs), 0) == labels)
    earlier = jnp.sum(dot(counts.astype(BF16), of_cluster), axis=0, keepdims=True)
    out_ref[...] = labels * CAP + (rank_ref[...] + earlier).astype(jnp.int32)


def column_of(ref):
    return jnp.where(ref[:, 0:1].astype(F32) < 1.5, 0.0, -4.0)


def penalties(ref):
    column = column_of(ref)
    pick = ones_where(iota((8, 256), 1) == 0)
    row = jnp.where(dot_t(pick, ref[:, 0:256])[0:1, :] < 1.5, 0.0, -4.0)
    return column, row


def over_columns(scores):
    return jnp.max(scores.reshape(BLOCK // 8, 8, BLOCK), axis=0)


def over_rows(scores):
    return jnp.maximum(scores[:, :LANES], scores[:, LANES:])


def as_line(columns, rows):
    out = []
    for column, row in zip(columns, rows):
        line = jnp.max(column, axis=0, keepdims=True)
        if row is not None:
            turned = [jnp.max(row[h : h + LANES].T, axis=0, keepdims=True) for h in (0, LANES)]
            line = jnp.maximum(line, jnp.concatenate(turned, axis=1))
        out.append(line)
    return jnp.concatenate(out, axis=1)


def larger(a, b):
    return b if a is None else jnp.maximum(a, b)


def within(ref, penalty, columns, rows):
    column, row = penalty
    count = ref.shape[0] // BLOCK
    for i in range(count):
        for j in range(i, count):
            at, to = i * BLOCK, j * BLOCK
            scores = dot_t(ref[at : at + BLOCK, :], ref[to : to + BLOCK, :])
            scores = scores + column[at : at + BLOCK] + row[:, to : to + BLOCK]
            if i == j:
                other = iota((BLOCK, BLOCK), 0) != iota((BLOCK, BLOCK), 1)
                scores = jnp.where(other, scores, -4.0)
            else:
                rows[i] = larger(rows[i], over_rows(scores))
            columns[j] = larger(columns[j], over_columns(scores))


def between(a_ref, a_penalty, b_ref, b_penalty, rows, columns):
    for i in range(a_ref.shape[0] // BLOCK):
        for j in range(b_ref.shape[0] // BLOCK):
            at, to = i * BLOCK, j * BLOCK
            scores = dot_t(a_ref[at : at + BLOCK, :], b_ref[to : to + BLOCK, :])
            scores = scores + a_penalty[0][at : at + BLOCK] + b_penalty[1][:, to : to + BLOCK]
            rows[i] = larger(rows[i], over_rows(scores))
            columns[j] = larger(columns[j], over_columns(scores))


def nothing(ref):
    return [None] * (ref.shape[0] // BLOCK)


def best_own(own_ref, found_ref):
    columns, rows = nothing(own_ref), nothing(own_ref)
    penalty = penalties(own_ref)
    within(own_ref, penalty, columns, rows)
    found_ref[0:1, :] = jnp.maximum(as_line(columns, rows), -1.0)
    found_ref[1:2, :] = penalty[1]


def best_more(own_ref, more_ref, found_ref, best_ref, rows_ref):
    rows, of_own = nothing(more_ref), nothing(own_ref)
    penalty = (column_of(more_ref), None)
    between(more_ref, penalty, own_ref, (None, found_ref[1:2, :]), rows, of_own)
    rows_ref[...] = jnp.concatenate(rows, axis=0)
    best_ref[...] = jnp.maximum(as_line(of_own, nothing(own_ref)), found_ref[0:1, :])


def histogram_parts(best, penalty):
    width = 2.0 / (BINS - 1)
    centers = -1.0 + iota((BINS, 1), 0).astype(F32) * width
    weights = jnp.maximum(1.0 - jnp.abs(best - centers) / width, 0.0)
    weights = jnp.where(penalty < 0.0, 0.0, weights)
    folded = weights[:, 0:LANES]
    for s in range(LANES, best.shape[1], LANES):
        folded = folded + weights[:, s : s + LANES]
    return folded


def best_last(
    own_ref, last_ref, so_far_ref, found_ref, more_rows_ref, theirs_ref, out_ref
):
    total = own_ref.shape[0]
    own_penalty = (None, found_ref[1:2, :])
    rows, of_own = nothing(last_ref), nothing(own_ref)
    starts = range(0, more_rows_ref.shape[0], BLOCK)
    more_rows = [more_rows_ref[s : s + BLOCK, :] for s in starts]
    between(last_ref, (column_of(last_ref), None), own_ref, own_penalty, rows, of_own)
    best = jnp.maximum(as_line(of_own, nothing(own_ref)), so_far_ref[...])
    rows = more_rows + rows
    their_line = [theirs_ref[0:1, s : s + BLOCK] for s in range(0, total, BLOCK)]
    their_best = as_line(their_line, rows)
    mine = histogram_parts(best, own_penalty[1])
    theirs = histogram_parts(their_best, theirs_ref[1:2, :])
    hist = jnp.sum((mine + theirs).T, axis=0, keepdims=True)
    high = best.astype(BF16).astype(F32)
    low = (best - high) * LOW_SCALE
    high = high * HIGH_SCALE
    hist = hist * HIST_SCALE
    sub = iota((8, LANES), 0)
    left = iota((1, LANES), 1) < CAP
    blocks = []
    for s in range(0, total, 2 * LANES):
        block = jnp.broadcast_to(hist, (8, LANES))
        for h in range(2):
            at = s + h * LANES
            top, rest = high[:, at : at + LANES], low[:, at : at + LANES]
            first = jnp.where(left, top, pltpu.roll(rest, CAP, 1))
            second = jnp.where(left, pltpu.roll(top, CAP, 1), rest)
            block = jnp.where(sub == 4 * h + 1, first, block)
            block = jnp.where(sub == 4 * h + 3, second, block)
        blocks.append(block)
    block = jnp.concatenate(blocks, axis=0)
    for at in range(0, out_ref.shape[0], block.shape[0]):
        out_ref[at : at + block.shape[0], :] = block


def pick_results(index_ref, got_ref, best_ref, hist_ref):
    lines = got_ref.shape[0]
    docs = index_ref.shape[1]
    index = index_ref[...]
    line = lax.shift_right_logical(index, 6) * 2 + 1
    rank = lax.bitwise_and(index, CAP - 1)
    onehot = ones_where(iota((lines, docs), 0) == line)
    got = got_ref[...]
    turned = got.T
    high = turned.astype(BF16)
    low = (turned - high.astype(F32)).astype(BF16)
    picked = dot(high, onehot) + dot(low, onehot)
    lane = iota((LANES, docs), 0)
    picked = picked * jnp.where(lane < CAP, 1.0 / HIGH_SCALE, 1.0 / LOW_SCALE)
    wanted = lax.bitwise_and(lane, CAP - 1) == rank
    best_ref[...] = jnp.sum(jnp.where(wanted, picked, 0.0), axis=0, keepdims=True)
    even = lax.bitwise_and(iota((8, LANES), 0), 1) == 0
    total = jnp.zeros((8, LANES), F32)
    for s in range(0, lines, 8):
        total = total + jnp.where(even, got[s : s + 8, :], 0.0)
    hist_ref[...] = jnp.sum(total, axis=0, keepdims=True) * (1.0 / (HIST_SCALE * lines * docs))


VMEM = pl.BlockSpec(memory_space=pltpu.VMEM)
ANY = pl.BlockSpec(memory_space=pl.ANY)


def call(kernel, outs, specs, flops, scratch=()):
    many = isinstance(outs, tuple)
    return pl.pallas_call(
        kernel,
        out_shape=outs,
        in_specs=specs,
        out_specs=tuple(VMEM for _ in outs) if many else VMEM,
        scratch_shapes=scratch,
        compiler_params=pltpu.CompilerParams(vmem_limit_bytes=24 * 2**20),
        cost_estimate=pl.CostEstimate(flops=flops, bytes_accessed=4000000, transcendentals=0),
    )


def shape(dims, dtype):
    return jax.ShapeDtypeStruct(dims, dtype)


def in_hbm(x):
    return pltpu.with_memory_space_constraint(x, pltpu.HBM)


def exchange(x, axes):
    return lax.all_to_all(x, axes, split_axis=0, concat_axis=0, tiled=True)


def shards(embeddings, document_cluster_index):
    row_count = lax.axis_size(ROWS)
    col_count = lax.axis_size(COLS)
    docs, width = embeddings.shape
    labels = document_cluster_index.reshape(1, docs)
    block = CAP * width // LANES + 8
    sends, rank = call(
        normalise_and_slot,
        (shape((row_count, block, LANES), BF16), shape((1, docs), F32)),
        [ANY, ANY],
        2 * row_count * CAP * docs * width,
        [
            pltpu.VMEM((1, docs), jnp.int32),
            pltpu.VMEM((docs, width), BF16),
            pltpu.SemaphoreType.DMA((1 + PIECES,)),
        ],
    )(in_hbm(labels), in_hbm(embeddings))
    got = exchange(sends, ROWS)
    total = GROUP_CLUSTERS * CAP
    sends = call(reslot, shape((total, width), BF16), [VMEM], 2 * total * row_count * CAP * width)(
        got
    )
    own = exchange(sends.reshape(GROUP_CLUSTERS, CAP, width), CHIPS)
    own, got = lax.optimization_barrier((own.reshape(total, width), got))
    pairs = [(i, i ^ 1) for i in range(col_count)]
    half = total // 2
    other = [lax.ppermute(own[s : s + half], COLS, pairs) for s in (0, half)]
    flops = 2 * total * half * width
    lines = row_count * GROUP_CLUSTERS * 2
    found = call(best_own, shape((2, total), F32), [VMEM], flops)(own)
    theirs = lax.ppermute(found, COLS, pairs)
    parts = (shape((1, total), F32), shape((half, LANES), F32))
    best, more_rows = call(best_more, parts, [VMEM] * 3, flops)(own, other[0], found)
    index = call(return_index, shape((1, docs), jnp.int32), [VMEM] * 3, 2**26)(labels, rank, got)
    results = call(best_last, shape((lines, LANES), F32), [VMEM] * 6, flops)(
        own, other[1], best, found, more_rows, theirs
    )
    results, index = lax.optimization_barrier((results, index))
    results = exchange(results.astype(WIRE).reshape(lines // 2, 2, LANES), SAME_CORE)
    results = results.reshape(lines, LANES).astype(F32)
    best, hist = call(
        pick_results, (shape((1, docs), F32), shape((1, BINS), F32)), [VMEM, VMEM], 2**26
    )(index, results)
    return (best.reshape(docs), hist.reshape(BINS))


def solution(mesh):
    torus = Mesh(
        mesh.devices.reshape(2, 4, 2, 8, 2), ("rows_0", "rows_1", "cols_0", "cols_1", "cols_2")
    )
    in_specs = (P(ALL, None), P(ALL))
    out_specs = (P(ALL), P())
    return jax.shard_map(
        shards, mesh=torus, in_specs=in_specs, out_specs=out_specs, check_vma=False
    )
```

```python
import jax
import jax.numpy as jnp
from jax import lax
from jax.experimental import pallas as pl
from jax.experimental.pallas import tpu as pltpu
from jax.sharding import Mesh
from jax.sharding import PartitionSpec as P

CAP = 64
GROUP_CLUSTERS = 16
BINS = 128
ROWS = ("rows_1", "rows_0")
COLS = ("cols_0", "cols_1", "cols_2")
CHIPS = ("cols_0", "cols_1")
ALL = ("rows_0", "rows_1") + COLS
SAME_CORE = ROWS + CHIPS
LANES = 128
BLOCK = 256
EMPTY = 2.0
F32 = jnp.float32
BF16 = jnp.bfloat16
WIRE = jnp.float16
HIGH_SCALE = 2.0**10
LOW_SCALE = 2.0**18
HIST_SCALE = 16.0


def iota(shape, dim):
    return lax.broadcasted_iota(jnp.int32, shape, dim)


def dot(a, b):
    return lax.dot_general(a, b, (((1,), (0,)), ((), ())), preferred_element_type=F32)


def dot_t(a, b):
    return lax.dot_general(a, b, (((1,), (1,)), ((), ())), preferred_element_type=F32)


def ones_where(mask):
    return jnp.where(mask, 1.0, 0.0).astype(BF16)


def before(n):
    return ones_where(iota((n, n), 0) < iota((n, n), 1))


def rank_of(onehot, n):
    earlier = dot(onehot, before(n))
    return jnp.sum(onehot.astype(F32) * earlier, axis=0, keepdims=True)


def normalise_and_slot(labels_hbm, embeddings_hbm, out_ref, rank_ref, labels_ref, embeddings_ref, sems):
    labels_copy = pltpu.make_async_copy(labels_hbm, labels_ref, sems.at[0])
    embeddings_copy = pltpu.make_async_copy(embeddings_hbm, embeddings_ref, sems.at[1])
    labels_copy.start()
    embeddings_copy.start()
    docs, width = embeddings_ref.shape
    groups = out_ref.shape[0]
    clusters = groups * GROUP_CLUSTERS
    labels_copy.wait()
    labels = labels_ref[...]
    group = lax.shift_right_logical(labels, 4)
    onehot = ones_where(iota((groups, docs), 0) == group)
    slot = group * CAP + rank_of(onehot, docs).astype(jnp.int32)
    places = ones_where(iota((groups * CAP, docs), 0) == slot)
    embeddings_copy.wait()
    values = embeddings_ref[...].astype(F32)
    total = jnp.sum(values * values, axis=1, keepdims=True)
    normed = (values * lax.rsqrt(total + 1e-06)).astype(BF16)
    shifted = jnp.broadcast_to((labels + 1).astype(F32), (8, docs)).astype(BF16)
    slot_labels = dot_t(shifted, places)
    of_cluster = ones_where(iota((clusters, docs), 0) == labels)
    counts = dot_t(jnp.ones((8, docs), BF16), of_cluster)
    row = iota((8, LANES), 0)
    meta = jnp.where(row == groups * CAP // LANES, counts, 0.0)
    for s in range(groups * CAP // LANES):
        meta = jnp.where(row == s, slot_labels[:, s * LANES : (s + 1) * LANES], meta)
    meta = meta.astype(BF16)
    rank_ref[...] = rank_of(of_cluster, docs)
    rows = dot(places, normed).astype(BF16)
    pieces = width // LANES
    for g in range(groups):
        for f in range(pieces):
            block = rows[g * CAP : (g + 1) * CAP, f * LANES : (f + 1) * LANES]
            out_ref[g, f * CAP : (f + 1) * CAP, :] = block
        out_ref[g, pieces * CAP :, :] = meta


def slot_labels_of(got_ref, me):
    groups = got_ref.shape[0]
    slots = groups * CAP
    at = got_ref.shape[1] - 8
    source = lax.shift_right_logical(iota((8, slots), 1), 6)
    row = iota((8, LANES), 0)
    per_row = LANES // CAP
    picked = []
    for g in range(groups):
        meta = got_ref[g, at:, :].astype(F32)
        line = jnp.where(row == lax.shift_right_logical(me, 1), meta, 0.0)
        picked.append(jnp.sum(line, axis=0, keepdims=True))
    lines = jnp.concatenate(picked, axis=0).astype(BF16)
    lane, to = iota((LANES, slots), 0), iota((LANES, slots), 1)
    start = lax.bitwise_and(me, per_row - 1) * CAP
    move = ones_where(lane == start + lax.bitwise_and(to, CAP - 1))
    spread = jnp.where(iota((groups, slots), 0) == source, dot(lines, move), 0.0)
    return jnp.sum(spread, axis=0, keepdims=True)


def reslot(got_ref, out_ref):
    groups = got_ref.shape[0]
    slots = groups * CAP
    width = out_ref.shape[1]
    me = lax.axis_index(ROWS)
    label = slot_labels_of(got_ref, me).astype(jnp.int32)
    cluster = label - 1 - me * GROUP_CLUSTERS
    onehot = ones_where(iota((GROUP_CLUSTERS, slots), 0) == cluster)
    place = cluster * CAP + rank_of(onehot, slots).astype(jnp.int32)
    place = jnp.where(label > 0, place, -1)
    counts = jnp.sum(onehot.astype(F32), axis=1, keepdims=True).astype(jnp.int32)
    total = GROUP_CLUSTERS * CAP
    step = total // 4
    pieces = width // LANES
    rows = jnp.concatenate(
        [got_ref[:, f * CAP : (f + 1) * CAP, :].reshape(slots, LANES) for f in range(pieces)],
        axis=1,
    )
    lane, rank = iota((CAP, LANES), 1), iota((CAP, LANES), 0)
    marks = []
    for c in range(GROUP_CLUSTERS):
        empty = (rank >= counts[c : c + 1, :]) & (lane == 0)
        marks.append(jnp.where(empty, EMPTY, 0.0))
    for s in range(0, total, step):
        places = ones_where(iota((step, slots), 0) + s == place)
        moved = dot(places, rows)
        out_ref[s : s + step, LANES:] = moved[:, LANES:].astype(BF16)
        mark = jnp.concatenate(marks[s // CAP : (s + step) // CAP], axis=0)
        out_ref[s : s + step, 0:LANES] = (moved[:, 0:LANES] + mark).astype(BF16)


def return_index(labels_ref, rank_ref, got_ref, out_ref):
    groups = got_ref.shape[0]
    docs = labels_ref.shape[1]
    clusters = groups * GROUP_CLUSTERS
    me = lax.axis_index(ROWS)
    at = got_ref.shape[1] - 8
    row = iota((8, LANES), 0)
    before_me = jnp.zeros((8, LANES), F32)
    for g in range(groups):
        before_me = before_me + jnp.where(g < me, got_ref[g, at:, :].astype(F32), 0.0)
    counts = jnp.where(row == groups * CAP // LANES, before_me, 0.0)
    labels = labels_ref[...]
    of_cluster = ones_where(iota((clusters, docs), 0) == labels)
    earlier = jnp.sum(dot(counts.astype(BF16), of_cluster), axis=0, keepdims=True)
    out_ref[...] = labels * CAP + (rank_ref[...] + earlier).astype(jnp.int32)


def column_of(ref):
    return jnp.where(ref[:, 0:1].astype(F32) < 1.5, 0.0, -4.0)


def penalties(ref):
    column = column_of(ref)
    pick = ones_where(iota((8, 256), 1) == 0)
    row = jnp.where(dot_t(pick, ref[:, 0:256])[0:1, :] < 1.5, 0.0, -4.0)
    return column, row


def over_columns(scores):
    return jnp.max(scores.reshape(BLOCK // 8, 8, BLOCK), axis=0)


def over_rows(scores):
    return jnp.maximum(scores[:, :LANES], scores[:, LANES:])


def as_line(columns, rows):
    out = []
    for column, row in zip(columns, rows):
        line = jnp.max(column, axis=0, keepdims=True)
        if row is not None:
            turned = [jnp.max(row[h : h + LANES].T, axis=0, keepdims=True) for h in (0, LANES)]
            line = jnp.maximum(line, jnp.concatenate(turned, axis=1))
        out.append(line)
    return jnp.concatenate(out, axis=1)


def larger(a, b):
    return b if a is None else jnp.maximum(a, b)


def within(ref, penalty, columns, rows):
    column, row = penalty
    count = ref.shape[0] // BLOCK
    for i in range(count):
        for j in range(i, count):
            at, to = i * BLOCK, j * BLOCK
            scores = dot_t(ref[at : at + BLOCK, :], ref[to : to + BLOCK, :])
            scores = scores + column[at : at + BLOCK] + row[:, to : to + BLOCK]
            if i == j:
                other = iota((BLOCK, BLOCK), 0) != iota((BLOCK, BLOCK), 1)
                scores = jnp.where(other, scores, -4.0)
            else:
                rows[i] = larger(rows[i], over_rows(scores))
            columns[j] = larger(columns[j], over_columns(scores))


def between(a_ref, a_penalty, b_ref, b_penalty, rows, columns):
    for i in range(a_ref.shape[0] // BLOCK):
        for j in range(b_ref.shape[0] // BLOCK):
            at, to = i * BLOCK, j * BLOCK
            scores = dot_t(a_ref[at : at + BLOCK, :], b_ref[to : to + BLOCK, :])
            scores = scores + a_penalty[0][at : at + BLOCK] + b_penalty[1][:, to : to + BLOCK]
            rows[i] = larger(rows[i], over_rows(scores))
            columns[j] = larger(columns[j], over_columns(scores))


def nothing(ref):
    return [None] * (ref.shape[0] // BLOCK)


def best_own(own_ref, found_ref):
    columns, rows = nothing(own_ref), nothing(own_ref)
    penalty = penalties(own_ref)
    within(own_ref, penalty, columns, rows)
    found_ref[0:1, :] = jnp.maximum(as_line(columns, rows), -1.0)
    found_ref[1:2, :] = penalty[1]


def best_more(own_ref, more_ref, found_ref, best_ref, rows_ref):
    rows, of_own = nothing(more_ref), nothing(own_ref)
    penalty = (column_of(more_ref), None)
    between(more_ref, penalty, own_ref, (None, found_ref[1:2, :]), rows, of_own)
    rows_ref[...] = jnp.concatenate(rows, axis=0)
    best_ref[...] = jnp.maximum(as_line(of_own, nothing(own_ref)), found_ref[0:1, :])


def histogram_parts(best, penalty):
    width = 2.0 / (BINS - 1)
    centers = -1.0 + iota((BINS, 1), 0).astype(F32) * width
    weights = jnp.maximum(1.0 - jnp.abs(best - centers) / width, 0.0)
    weights = jnp.where(penalty < 0.0, 0.0, weights)
    folded = weights[:, 0:LANES]
    for s in range(LANES, best.shape[1], LANES):
        folded = folded + weights[:, s : s + LANES]
    return folded


def best_last(
    own_ref, last_ref, so_far_ref, found_ref, more_rows_ref, theirs_ref, out_ref
):
    total = own_ref.shape[0]
    own_penalty = (None, found_ref[1:2, :])
    rows, of_own = nothing(last_ref), nothing(own_ref)
    starts = range(0, more_rows_ref.shape[0], BLOCK)
    more_rows = [more_rows_ref[s : s + BLOCK, :] for s in starts]
    between(last_ref, (column_of(last_ref), None), own_ref, own_penalty, rows, of_own)
    best = jnp.maximum(as_line(of_own, nothing(own_ref)), so_far_ref[...])
    rows = more_rows + rows
    their_line = [theirs_ref[0:1, s : s + BLOCK] for s in range(0, total, BLOCK)]
    their_best = as_line(their_line, rows)
    mine = histogram_parts(best, own_penalty[1])
    theirs = histogram_parts(their_best, theirs_ref[1:2, :])
    hist = jnp.sum((mine + theirs).T, axis=0, keepdims=True)
    high = best.astype(BF16).astype(F32)
    low = (best - high) * LOW_SCALE
    high = high * HIGH_SCALE
    hist = hist * HIST_SCALE
    sub = iota((8, LANES), 0)
    left = iota((1, LANES), 1) < CAP
    blocks = []
    for s in range(0, total, 2 * LANES):
        block = jnp.broadcast_to(hist, (8, LANES))
        for h in range(2):
            at = s + h * LANES
            top, rest = high[:, at : at + LANES], low[:, at : at + LANES]
            first = jnp.where(left, top, pltpu.roll(rest, CAP, 1))
            second = jnp.where(left, pltpu.roll(top, CAP, 1), rest)
            block = jnp.where(sub == 4 * h + 1, first, block)
            block = jnp.where(sub == 4 * h + 3, second, block)
        blocks.append(block)
    block = jnp.concatenate(blocks, axis=0)
    for at in range(0, out_ref.shape[0], block.shape[0]):
        out_ref[at : at + block.shape[0], :] = block


def pick_results(index_ref, got_ref, best_ref, hist_ref):
    lines = got_ref.shape[0]
    docs = index_ref.shape[1]
    index = index_ref[...]
    line = lax.shift_right_logical(index, 6) * 2 + 1
    rank = lax.bitwise_and(index, CAP - 1)
    onehot = ones_where(iota((lines, docs), 0) == line)
    got = got_ref[...]
    turned = got.T
    high = turned.astype(BF16)
    low = (turned - high.astype(F32)).astype(BF16)
    picked = dot(high, onehot) + dot(low, onehot)
    lane = iota((LANES, docs), 0)
    picked = picked * jnp.where(lane < CAP, 1.0 / HIGH_SCALE, 1.0 / LOW_SCALE)
    wanted = lax.bitwise_and(lane, CAP - 1) == rank
    best_ref[...] = jnp.sum(jnp.where(wanted, picked, 0.0), axis=0, keepdims=True)
    even = lax.bitwise_and(iota((8, LANES), 0), 1) == 0
    total = jnp.zeros((8, LANES), F32)
    for s in range(0, lines, 8):
        total = total + jnp.where(even, got[s : s + 8, :], 0.0)
    hist_ref[...] = jnp.sum(total, axis=0, keepdims=True) * (1.0 / (HIST_SCALE * lines * docs))


VMEM = pl.BlockSpec(memory_space=pltpu.VMEM)
ANY = pl.BlockSpec(memory_space=pl.ANY)


def call(kernel, outs, specs, flops, scratch=()):
    many = isinstance(outs, tuple)
    return pl.pallas_call(
        kernel,
        out_shape=outs,
        in_specs=specs,
        out_specs=tuple(VMEM for _ in outs) if many else VMEM,
        scratch_shapes=scratch,
        compiler_params=pltpu.CompilerParams(vmem_limit_bytes=24 * 2**20),
        cost_estimate=pl.CostEstimate(flops=flops, bytes_accessed=4000000, transcendentals=0),
    )


def shape(dims, dtype):
    return jax.ShapeDtypeStruct(dims, dtype)


def in_hbm(x):
    return pltpu.with_memory_space_constraint(x, pltpu.HBM)


def exchange(x, axes):
    return lax.all_to_all(x, axes, split_axis=0, concat_axis=0, tiled=True)


def shards(embeddings, document_cluster_index):
    row_count = lax.axis_size(ROWS)
    col_count = lax.axis_size(COLS)
    docs, width = embeddings.shape
    labels = document_cluster_index.reshape(1, docs)
    block = CAP * width // LANES + 8
    sends, rank = call(
        normalise_and_slot,
        (shape((row_count, block, LANES), BF16), shape((1, docs), F32)),
        [ANY, ANY],
        2 * row_count * CAP * docs * width,
        [
            pltpu.VMEM((1, docs), jnp.int32),
            pltpu.VMEM((docs, width), BF16),
            pltpu.SemaphoreType.DMA((2,)),
        ],
    )(in_hbm(labels), in_hbm(embeddings))
    got = exchange(sends, ROWS)
    total = GROUP_CLUSTERS * CAP
    sends = call(reslot, shape((total, width), BF16), [VMEM], 2 * total * row_count * CAP * width)(
        got
    )
    own = exchange(sends.reshape(GROUP_CLUSTERS, CAP, width), CHIPS)
    own, got = lax.optimization_barrier((own.reshape(total, width), got))
    pairs = [(i, i ^ 1) for i in range(col_count)]
    half = total // 2
    other = [lax.ppermute(own[s : s + half], COLS, pairs) for s in (0, half)]
    flops = 2 * total * half * width
    lines = row_count * GROUP_CLUSTERS * 2
    found = call(best_own, shape((2, total), F32), [VMEM], flops)(own)
    theirs = lax.ppermute(found, COLS, pairs)
    parts = (shape((1, total), F32), shape((half, LANES), F32))
    best, more_rows = call(best_more, parts, [VMEM] * 3, flops)(own, other[0], found)
    index = call(return_index, shape((1, docs), jnp.int32), [VMEM] * 3, 2**26)(labels, rank, got)
    results = call(best_last, shape((lines, LANES), F32), [VMEM] * 6, flops)(
        own, other[1], best, found, more_rows, theirs
    )
    results, index = lax.optimization_barrier((results, index))
    results = exchange(results.astype(WIRE).reshape(lines // 2, 2, LANES), SAME_CORE)
    results = results.reshape(lines, LANES).astype(F32)
    best, hist = call(
        pick_results, (shape((1, docs), F32), shape((1, BINS), F32)), [VMEM, VMEM], 2**26
    )(index, results)
    return (best.reshape(docs), hist.reshape(BINS))


def solution(mesh):
    torus = Mesh(
        mesh.devices.reshape(2, 4, 2, 8, 2), ("rows_0", "rows_1", "cols_0", "cols_1", "cols_2")
    )
    in_specs = (P(ALL, None), P(ALL))
    out_specs = (P(ALL), P())
    return jax.shard_map(
        shards, mesh=torus, in_specs=in_specs, out_specs=out_specs, check_vma=False
    )
```

```python
import jax
import jax.numpy as jnp
from jax import lax
from jax.experimental import pallas as pl
from jax.experimental.pallas import tpu as pltpu
from jax.sharding import Mesh
from jax.sharding import PartitionSpec as P

CAP = 64
GROUP_CLUSTERS = 16
BINS = 128
ROWS = ("rows_1", "rows_0")
COLS = ("cols_0", "cols_1", "cols_2")
CHIPS = ("cols_0", "cols_1")
ALL = ("rows_0", "rows_1") + COLS
SAME_CORE = ROWS + CHIPS
LANES = 128
BLOCK = 256
EMPTY = 2.0
F32 = jnp.float32
BF16 = jnp.bfloat16
WIRE = jnp.float16
HIGH_SCALE = 2.0**10
LOW_SCALE = 2.0**18
HIST_SCALE = 16.0


def iota(shape, dim):
    return lax.broadcasted_iota(jnp.int32, shape, dim)


def dot(a, b):
    return lax.dot_general(a, b, (((1,), (0,)), ((), ())), preferred_element_type=F32)


def dot_t(a, b):
    return lax.dot_general(a, b, (((1,), (1,)), ((), ())), preferred_element_type=F32)


def ones_where(mask):
    return jnp.where(mask, 1.0, 0.0).astype(BF16)


def before(n):
    return ones_where(iota((n, n), 0) < iota((n, n), 1))


def rank_of(onehot, n):
    earlier = dot(onehot, before(n))
    return jnp.sum(onehot.astype(F32) * earlier, axis=0, keepdims=True)


def normalise_and_slot(labels_hbm, embeddings_hbm, out_ref, rank_ref, labels_ref, embeddings_ref, sems):
    labels_copy = pltpu.make_async_copy(labels_hbm, labels_ref, sems.at[0])
    embeddings_copy = pltpu.make_async_copy(embeddings_hbm, embeddings_ref, sems.at[1])
    labels_copy.start()
    embeddings_copy.start()
    docs, width = embeddings_ref.shape
    groups = out_ref.shape[0]
    clusters = groups * GROUP_CLUSTERS
    labels_copy.wait()
    labels = labels_ref[...]
    group = lax.shift_right_logical(labels, 4)
    onehot = ones_where(iota((groups, docs), 0) == group)
    slot = group * CAP + rank_of(onehot, docs).astype(jnp.int32)
    places = ones_where(iota((groups * CAP, docs), 0) == slot)
    embeddings_copy.wait()
    values = embeddings_ref[...].astype(F32)
    total = jnp.sum(values * values, axis=1, keepdims=True)
    normed = (values * lax.rsqrt(total + 1e-06)).astype(BF16)
    shifted = jnp.broadcast_to((labels + 1).astype(F32), (8, docs)).astype(BF16)
    slot_labels = dot_t(shifted, places)
    of_cluster = ones_where(iota((clusters, docs), 0) == labels)
    counts = dot_t(jnp.ones((8, docs), BF16), of_cluster)
    row = iota((8, LANES), 0)
    meta = jnp.where(row == groups * CAP // LANES, counts, 0.0)
    for s in range(groups * CAP // LANES):
        meta = jnp.where(row == s, slot_labels[:, s * LANES : (s + 1) * LANES], meta)
    meta = meta.astype(BF16)
    rank_ref[...] = rank_of(of_cluster, docs)
    rows = dot(places, normed).astype(BF16)
    pieces = width // LANES
    for g in range(groups):
        for f in range(pieces):
            block = rows[g * CAP : (g + 1) * CAP, f * LANES : (f + 1) * LANES]
            out_ref[g, f * CAP : (f + 1) * CAP, :] = block
        out_ref[g, pieces * CAP :, :] = meta


def slot_labels_of(got_ref, me):
    groups = got_ref.shape[0]
    slots = groups * CAP
    at = got_ref.shape[1] - 8
    source = lax.shift_right_logical(iota((8, slots), 1), 6)
    row = iota((8, LANES), 0)
    per_row = LANES // CAP
    picked = []
    for g in range(groups):
        meta = got_ref[g, at:, :].astype(F32)
        line = jnp.where(row == lax.shift_right_logical(me, 1), meta, 0.0)
        picked.append(jnp.sum(line, axis=0, keepdims=True))
    lines = jnp.concatenate(picked, axis=0).astype(BF16)
    lane, to = iota((LANES, slots), 0), iota((LANES, slots), 1)
    start = lax.bitwise_and(me, per_row - 1) * CAP
    move = ones_where(lane == start + lax.bitwise_and(to, CAP - 1))
    spread = jnp.where(iota((groups, slots), 0) == source, dot(lines, move), 0.0)
    return jnp.sum(spread, axis=0, keepdims=True)


def reslot(got_ref, out_ref):
    groups = got_ref.shape[0]
    slots = groups * CAP
    width = out_ref.shape[1]
    me = lax.axis_index(ROWS)
    label = slot_labels_of(got_ref, me).astype(jnp.int32)
    cluster = label - 1 - me * GROUP_CLUSTERS
    onehot = ones_where(iota((GROUP_CLUSTERS, slots), 0) == cluster)
    place = cluster * CAP + rank_of(onehot, slots).astype(jnp.int32)
    place = jnp.where(label > 0, place, -1)
    counts = jnp.sum(onehot.astype(F32), axis=1, keepdims=True).astype(jnp.int32)
    total = GROUP_CLUSTERS * CAP
    step = total // 4
    pieces = width // LANES
    rows = jnp.concatenate(
        [got_ref[:, f * CAP : (f + 1) * CAP, :].reshape(slots, LANES) for f in range(pieces)],
        axis=1,
    )
    lane, rank = iota((CAP, LANES), 1), iota((CAP, LANES), 0)
    marks = []
    for c in range(GROUP_CLUSTERS):
        empty = (rank >= counts[c : c + 1, :]) & (lane == 0)
        marks.append(jnp.where(empty, EMPTY, 0.0))
    for s in range(0, total, step):
        places = ones_where(iota((step, slots), 0) + s == place)
        moved = dot(places, rows)
        out_ref[s : s + step, LANES:] = moved[:, LANES:].astype(BF16)
        mark = jnp.concatenate(marks[s // CAP : (s + step) // CAP], axis=0)
        out_ref[s : s + step, 0:LANES] = (moved[:, 0:LANES] + mark).astype(BF16)


def return_index(labels_ref, rank_ref, got_ref, out_ref):
    groups = got_ref.shape[0]
    docs = labels_ref.shape[1]
    clusters = groups * GROUP_CLUSTERS
    me = lax.axis_index(ROWS)
    at = got_ref.shape[1] - 8
    row = iota((8, LANES), 0)
    before_me = jnp.zeros((8, LANES), F32)
    for g in range(groups):
        before_me = before_me + jnp.where(g < me, got_ref[g, at:, :].astype(F32), 0.0)
    counts = jnp.where(row == groups * CAP // LANES, before_me, 0.0)
    labels = labels_ref[...]
    of_cluster = ones_where(iota((clusters, docs), 0) == labels)
    earlier = jnp.sum(dot(counts.astype(BF16), of_cluster), axis=0, keepdims=True)
    out_ref[...] = labels * CAP + (rank_ref[...] + earlier).astype(jnp.int32)


def column_of(ref):
    return jnp.where(ref[:, 0:1].astype(F32) < 1.5, 0.0, -4.0)


def penalties(ref):
    column = column_of(ref)
    pick = ones_where(iota((8, 256), 1) == 0)
    row = jnp.where(dot_t(pick, ref[:, 0:256])[0:1, :] < 1.5, 0.0, -4.0)
    return column, row


def over_columns(scores):
    return jnp.max(scores.reshape(BLOCK // 8, 8, BLOCK), axis=0)


def over_rows(scores):
    return jnp.maximum(scores[:, :LANES], scores[:, LANES:])


def as_line(columns, rows):
    out = []
    for column, row in zip(columns, rows):
        line = jnp.max(column, axis=0, keepdims=True)
        if row is not None:
            turned = [jnp.max(row[h : h + LANES].T, axis=0, keepdims=True) for h in (0, LANES)]
            line = jnp.maximum(line, jnp.concatenate(turned, axis=1))
        out.append(line)
    return jnp.concatenate(out, axis=1)


def larger(a, b):
    return b if a is None else jnp.maximum(a, b)


def within(ref, penalty, columns, rows):
    column, row = penalty
    count = ref.shape[0] // BLOCK
    for i in range(count):
        for j in range(i, count):
            at, to = i * BLOCK, j * BLOCK
            scores = dot_t(ref[at : at + BLOCK, :], ref[to : to + BLOCK, :])
            scores = scores + column[at : at + BLOCK] + row[:, to : to + BLOCK]
            if i == j:
                other = iota((BLOCK, BLOCK), 0) != iota((BLOCK, BLOCK), 1)
                scores = jnp.where(other, scores, -4.0)
            else:
                rows[i] = larger(rows[i], over_rows(scores))
            columns[j] = larger(columns[j], over_columns(scores))


def between(a_ref, a_penalty, b_ref, b_penalty, rows, columns):
    for i in range(a_ref.shape[0] // BLOCK):
        for j in range(b_ref.shape[0] // BLOCK):
            at, to = i * BLOCK, j * BLOCK
            scores = dot_t(a_ref[at : at + BLOCK, :], b_ref[to : to + BLOCK, :])
            scores = scores + a_penalty[0][at : at + BLOCK] + b_penalty[1][:, to : to + BLOCK]
            rows[i] = larger(rows[i], over_rows(scores))
            columns[j] = larger(columns[j], over_columns(scores))


def nothing(ref):
    return [None] * (ref.shape[0] // BLOCK)


def best_own(own_ref, labels_ref, rank_ref, got_ref, found_ref, index_ref):
    return_index(labels_ref, rank_ref, got_ref, index_ref)
    columns, rows = nothing(own_ref), nothing(own_ref)
    penalty = penalties(own_ref)
    within(own_ref, penalty, columns, rows)
    best = jnp.maximum(as_line(columns, rows), -1.0)
    found_ref[...] = jnp.where(penalty[1] < 0.0, -8.0, best)


def penalty_of(found):
    return jnp.where(found < -4.0, -4.0, 0.0)


def best_more(own_ref, more_ref, found_ref, best_ref, rows_ref):
    rows, of_own = nothing(more_ref), nothing(own_ref)
    penalty = (column_of(more_ref), None)
    between(more_ref, penalty, own_ref, (None, penalty_of(found_ref[...])), rows, of_own)
    rows_ref[...] = jnp.concatenate(rows, axis=0)
    best_ref[...] = jnp.maximum(as_line(of_own, nothing(own_ref)), found_ref[...])


def histogram_parts(best, penalty):
    width = 2.0 / (BINS - 1)
    centers = -1.0 + iota((BINS, 1), 0).astype(F32) * width
    weights = jnp.maximum(1.0 - jnp.abs(best - centers) / width, 0.0)
    weights = jnp.where(penalty < 0.0, 0.0, weights)
    folded = weights[:, 0:LANES]
    for s in range(LANES, best.shape[1], LANES):
        folded = folded + weights[:, s : s + LANES]
    return folded


def best_last(
    own_ref, last_ref, so_far_ref, found_ref, more_rows_ref, theirs_ref, out_ref
):
    total = own_ref.shape[0]
    own_penalty = (None, penalty_of(found_ref[...]))
    rows, of_own = nothing(last_ref), nothing(own_ref)
    starts = range(0, more_rows_ref.shape[0], BLOCK)
    more_rows = [more_rows_ref[s : s + BLOCK, :] for s in starts]
    between(last_ref, (column_of(last_ref), None), own_ref, own_penalty, rows, of_own)
    best = jnp.maximum(as_line(of_own, nothing(own_ref)), so_far_ref[...])
    rows = more_rows + rows
    their_line = [theirs_ref[:, s : s + BLOCK] for s in range(0, total, BLOCK)]
    their_best = as_line(their_line, rows)
    mine = histogram_parts(best, own_penalty[1])
    theirs = histogram_parts(their_best, penalty_of(theirs_ref[...]))
    hist = jnp.sum((mine + theirs).T, axis=0, keepdims=True)
    high = best.astype(BF16).astype(F32)
    low = (best - high) * LOW_SCALE
    high = high * HIGH_SCALE
    hist = hist * HIST_SCALE
    sub = iota((8, LANES), 0)
    left = iota((1, LANES), 1) < CAP
    blocks = []
    for s in range(0, total, 2 * LANES):
        block = jnp.broadcast_to(hist, (8, LANES))
        for h in range(2):
            at = s + h * LANES
            top, rest = high[:, at : at + LANES], low[:, at : at + LANES]
            first = jnp.where(left, top, pltpu.roll(rest, CAP, 1))
            second = jnp.where(left, pltpu.roll(top, CAP, 1), rest)
            block = jnp.where(sub == 4 * h + 1, first, block)
            block = jnp.where(sub == 4 * h + 3, second, block)
        blocks.append(block)
    block = jnp.concatenate(blocks, axis=0)
    for at in range(0, out_ref.shape[0], block.shape[0]):
        out_ref[at : at + block.shape[0], :] = block


def pick_results(index_ref, got_ref, best_ref, hist_ref):
    lines = got_ref.shape[0]
    docs = index_ref.shape[1]
    index = index_ref[...]
    line = lax.shift_right_logical(index, 6) * 2 + 1
    rank = lax.bitwise_and(index, CAP - 1)
    onehot = ones_where(iota((lines, docs), 0) == line)
    got = got_ref[...]
    turned = got.T
    high = turned.astype(BF16)
    low = (turned - high.astype(F32)).astype(BF16)
    picked = dot(high, onehot) + dot(low, onehot)
    lane = iota((LANES, docs), 0)
    picked = picked * jnp.where(lane < CAP, 1.0 / HIGH_SCALE, 1.0 / LOW_SCALE)
    wanted = lax.bitwise_and(lane, CAP - 1) == rank
    best_ref[...] = jnp.sum(jnp.where(wanted, picked, 0.0), axis=0, keepdims=True)
    even = lax.bitwise_and(iota((8, LANES), 0), 1) == 0
    total = jnp.zeros((8, LANES), F32)
    for s in range(0, lines, 8):
        total = total + jnp.where(even, got[s : s + 8, :], 0.0)
    hist_ref[...] = jnp.sum(total, axis=0, keepdims=True) * (1.0 / (HIST_SCALE * lines * docs))


VMEM = pl.BlockSpec(memory_space=pltpu.VMEM)
ANY = pl.BlockSpec(memory_space=pl.ANY)


def call(kernel, outs, specs, flops, scratch=()):
    many = isinstance(outs, tuple)
    return pl.pallas_call(
        kernel,
        out_shape=outs,
        in_specs=specs,
        out_specs=tuple(VMEM for _ in outs) if many else VMEM,
        scratch_shapes=scratch,
        compiler_params=pltpu.CompilerParams(vmem_limit_bytes=24 * 2**20),
        cost_estimate=pl.CostEstimate(flops=flops, bytes_accessed=4000000, transcendentals=0),
    )


def shape(dims, dtype):
    return jax.ShapeDtypeStruct(dims, dtype)


def in_hbm(x):
    return pltpu.with_memory_space_constraint(x, pltpu.HBM)


def exchange(x, axes):
    return lax.all_to_all(x, axes, split_axis=0, concat_axis=0, tiled=True)


def shards(embeddings, document_cluster_index):
    row_count = lax.axis_size(ROWS)
    col_count = lax.axis_size(COLS)
    docs, width = embeddings.shape
    labels = document_cluster_index.reshape(1, docs)
    block = CAP * width // LANES + 8
    sends, rank = call(
        normalise_and_slot,
        (shape((row_count, block, LANES), BF16), shape((1, docs), F32)),
        [ANY, ANY],
        2 * row_count * CAP * docs * width,
        [
            pltpu.VMEM((1, docs), jnp.int32),
            pltpu.VMEM((docs, width), BF16),
            pltpu.SemaphoreType.DMA((2,)),
        ],
    )(in_hbm(labels), in_hbm(embeddings))
    got = exchange(sends, ROWS)
    total = GROUP_CLUSTERS * CAP
    sends = call(reslot, shape((total, width), BF16), [VMEM], 2 * total * row_count * CAP * width)(
        got
    )
    own = exchange(sends.reshape(GROUP_CLUSTERS, CAP, width), CHIPS)
    own, got = lax.optimization_barrier((own.reshape(total, width), got))
    pairs = [(i, i ^ 1) for i in range(col_count)]
    half = total // 2
    other = [lax.ppermute(own[s : s + half], COLS, pairs) for s in (0, half)]
    flops = 2 * total * half * width
    lines = row_count * GROUP_CLUSTERS * 2
    outs = (shape((1, total), F32), shape((1, docs), jnp.int32))
    found, index = call(best_own, outs, [VMEM] * 4, flops)(own, labels, rank, got)
    theirs = lax.ppermute(found, COLS, pairs)
    parts = (shape((1, total), F32), shape((half, LANES), F32))
    best, more_rows = call(best_more, parts, [VMEM] * 3, flops)(own, other[0], found)
    results = call(best_last, shape((lines, LANES), F32), [VMEM] * 6, flops)(
        own, other[1], best, found, more_rows, theirs
    )
    results = exchange(results.astype(WIRE).reshape(lines // 2, 2, LANES), SAME_CORE)
    results = results.reshape(lines, LANES).astype(F32)
    best, hist = call(
        pick_results, (shape((1, docs), F32), shape((1, BINS), F32)), [VMEM, VMEM], 2**26
    )(index, results)
    return (best.reshape(docs), hist.reshape(BINS))


def solution(mesh):
    torus = Mesh(
        mesh.devices.reshape(2, 4, 2, 8, 2), ("rows_0", "rows_1", "cols_0", "cols_1", "cols_2")
    )
    in_specs = (P(ALL, None), P(ALL))
    out_specs = (P(ALL), P())
    return jax.shard_map(
        shards, mesh=torus, in_specs=in_specs, out_specs=out_specs, check_vma=False
    )
```
